768 devices in a mesh: cluster: 96 (over y, z), sub: 8 (over x, core).
Axes of the slice: x: 4, y: 8, z: 12, core: 2. Of those that a mesh axis runs over, the one named last changes fastest.
Arguments:
- rhs: float32 [3072, 4, 384], P(('cluster', 'sub')), may hold values from -8 to 8
- operators: bfloat16 [3072, 384, 384], P(('cluster', 'sub')), may hold values from -1 to 5
- signs: int32 [3072, 384], P(('cluster', 'sub')), may hold values from -1 to 1, as said below
- links: int32 [3072, 3, 128], P(('cluster', 'sub')), may hold values from 0 to 127, as said below
- cluster_basis: float32 [3072, 24, 384], P(('cluster', 'sub')), may hold values from -0.3125 to 0.3125
- corner_basis: float32 [3072, 8, 384], P(('cluster', 'sub')), may hold values from -0.3125 to 0.3125
- corner_ids: int32 [3072, 8], P(('cluster', 'sub')), may hold values from 0 to 1535
- cluster_coarse: float32 [96, 768, 768], P('cluster', 'sub'), may hold values from -1 to 3
- global_coarse: float32 [1536, 1536], P('sub'), may hold values from -0.2 to 0.5
Outputs:
- multipliers: float32 [3072, 4, 384], P(('cluster', 'sub'))
- residual: float32 [3072, 4, 384], P(('cluster', 'sub'))
The draws below stay inside these ranges and needn't reach their ends.
Inputs may be any that keep to these rules, and one draw needn't show every extreme that they name: `signs`: each entry is -1 or 1. Each links[s, b] is a permutation of 0 to 127; both subdomains of an interface pair hold the same permutation for it.
All inputs are finite; a program needn't handle non-finite values.
Results may differ from the reference program's by a relative error of at most 0.007.
Values sent between devices are 32-bit elements; how exact they have to be, the bound alone decides.
No kernel may reach another device: no remote copies, remote signals or barrier semaphores. Data moves between devices by JAX's collectives and lax.ppermute only.
A program may use at most 32 MiB of HBM per device.

```python
import math
from functools import partial
import jax
import jax.numpy as jnp
from jax import lax

SUB_DEV = 4
LOADS = 4
BLK = 128
KC = 24
CORN = 8
ITERS = 2
DUAL = 384
CLUSTERS = 96
SUBS = 3072
CCO = 768
NG = 1536
N_SUB = 8


def draw_rhs(key, part):
    position = jnp.arange(SUBS, dtype=jnp.float32) / SUBS
    values = jnp.clip(jax.random.normal(key, (SUBS, LOADS, DUAL), jnp.float32), -4.0, 4.0)
    scaling = 0.6 + 1.2 * position
    return values * scaling[:, None, None]


def draw_operators(key, part):
    first_key, second_key = jax.random.split(key)
    identity = jnp.eye(DUAL, dtype=jnp.float32)
    diagonal = jnp.exp(jax.random.uniform(first_key, (SUBS, DUAL), jnp.float32, 0.0, math.log(4.0)))
    coupling = jnp.clip(jax.random.normal(second_key, (SUBS, DUAL, DUAL), jnp.float32), -4.0, 4.0) * (0.3 / math.sqrt(DUAL))
    return (coupling * (1.0 - identity) + diagonal[:, :, None] * identity).astype(jnp.bfloat16)


def coarse_matrix(key, leading, order):
    second_key = jax.random.fold_in(key, 1)
    identity = jnp.eye(order, dtype=jnp.float32)
    diagonal = jnp.ones(leading + (order,), jnp.float32)
    coupling = jnp.clip(jax.random.normal(second_key, leading + (order, order), jnp.float32), -4.0, 4.0) * (0.5 / math.sqrt(order))
    return coupling * (1.0 - identity) + diagonal[..., None] * identity


def draw_cluster_coarse(key, part):
    return coarse_matrix(key, (CLUSTERS,), CCO)


def draw_global_coarse(key, part):
    return 0.15 * coarse_matrix(key, (), NG)


def draw_signs(key, part):
    return 2 * jax.random.randint(key, (SUBS, DUAL), 0, 2, jnp.int32) - 1


def shuffle(base_key, pair_id):
    return jax.random.permutation(jax.random.fold_in(base_key, pair_id), BLK)


def draw_links(key, part):
    numbers = jnp.arange(SUBS, dtype=jnp.int32)
    member = numbers % SUB_DEV
    position = numbers // SUB_DEV % N_SUB
    cluster = numbers // (SUB_DEV * N_SUB)
    stride = SUB_DEV * N_SUB
    down_pair = jnp.where(position > 0, numbers - SUB_DEV, numbers + SUBS)
    across_pair = jnp.where(member % 2 == 0, numbers, jnp.where(cluster > 0, numbers - stride - 1, numbers + SUBS))
    inside_key = jax.random.fold_in(key, 11)
    outside_key = jax.random.fold_in(key, 23)
    up_order = jax.vmap(partial(shuffle, inside_key))(numbers)
    down_order = jax.vmap(partial(shuffle, inside_key))(down_pair)
    across_order = jax.vmap(partial(shuffle, outside_key))(across_pair)
    return jnp.stack([up_order, down_order, across_order], axis=1).astype(jnp.int32)


def with_ends(values, stream_key, least, largest):
    index_at = [jax.random.randint(jax.random.fold_in(stream_key, axis), (), 0, length) for axis, length in enumerate(values.shape)]
    widest = values.shape.index(max(values.shape))
    neighbour = index_at[:widest] + [(index_at[widest] + 1) % values.shape[widest]] + index_at[widest + 1:]
    return values.at[tuple(index_at)].set(least).at[tuple(neighbour)].set(largest)


def shard_levels(stream_key, shape, pieces, smallest, largest):
    factor_of = 1.0
    for dim, blocks in pieces:
        draws = jax.random.uniform(jax.random.fold_in(jax.random.fold_in(stream_key, 6), dim), (blocks,), jnp.float32, smallest / len(pieces), largest / len(pieces))
        factor_of = factor_of * jnp.repeat(jnp.exp(draws), shape[dim] // blocks).reshape((-1,) + (1,) * (len(shape) - 1 - dim))
    return factor_of


def scatter_about(key, shape, deviation, most, pieces=(), held_as=jnp.bfloat16):
    entries = jax.random.normal(key, shape, jnp.float32) * deviation
    if len(pieces) > 0:
        entries = shard_levels(key, shape, pieces, -0.22, 0.18) * entries
    return jnp.clip(entries, min=-most, max=most).astype(held_as)


def setup_inputs(seed: int = 0) -> dict:
    streams_of = jax.random.split(jax.random.key(seed), 10)
    rhs = draw_rhs(jax.random.fold_in(streams_of[9], 71), 0)
    operators = draw_operators(jax.random.fold_in(streams_of[9], 71), 0)
    signs = draw_signs(jax.random.fold_in(streams_of[9], 71), 0)
    links = draw_links(jax.random.fold_in(streams_of[9], 71), 0)
    cluster_basis = scatter_about(streams_of[4], (SUBS, KC, DUAL), DUAL ** -0.5, 0.3125, ((0, 768),), jnp.float32)
    corner_basis = scatter_about(streams_of[5], (SUBS, CORN, DUAL), DUAL ** -0.5, 0.3125, ((0, 768),), jnp.float32)
    corner_ids = with_ends(jax.random.randint(streams_of[6], (SUBS, CORN), 0, NG), jax.random.fold_in(streams_of[6], 1), 0, NG - 1).astype(jnp.int32)
    cluster_coarse = draw_cluster_coarse(jax.random.fold_in(streams_of[9], 71), 0)
    global_coarse = draw_global_coarse(jax.random.fold_in(streams_of[9], 71), 0)
    return {"rhs": rhs, "operators": operators, "signs": signs, "links": links, "cluster_basis": cluster_basis, "corner_basis": corner_basis, "corner_ids": corner_ids, "cluster_coarse": cluster_coarse, "global_coarse": global_coarse}


HIGHEST_PRECISION = lax.Precision.HIGHEST


def invert(order):
    row_index = jnp.broadcast_to(jnp.arange(order.shape[0], dtype=jnp.int32)[:, None], order.shape)
    col_index = jnp.broadcast_to(jnp.arange(order.shape[1], dtype=jnp.int32)[None, :], order.shape)
    return jnp.zeros_like(order).at[row_index, order].set(col_index)


def permuted(blocks, order):
    return jnp.take_along_axis(blocks, order[:, None, :], axis=2)


def swap(vector, tables):
    inv_up, order_down, inv_across, order_across = tables
    up_part = vector[:, :, :BLK]
    down_part = vector[:, :, BLK:2 * BLK]
    across = vector[:, :, 2 * BLK:]
    send_up = permuted(up_part, inv_up)
    send_down = permuted(down_part, order_down)
    parity = (jnp.arange(SUBS, dtype=jnp.int32) % 2) == 0
    send_across = jnp.where(parity[:, None, None], permuted(across, inv_across), permuted(across, order_across))
    layout = (CLUSTERS, N_SUB, SUB_DEV, LOADS, BLK)
    down_grid = send_down.reshape(layout)
    up_grid = send_up.reshape(layout)
    zero_rows = jnp.zeros_like(down_grid[:, :1])
    new_up = jnp.concatenate([down_grid[:, 1:], zero_rows], axis=1).reshape(SUBS, LOADS, BLK)
    new_down = jnp.concatenate([zero_rows, up_grid[:, :-1]], axis=1).reshape(SUBS, LOADS, BLK)
    paired = send_across.reshape(CLUSTERS, N_SUB, SUB_DEV // 2, 2, LOADS, BLK)
    even_part = paired[:, :, :, 0]
    odd_part = paired[:, :, :, 1]
    empty_part = jnp.zeros_like(even_part[:1])
    new_even = jnp.concatenate([odd_part[1:], empty_part], axis=0)
    new_odd = jnp.concatenate([empty_part, even_part[:-1]], axis=0)
    new_across = jnp.stack([new_even, new_odd], axis=3).reshape(SUBS, LOADS, BLK)
    return jnp.concatenate([new_up, new_down, new_across], axis=2)


def apply(vector, sign_field, operators, tables):
    spread = sign_field * (vector + swap(vector, tables))
    spread_bf = spread.astype(jnp.bfloat16)
    product = jnp.einsum("srk,skl->srl", spread_bf.astype(jnp.float32), operators.astype(jnp.float32), precision=HIGHEST_PRECISION)
    signed = sign_field * product
    result = signed + swap(signed, tables)
    curvature = jnp.sum(vector * result, axis=(0, 2))
    return result, curvature


def project(vector, cluster_basis, corner_basis, corner_ids, cluster_coarse, global_coarse):
    per_cluster = SUBS // CLUSTERS
    cluster_coef = jnp.einsum("srl,skl->srk", vector, cluster_basis, precision=HIGHEST_PRECISION)
    grouped = cluster_coef.reshape(CLUSTERS, per_cluster, LOADS, KC).transpose(0, 2, 1, 3).reshape(CLUSTERS, LOADS, CCO)
    solved = jnp.einsum("crm,cmn->crn", grouped, cluster_coarse, precision=HIGHEST_PRECISION)
    spread_back = solved.reshape(CLUSTERS, LOADS, per_cluster, KC).transpose(1, 0, 2, 3).reshape(LOADS, SUBS, KC)
    fix_cluster = jnp.einsum("rsk,skl->srl", spread_back, cluster_basis, precision=HIGHEST_PRECISION)
    flat_ids = corner_ids.reshape(-1).astype(jnp.int32)
    corner_coef = jnp.einsum("scl,srl->scr", corner_basis, vector, precision=HIGHEST_PRECISION).reshape(SUBS * CORN, LOADS)
    corner_sum = jax.ops.segment_sum(corner_coef, flat_ids, num_segments=NG)
    global_coef = jnp.dot(corner_sum.T, global_coarse, precision=HIGHEST_PRECISION)
    picked = jnp.take(global_coef, flat_ids, axis=1).reshape(LOADS, SUBS, CORN)
    fix_corner = jnp.einsum("rsc,scl->srl", picked, corner_basis, precision=HIGHEST_PRECISION)
    squares = jnp.sum(vector * vector, axis=(0, 2))
    return vector - fix_cluster - fix_corner, squares


def reference(rhs, operators, signs, links, cluster_basis, corner_basis, corner_ids, cluster_coarse, global_coarse):
    sign_field = signs.astype(jnp.float32)[:, None, :]
    tables = (invert(links[:, 0]), links[:, 1], invert(links[:, 2]), links[:, 2])
    residual = rhs
    projected, residual_norm = project(residual, cluster_basis, corner_basis, corner_ids, cluster_coarse, global_coarse)
    direction = projected
    multipliers = jnp.zeros_like(rhs)
    for iteration in range(ITERS):
        product, curvature = apply(direction, sign_field, operators, tables)
        step_size = (residual_norm / curvature)[None, :, None]
        multipliers = multipliers + step_size * direction
        residual = residual - step_size * product
        if iteration + 1 < ITERS:
            projected, norm_next = project(residual, cluster_basis, corner_basis, corner_ids, cluster_coarse, global_coarse)
            direction = projected + (norm_next / residual_norm)[None, :, None] * direction
            residual_norm = norm_next
    return multipliers, residual
```

```python
import jax
import jax.numpy as jnp
from jax import lax
from jax.experimental import pallas as pl
from jax.experimental.pallas import tpu as pltpu
from jax.sharding import PartitionSpec as P

F32 = jnp.float32
BF16 = jnp.bfloat16
I32 = jnp.int32
R = 4
S = 4
ROWS = R * S
B = 128
D = 384
KC = 24
NB = 128
NCL = S * KC
CHUNK = 192
NSUB = 8


def iota(shape, dim):
    return lax.broadcasted_iota(I32, shape, dim)


def split(x):
    hi = x.astype(BF16)
    return hi, (x - hi.astype(F32)).astype(BF16)


def mm(a, b):
    return lax.dot_general(a, b, (((1,), (0,)), ((), ())), preferred_element_type=F32)


def mm_t(a, b):
    return lax.dot_general(a, b, (((1,), (1,)), ((), ())), preferred_element_type=F32)


def dot2(x, w, f=mm):
    n = x.shape[0]
    xh, xl = split(x)
    wh, wl = split(w)
    xs = jnp.concatenate([xh, xl], axis=0)
    both = f(xs, wh)
    return both[:n] + both[n:] + f(xh, wl)


def lanes_of_sub(shape):
    lane = iota(shape, 1)
    return jnp.where(lane < NCL, lane // KC, (lane - NCL) // 8)


def own_mask():
    return iota((ROWS, NB), 0) // R == lanes_of_sub((ROWS, NB))


def by_load(x):
    y = x[:8] + x[8:]
    y = y + pltpu.roll(y, 4, 0)
    return jnp.concatenate([y, y], axis=0)


def coefs(v, w):
    return by_load(jnp.where(own_mask(), dot2(v, w, mm_t), 0.0))


def spread_back(sol, w):
    return dot2(jnp.where(own_mask(), sol, 0.0), w)


def ids_row(ids):
    lane = iota((8, NB), 1)
    row = jnp.full((8, NB), -1, I32)
    for s in range(S):
        for c in range(8):
            row = jnp.where(lane == NCL + 8 * s + c, ids[s, c], row)
    return row


def to_column(row):
    full = jnp.broadcast_to(row[:1], (NB, NB))
    eye = iota((NB, NB), 0) == iota((NB, NB), 1)
    return jnp.sum(jnp.where(eye, full, 0.0), axis=1, keepdims=True)


def write_message(msg, coef, cc, ids, scalars):
    row = ids_row(ids).astype(F32)
    col = to_column(row).astype(I32)
    c4 = coef[:8]
    hi, lo = split(c4)
    low = (c4 - hi.astype(F32) - lo.astype(F32)).astype(BF16)
    parts = jnp.concatenate([hi[:8], lo[:8], low[:8]], axis=0)
    ccp = dot2(jnp.where(iota((8, NB), 1) < NCL, c4, 0.0)[:, :NCL], cc[...])
    lane = iota((8, B), 1)
    extra = jnp.zeros((8, B), F32)
    for j, val in enumerate(scalars):
        extra = jnp.where(lane == 64 + j, val, extra)
    for k in range(NSUB):
        n = iota((NB, 2 * B), 1)
        onehot = jnp.where((col == n + CHUNK * k) & (n < CHUNK), 1.0, 0.0).astype(BF16)
        y = mm(parts, onehot)
        y = y[:8] + y[8:16] + y[16:24]
        first = y[:, :B]
        second = y[:, B:] + extra
        at = NCL * k
        tile, off = at // B, at % B
        here = ccp[:, tile * B : (tile + 1) * B]
        if off:
            here = pltpu.roll(here, B - off, 1)
            if off + NCL > B:
                after = pltpu.roll(ccp[:, (tile + 1) * B : (tile + 2) * B], B - off, 1)
                here = jnp.where(lane < B - off, here, after)
        third = jnp.where(lane < NCL, here, row)
        msg[k, :, 0:B] = first[:R]
        msg[k, :, B : 2 * B] = second[:R]
        msg[k, :, 2 * B : 3 * B] = third[:R]


def row_dot(a, b):
    return by_load(jnp.sum(a * b, axis=1, keepdims=True))


def k_start(ids, rhs, cb, kb, cc, signs, links, msg, w_out, v_out, sg_out, idx_out):
    for s in range(S):
        v_out[R * s : R * s + R, :] = rhs[s]
        sg_out[R * s : R * s + R, :] = jnp.broadcast_to(signs[s : s + 1, :].astype(F32), (R, D))
        w_out[KC * s : KC * s + KC, :] = cb[s]
        w_out[NCL + 8 * s : NCL + 8 * s + 8, :] = kb[s]
    pos = iota((8, B), 1).astype(BF16)
    for s in range(S):
        for b in range(3):
            q = links[s, b : b + 1, :]
            if b == 0 or (b == 2 and s % 2 == 0):
                hot = jnp.where(iota((B, B), 0) == q, 1.0, 0.0).astype(BF16)
                q = mm_t(pos, hot)[:1].astype(I32)
            idx_out[b, R * s : R * s + R, :] = jnp.broadcast_to(q, (R, B))
    v = v_out[...]
    coef = coefs(v, w_out[...])
    write_message(msg, coef, cc, ids, [row_dot(v, v)[:8]])


def k_rows(recv, out, csol):
    total = recv[0]
    for k in range(1, NSUB):
        total = total + recv[k]
    x = jnp.concatenate([total[:, :B], total[:, B : 2 * B]], axis=0)
    out[...] = jnp.broadcast_to(x[None], out.shape)
    csol[...] = jnp.where(iota((R, B), 1) < NCL, total[:, 2 * B :], 0.0)


def k_picked(recv, gc, hi_out, lo_out):
    lane = iota((8, B), 1)
    cols = []
    for half in range(2):
        ids = jnp.zeros((8, B), F32)
        for j in range(4):
            row = jnp.broadcast_to(recv[4 * half + j, 0:1, 2 * B : 3 * B], (8, B))
            ids = jnp.where(lane // 32 == j, pltpu.roll(row, (32 + 32 * j) % B, 1), ids)
        cols.append(ids[:1].astype(I32))
    ids = jnp.concatenate(cols, axis=1)
    n = iota((gc.shape[1], 2 * B), 0)
    onehot = jnp.where(n == ids, 1.0, 0.0).astype(BF16)
    gh, gl = split(gc[...])
    zero = jnp.zeros((2 * B - CHUNK, 2 * B), BF16)
    hi_out[0:CHUNK, :] = mm(gh, onehot).astype(BF16)
    hi_out[CHUNK : 2 * B, :] = zero
    lo_out[0:CHUNK, :] = mm(gl, onehot).astype(BF16)
    lo_out[CHUNK : 2 * B, :] = zero


def k_global(recv, gh, gl, msg, scal):
    total = jnp.sum(recv[...], axis=0)
    first = jnp.concatenate([total[:R], total[:R]], axis=0)
    second = jnp.concatenate([total[R:], total[R:]], axis=0)
    lane = iota((8, B), 1)
    x = jnp.concatenate([first, jnp.where(lane < 64, second, 0.0)], axis=1)
    xh, xl = split(x)
    y = mm(jnp.concatenate([xh, xl], axis=0), gh[...])
    y = y[:8] + y[8:] + mm(xh, gl[...])
    for k in range(NSUB):
        tile, j = k // 4, k % 4
        here = pltpu.roll(y[:, tile * B : (tile + 1) * B], (96 - 32 * j) % B, 1)
        msg[k] = jnp.where(lane < NCL, 0.0, here)[:R]
    scal[...] = jnp.concatenate([second, second], axis=0)


def solution_of(recv, csol):
    total = recv[0]
    for k in range(1, NSUB):
        total = total + recv[k]
    sol = total + csol[...]
    sol = jnp.concatenate([sol, sol], axis=0)
    return jnp.concatenate([sol, sol], axis=0)


def write_sends(v, idx, up, down, even, odd):
    def moved(b):
        return jnp.take_along_axis(v[:, b * B : (b + 1) * B], idx[b], axis=1)

    up[...] = moved(0)
    down[...] = moved(1)
    across = moved(2)
    for h in range(2):
        even[R * h : R * h + R, :] = across[8 * h : 8 * h + 4]
        odd[R * h : R * h + R, :] = across[8 * h + 4 : 8 * h + 8]


def received(from_next, from_prev, odd_in, even_in):
    across = jnp.concatenate(
        [odd_in[0:R, :], even_in[0:R, :], odd_in[R : 2 * R, :], even_in[R : 2 * R, :]], axis=0
    )
    return jnp.concatenate([from_next[...], from_prev[...], across], axis=1)


def k_first_direction(recv, csol, w, v, idx, d_out, up, down, even, odd):
    d = v[...] - spread_back(solution_of(recv, csol), w[...])
    d_out[...] = d
    write_sends(d, idx, up, down, even, odd)


def image_of(d, pi, sg, ops):
    spread = sg * (d + pi)
    low = spread.astype(BF16)
    image = jnp.zeros((ROWS, D), F32)
    row = iota((ROWS, D), 0) // R
    for s in range(S):
        image = jnp.where(row == s, mm(low, ops[s]), image)
    return sg * image, row_dot(spread, image)


def k_image(d, fn, fp, oi, ei, sg, ops, idx, signed_out, curv, up, down, even, odd):
    signed, c = image_of(d[...], received(fn, fp, oi, ei), sg[...], ops)
    signed_out[...] = signed
    curv[...] = jnp.broadcast_to(c[:8], (8, B))
    write_sends(signed, idx, up, down, even, odd)


def k_product(ids, signed, fn, fp, oi, ei, v, w, cc, curv, ap_out, msg):
    ap = signed[...] + received(fn, fp, oi, ei)
    ap_out[...] = ap
    scalars = [curv[...][:, :1], row_dot(v[...], ap)[:8], row_dot(ap, ap)[:8]]
    write_message(msg, coefs(ap, w[...]), cc, ids, scalars)


def scalar_at(scal, j):
    return jnp.sum(jnp.where(iota((ROWS, B), 1) == 64 + j, scal, 0.0), axis=1, keepdims=True)


def k_next_direction(recv, csol, scal0, scal1, w, d, ap, v, idx, r_out, x_out, d_out, up, down, even, odd):
    rho = scalar_at(scal0[...], 0)
    s1 = scal1[...]
    step = rho / scalar_at(s1, 0)
    rho_new = rho - 2.0 * step * scalar_at(s1, 1) + step * step * scalar_at(s1, 2)
    ap_ = ap[...]
    d0 = d[...]
    r_out[...] = v[...] - step * ap_
    x_out[...] = step * d0
    projected = d0 - step * (ap_ - spread_back(solution_of(recv, csol), w[...]))
    d1 = projected + (rho_new / rho) * d0
    d_out[...] = d1
    write_sends(d1, idx, up, down, even, odd)


def k_last_image(d, r, fn, fp, oi, ei, sg, ops, idx, signed_out, msg, up, down, even, odd):
    signed, c = image_of(d[...], received(fn, fp, oi, ei), sg[...], ops)
    rho = row_dot(r[...], r[...])
    signed_out[...] = signed
    lane = iota((8, B), 1)
    row = iota((8, B), 0)
    both = jnp.where(lane == row, c[:8], jnp.where(lane == row + R, rho[:8], 0.0))
    line = jnp.sum(jnp.where(row < R, both, 0.0), axis=0, keepdims=True)
    msg[...] = jnp.broadcast_to(line[None], msg.shape)
    write_sends(signed, idx, up, down, even, odd)


def k_total(recv, out):
    out[...] = jnp.broadcast_to(jnp.sum(recv[...], axis=0, keepdims=True), out.shape)


def k_finish(recv, signed, fn, fp, oi, ei, x, r, d, x_out, r_out):
    line = jnp.broadcast_to(jnp.sum(recv[...], axis=0), (ROWS, B))
    lane = iota((ROWS, B), 1)
    row = iota((ROWS, B), 0) % R
    curv = jnp.sum(jnp.where(lane == row, line, 0.0), axis=1, keepdims=True)
    rho = jnp.sum(jnp.where(lane == row + R, line, 0.0), axis=1, keepdims=True)
    step = rho / curv
    xn = x[...] + step * d[...]
    rn = r[...] - step * (signed[...] + received(fn, fp, oi, ei))
    for s in range(S):
        x_out[s] = xn[R * s : R * s + R]
        r_out[s] = rn[R * s : R * s + R]


def call(body, outs, *args, smem=()):
    specs = [
        pl.BlockSpec(memory_space=pltpu.SMEM if i in smem else pltpu.VMEM) for i in range(len(args))
    ]
    out_shape = tuple(jax.ShapeDtypeStruct(s, t) for s, t in outs)
    return pl.pallas_call(
        body,
        out_shape=out_shape,
        in_specs=specs,
        out_specs=tuple(pl.BlockSpec(memory_space=pltpu.VMEM) for _ in outs),
        name=body.__name__,
    )(*args)


def to_owner(x, axis):
    return lax.all_to_all(x, axis, 0, 0, tiled=True)


FIELD = ((ROWS, D), F32)
SENDS = (((ROWS, B), F32), ((ROWS, B), F32), ((2 * R, B), F32), ((2 * R, B), F32))


def exchange(up, down, even, odd, n_sub, n_cl):
    def ahead(n):
        return [(i, i + 1) for i in range(n - 1)]

    def back(n):
        return [(i + 1, i) for i in range(n - 1)]

    odd_in = lax.ppermute(odd, "cluster", back(n_cl))
    even_in = lax.ppermute(even, "cluster", ahead(n_cl))
    from_prev = lax.ppermute(up, "sub", ahead(n_sub))
    from_next = lax.ppermute(down, "sub", back(n_sub))
    return from_next, from_prev, odd_in, even_in


def local(rhs, operators, signs, links, cb, kb, ids, cluster_coarse, gc):
    n_sub = lax.axis_size("sub")
    n_cl = lax.axis_size("cluster")
    cc = cluster_coarse.reshape(NCL, NSUB * NCL)
    message = ((NSUB, R, D), F32)
    spread_rows = (((n_cl, 8, B), F32), ((R, B), F32))
    picked = ((2 * B, 2 * B), BF16)
    answer = (((NSUB, R, B), F32), ((ROWS, B), F32))

    msg, w, v, sg, idx = call(
        k_start,
        (message, ((NB, D), F32), FIELD, FIELD, ((3, ROWS, B), I32)),
        ids, rhs, cb, kb, cc, signs, links, smem=(0,),
    )
    recv = to_owner(msg, "sub")
    rows, csol = call(k_rows, spread_rows, recv)
    gh, gl = call(k_picked, (picked, picked), recv, gc)
    back, scal0 = call(k_global, answer, to_owner(rows, "cluster"), gh, gl)
    d, *sends = call(
        k_first_direction, (FIELD, *SENDS), to_owner(back, "sub"), csol, w, v, idx
    )
    got = exchange(*sends, n_sub, n_cl)
    signed, curv, *sends = call(
        k_image, (FIELD, ((8, B), F32), *SENDS), d, *got, sg, operators, idx
    )
    got = exchange(*sends, n_sub, n_cl)
    ap, msg = call(k_product, (FIELD, message), ids, signed, *got, v, w, cc, curv, smem=(0,))
    rows, csol = call(k_rows, spread_rows, to_owner(msg, "sub"))
    back, scal1 = call(k_global, answer, to_owner(rows, "cluster"), gh, gl)
    r, x, d1, *sends = call(
        k_next_direction,
        (FIELD, FIELD, FIELD, *SENDS),
        to_owner(back, "sub"), csol, scal0, scal1, w, d, ap, v, idx,
    )
    got = exchange(*sends, n_sub, n_cl)
    signed, msg, *sends = call(
        k_last_image, (FIELD, ((NSUB, 1, B), F32), *SENDS), d1, r, *got, sg, operators, idx
    )
    got = exchange(*sends, n_sub, n_cl)
    (line,) = call(k_total, (((n_cl, 1, B), F32),), to_owner(msg, "sub"))
    out = ((S, R, D), F32)
    return call(k_finish, (out, out), to_owner(line, "cluster"), signed, *got, x, r, d1)


def solution(mesh):
    both = ("cluster", "sub")
    in_specs = (
        P(both, None, None),
        P(both, None, None),
        P(both, None),
        P(both, None, None),
        P(both, None, None),
        P(both, None, None),
        P(both, None),
        P("cluster", "sub", None),
        P("sub", None),
    )
    out_specs = (P(both, None, None), P(both, None, None))
    return jax.shard_map(local, mesh=mesh, in_specs=in_specs, out_specs=out_specs, check_vma=False)
```

```python
import jax
import jax.numpy as jnp
from jax import lax
from jax.experimental import pallas as pl
from jax.experimental.pallas import tpu as pltpu
from jax.sharding import PartitionSpec as P

F32 = jnp.float32
BF16 = jnp.bfloat16
I32 = jnp.int32
R = 4
S = 4
ROWS = R * S
B = 128
D = 384
KC = 24
NB = 128
NCL = S * KC
CHUNK = 192
NSUB = 8
VMEM_LIMIT = 16 * 2**20


def iota(shape, dim):
    return lax.broadcasted_iota(I32, shape, dim)


def split(x):
    hi = x.astype(BF16)
    return hi, (x - hi.astype(F32)).astype(BF16)


def mm(a, b):
    return lax.dot_general(a, b, (((1,), (0,)), ((), ())), preferred_element_type=F32)


def mm_t(a, b):
    return lax.dot_general(a, b, (((1,), (1,)), ((), ())), preferred_element_type=F32)


def dot2(x, w, f=mm):
    n = x.shape[0]
    xh, xl = split(x)
    wh, wl = split(w)
    xs = jnp.concatenate([xh, xl], axis=0)
    both = f(xs, wh)
    return both[:n] + both[n:] + f(xh, wl)


def lanes_of_sub(shape):
    lane = iota(shape, 1)
    return jnp.where(lane < NCL, lane // KC, (lane - NCL) // 8)


def own_mask():
    return iota((ROWS, NB), 0) // R == lanes_of_sub((ROWS, NB))


def by_load(x):
    y = x[:8] + x[8:]
    y = y + pltpu.roll(y, 4, 0)
    return jnp.concatenate([y, y], axis=0)


def coefs(v, w):
    return by_load(jnp.where(own_mask(), dot2(v, w, mm_t), 0.0))


def spread_back(sol, w):
    return dot2(jnp.where(own_mask(), sol, 0.0), w)


def ids_row(ids):
    lane = iota((8, NB), 1)
    row = jnp.full((8, NB), -1, I32)
    for s in range(S):
        for c in range(8):
            row = jnp.where(lane == NCL + 8 * s + c, ids[s, c], row)
    return row


def to_column(row):
    full = jnp.broadcast_to(row[:1], (NB, NB))
    eye = iota((NB, NB), 0) == iota((NB, NB), 1)
    return jnp.sum(jnp.where(eye, full, 0.0), axis=1, keepdims=True)


def write_message(msg, coef, cc, ids, scalars):
    row = ids_row(ids).astype(F32)
    col = to_column(row).astype(I32)
    c4 = coef[:8]
    hi, lo = split(c4)
    low = (c4 - hi.astype(F32) - lo.astype(F32)).astype(BF16)
    parts = jnp.concatenate([hi[:8], lo[:8], low[:8]], axis=0)
    ccp = dot2(jnp.where(iota((8, NB), 1) < NCL, c4, 0.0)[:, :NCL], cc[...])
    lane = iota((8, B), 1)
    extra = jnp.zeros((8, B), F32)
    for j, val in enumerate(scalars):
        extra = jnp.where(lane == 64 + j, val, extra)
    for k in range(NSUB):
        n = iota((NB, 2 * B), 1)
        onehot = jnp.where((col == n + CHUNK * k) & (n < CHUNK), 1.0, 0.0).astype(BF16)
        y = mm(parts, onehot)
        y = y[:8] + y[8:16] + y[16:24]
        first = y[:, :B]
        second = y[:, B:] + extra
        at = NCL * k
        tile, off = at // B, at % B
        here = ccp[:, tile * B : (tile + 1) * B]
        if off:
            here = pltpu.roll(here, B - off, 1)
            if off + NCL > B:
                after = pltpu.roll(ccp[:, (tile + 1) * B : (tile + 2) * B], B - off, 1)
                here = jnp.where(lane < B - off, here, after)
        third = jnp.where(lane < NCL, here, row)
        msg[k, :, 0:B] = first[:R]
        msg[k, :, B : 2 * B] = second[:R]
        msg[k, :, 2 * B : 3 * B] = third[:R]


def row_dot(a, b):
    return by_load(jnp.sum(a * b, axis=1, keepdims=True))


def k_start(ids, rhs, cb, kb, cc, signs, links, msg, w_out, v_out, sg_out, idx_out):
    for s in range(S):
        v_out[R * s : R * s + R, :] = rhs[s]
        sg_out[R * s : R * s + R, :] = jnp.broadcast_to(signs[s : s + 1, :].astype(F32), (R, D))
        w_out[KC * s : KC * s + KC, :] = cb[s]
        w_out[NCL + 8 * s : NCL + 8 * s + 8, :] = kb[s]
    pos = iota((8, B), 1).astype(BF16)
    for s in range(S):
        for b in range(3):
            q = links[s, b : b + 1, :]
            if b == 0 or (b == 2 and s % 2 == 0):
                hot = jnp.where(iota((B, B), 0) == q, 1.0, 0.0).astype(BF16)
                q = mm_t(pos, hot)[:1].astype(I32)
            idx_out[b, R * s : R * s + R, :] = jnp.broadcast_to(q, (R, B))
    v = v_out[...]
    coef = coefs(v, w_out[...])
    write_message(msg, coef, cc, ids, [row_dot(v, v)[:8]])


def k_rows(recv, out, csol):
    total = recv[0]
    for k in range(1, NSUB):
        total = total + recv[k]
    x = jnp.concatenate([total[:, :B], total[:, B : 2 * B]], axis=0)
    out[...] = jnp.broadcast_to(x[None], out.shape)
    csol[...] = jnp.where(iota((R, B), 1) < NCL, total[:, 2 * B :], 0.0)


def k_picked(recv, gc, hi_out, lo_out):
    lane = iota((8, B), 1)
    cols = []
    for half in range(2):
        ids = jnp.zeros((8, B), F32)
        for j in range(4):
            row = jnp.broadcast_to(recv[4 * half + j, 0:1, 2 * B : 3 * B], (8, B))
            ids = jnp.where(lane // 32 == j, pltpu.roll(row, (32 + 32 * j) % B, 1), ids)
        cols.append(ids[:1].astype(I32))
    ids = jnp.concatenate(cols, axis=1)
    n = iota((gc.shape[1], 2 * B), 0)
    onehot = jnp.where(n == ids, 1.0, 0.0).astype(BF16)
    gh, gl = split(gc[...])
    zero = jnp.zeros((2 * B - CHUNK, 2 * B), BF16)
    hi_out[0:CHUNK, :] = mm(gh, onehot).astype(BF16)
    hi_out[CHUNK : 2 * B, :] = zero
    lo_out[0:CHUNK, :] = mm(gl, onehot).astype(BF16)
    lo_out[CHUNK : 2 * B, :] = zero


def k_first_rows(recv, gc, out, csol, hi_out, lo_out):
    k_rows(recv, out, csol)
    k_picked(recv, gc, hi_out, lo_out)


def k_global(recv, gh, gl, msg, scal):
    total = jnp.sum(recv[...], axis=0)
    first = jnp.concatenate([total[:R], total[:R]], axis=0)
    second = jnp.concatenate([total[R:], total[R:]], axis=0)
    lane = iota((8, B), 1)
    x = jnp.concatenate([first, jnp.where(lane < 64, second, 0.0)], axis=1)
    xh, xl = split(x)
    y = mm(jnp.concatenate([xh, xl], axis=0), gh[...])
    y = y[:8] + y[8:] + mm(xh, gl[...])
    for k in range(NSUB):
        tile, j = k // 4, k % 4
        here = pltpu.roll(y[:, tile * B : (tile + 1) * B], (96 - 32 * j) % B, 1)
        msg[k] = jnp.where(lane < NCL, 0.0, here)[:R]
    scal[...] = jnp.concatenate([second, second], axis=0)


def solution_of(recv, csol):
    total = recv[0]
    for k in range(1, NSUB):
        total = total + recv[k]
    sol = total + csol[...]
    sol = jnp.concatenate([sol, sol], axis=0)
    return jnp.concatenate([sol, sol], axis=0)


def write_sends(v, idx, up, down, even, odd):
    def moved(b):
        return jnp.take_along_axis(v[:, b * B : (b + 1) * B], idx[b], axis=1)

    up[...] = moved(0)
    down[...] = moved(1)
    across = moved(2)
    for h in range(2):
        even[R * h : R * h + R, :] = across[8 * h : 8 * h + 4]
        odd[R * h : R * h + R, :] = across[8 * h + 4 : 8 * h + 8]


def received(from_next, from_prev, odd_in, even_in):
    across = jnp.concatenate(
        [odd_in[0:R, :], even_in[0:R, :], odd_in[R : 2 * R, :], even_in[R : 2 * R, :]], axis=0
    )
    return jnp.concatenate([from_next[...], from_prev[...], across], axis=1)


def k_first_direction(recv, csol, w, v, idx, d_out, up, down, even, odd):
    d = v[...] - spread_back(solution_of(recv, csol), w[...])
    d_out[...] = d
    write_sends(d, idx, up, down, even, odd)


def image_of(d, pi, sg, ops):
    spread = sg * (d + pi)
    low = spread.astype(BF16)
    image = jnp.zeros((ROWS, D), F32)
    row = iota((ROWS, D), 0) // R
    for s in range(S):
        image = jnp.where(row == s, mm(low, ops[s]), image)
    return sg * image, row_dot(spread, image)


def k_image(d, fn, fp, oi, ei, sg, ops, idx, signed_out, curv, up, down, even, odd):
    signed, c = image_of(d[...], received(fn, fp, oi, ei), sg[...], ops)
    signed_out[...] = signed
    curv[...] = jnp.broadcast_to(c[:8], (8, B))
    write_sends(signed, idx, up, down, even, odd)


def k_product(ids, signed, fn, fp, oi, ei, v, w, cc, curv, ap_out, msg):
    ap = signed[...] + received(fn, fp, oi, ei)
    ap_out[...] = ap
    scalars = [curv[...][:, :1], row_dot(v[...], ap)[:8], row_dot(ap, ap)[:8]]
    write_message(msg, coefs(ap, w[...]), cc, ids, scalars)


def scalar_at(scal, j):
    return jnp.sum(jnp.where(iota((ROWS, B), 1) == 64 + j, scal, 0.0), axis=1, keepdims=True)


def k_next_direction(recv, csol, scal0, scal1, w, d, ap, v, idx, r_out, x_out, d_out, up, down, even, odd):
    rho = scalar_at(scal0[...], 0)
    s1 = scal1[...]
    step = rho / scalar_at(s1, 0)
    rho_new = rho - 2.0 * step * scalar_at(s1, 1) + step * step * scalar_at(s1, 2)
    ap_ = ap[...]
    d0 = d[...]
    r_out[...] = v[...] - step * ap_
    x_out[...] = step * d0
    projected = d0 - step * (ap_ - spread_back(solution_of(recv, csol), w[...]))
    d1 = projected + (rho_new / rho) * d0
    d_out[...] = d1
    write_sends(d1, idx, up, down, even, odd)


def k_last_image(d, r, fn, fp, oi, ei, sg, ops, idx, signed_out, msg, up, down, even, odd):
    signed, c = image_of(d[...], received(fn, fp, oi, ei), sg[...], ops)
    rho = row_dot(r[...], r[...])
    signed_out[...] = signed
    lane = iota((8, B), 1)
    row = iota((8, B), 0)
    both = jnp.where(lane == row, c[:8], jnp.where(lane == row + R, rho[:8], 0.0))
    line = jnp.sum(jnp.where(row < R, both, 0.0), axis=0, keepdims=True)
    msg[...] = jnp.broadcast_to(line[None], msg.shape)
    write_sends(signed, idx, up, down, even, odd)


def k_total(recv, out):
    out[...] = jnp.broadcast_to(jnp.sum(recv[...], axis=0, keepdims=True), out.shape)


def k_finish(recv, signed, fn, fp, oi, ei, x, r, d, x_out, r_out):
    line = jnp.broadcast_to(jnp.sum(recv[...], axis=0), (ROWS, B))
    lane = iota((ROWS, B), 1)
    row = iota((ROWS, B), 0) % R
    curv = jnp.sum(jnp.where(lane == row, line, 0.0), axis=1, keepdims=True)
    rho = jnp.sum(jnp.where(lane == row + R, line, 0.0), axis=1, keepdims=True)
    step = rho / curv
    xn = x[...] + step * d[...]
    rn = r[...] - step * (signed[...] + received(fn, fp, oi, ei))
    for s in range(S):
        x_out[s] = xn[R * s : R * s + R]
        r_out[s] = rn[R * s : R * s + R]


def call(body, outs, *args, smem=()):
    specs = [
        pl.BlockSpec(memory_space=pltpu.SMEM if i in smem else pltpu.VMEM) for i in range(len(args))
    ]
    out_shape = tuple(jax.ShapeDtypeStruct(s, t) for s, t in outs)
    return pl.pallas_call(
        body,
        out_shape=out_shape,
        in_specs=specs,
        out_specs=tuple(pl.BlockSpec(memory_space=pltpu.VMEM) for _ in outs),
        name=body.__name__,
        compiler_params=pltpu.CompilerParams(vmem_limit_bytes=VMEM_LIMIT),
    )(*args)


def to_owner(x, axis):
    return lax.all_to_all(x, axis, 0, 0, tiled=True)


FIELD = ((ROWS, D), F32)
SENDS = (((ROWS, B), F32), ((ROWS, B), F32), ((2 * R, B), F32), ((2 * R, B), F32))


def exchange(up, down, even, odd, n_sub, n_cl):
    def ahead(n):
        return [(i, i + 1) for i in range(n - 1)]

    def back(n):
        return [(i + 1, i) for i in range(n - 1)]

    odd_in = lax.ppermute(odd, "cluster", back(n_cl))
    even_in = lax.ppermute(even, "cluster", ahead(n_cl))
    from_prev = lax.ppermute(up, "sub", ahead(n_sub))
    from_next = lax.ppermute(down, "sub", back(n_sub))
    return from_next, from_prev, odd_in, even_in


def local(rhs, operators, signs, links, cb, kb, ids, cluster_coarse, gc):
    n_sub = lax.axis_size("sub")
    n_cl = lax.axis_size("cluster")
    cc = cluster_coarse.reshape(NCL, NSUB * NCL)
    message = ((NSUB, R, D), F32)
    spread_rows = (((n_cl, 8, B), F32), ((R, B), F32))
    picked = ((2 * B, 2 * B), BF16)
    answer = (((NSUB, R, B), F32), ((ROWS, B), F32))

    msg, w, v, sg, idx = call(
        k_start,
        (message, ((NB, D), F32), FIELD, FIELD, ((3, ROWS, B), I32)),
        ids, rhs, cb, kb, cc, signs, links, smem=(0,),
    )
    recv = to_owner(msg, "sub")
    rows, csol, gh, gl = call(k_first_rows, (*spread_rows, picked, picked), recv, gc)
    back, scal0 = call(k_global, answer, to_owner(rows, "cluster"), gh, gl)
    d, *sends = call(
        k_first_direction, (FIELD, *SENDS), to_owner(back, "sub"), csol, w, v, idx
    )
    got = exchange(*sends, n_sub, n_cl)
    signed, curv, *sends = call(
        k_image, (FIELD, ((8, B), F32), *SENDS), d, *got, sg, operators, idx
    )
    got = exchange(*sends, n_sub, n_cl)
    ap, msg = call(k_product, (FIELD, message), ids, signed, *got, v, w, cc, curv, smem=(0,))
    rows, csol = call(k_rows, spread_rows, to_owner(msg, "sub"))
    back, scal1 = call(k_global, answer, to_owner(rows, "cluster"), gh, gl)
    r, x, d1, *sends = call(
        k_next_direction,
        (FIELD, FIELD, FIELD, *SENDS),
        to_owner(back, "sub"), csol, scal0, scal1, w, d, ap, v, idx,
    )
    got = exchange(*sends, n_sub, n_cl)
    signed, msg, *sends = call(
        k_last_image, (FIELD, ((NSUB, 1, B), F32), *SENDS), d1, r, *got, sg, operators, idx
    )
    got = exchange(*sends, n_sub, n_cl)
    (line,) = call(k_total, (((n_cl, 1, B), F32),), to_owner(msg, "sub"))
    out = ((S, R, D), F32)
    return call(k_finish, (out, out), to_owner(line, "cluster"), signed, *got, x, r, d1)


def solution(mesh):
    both = ("cluster", "sub")
    in_specs = (
        P(both, None, None),
        P(both, None, None),
        P(both, None),
        P(both, None, None),
        P(both, None, None),
        P(both, None, None),
        P(both, None),
        P("cluster", "sub", None),
        P("sub", None),
    )
    out_specs = (P(both, None, None), P(both, None, None))
    return jax.shard_map(local, mesh=mesh, in_specs=in_specs, out_specs=out_specs, check_vma=False)
```

```python
import jax
import jax.numpy as jnp
from jax import lax
from jax.experimental import pallas as pl
from jax.experimental.pallas import tpu as pltpu
from jax.sharding import PartitionSpec as P

F32 = jnp.float32
BF16 = jnp.bfloat16
I32 = jnp.int32
R = 4
S = 4
ROWS = R * S
B = 128
D = 384
KC = 24
NB = 128
NCL = S * KC
CHUNK = 192
NSUB = 8
VMEM_LIMIT = 16 * 2**20


def iota(shape, dim):
    return lax.broadcasted_iota(I32, shape, dim)


def split(x):
    hi = x.astype(BF16)
    return hi, (x - hi.astype(F32)).astype(BF16)


def mm(a, b):
    return lax.dot_general(a, b, (((1,), (0,)), ((), ())), preferred_element_type=F32)


def mm_t(a, b):
    return lax.dot_general(a, b, (((1,), (1,)), ((), ())), preferred_element_type=F32)


def dot2(x, w, f=mm):
    n = x.shape[0]
    xh, xl = split(x)
    wh, wl = split(w)
    xs = jnp.concatenate([xh, xl], axis=0)
    both = f(xs, wh)
    return both[:n] + both[n:] + f(xh, wl)


def lanes_of_sub(shape):
    lane = iota(shape, 1)
    return jnp.where(lane < NCL, lane // KC, (lane - NCL) // 8)


def own_mask():
    return iota((ROWS, NB), 0) // R == lanes_of_sub((ROWS, NB))


def by_load(x):
    y = x[:8] + x[8:]
    y = y + pltpu.roll(y, 4, 0)
    return jnp.concatenate([y, y], axis=0)


def coefs(v, w):
    return by_load(jnp.where(own_mask(), dot2(v, w, mm_t), 0.0))


def spread_back(sol, w):
    return dot2(jnp.where(own_mask(), sol, 0.0), w)


def ids_row(ids):
    lane = iota((8, NB), 1)
    row = jnp.full((8, NB), -1, I32)
    for s in range(S):
        for c in range(8):
            row = jnp.where(lane == NCL + 8 * s + c, ids[s, c], row)
    return row


def to_column(row):
    full = jnp.broadcast_to(row[:1], (NB, NB))
    eye = iota((NB, NB), 0) == iota((NB, NB), 1)
    return jnp.sum(jnp.where(eye, full, 0.0), axis=1, keepdims=True)


def window(x, at, width):
    lane = iota((x.shape[0], B), 1)
    tile, off = at // B, at % B
    here = x[:, tile * B : (tile + 1) * B]
    if off:
        here = pltpu.roll(here, B - off, 1)
        if off + width > B:
            after = pltpu.roll(x[:, (tile + 1) * B : (tile + 2) * B], B - off, 1)
            here = jnp.where(lane < B - off, here, after)
    return here


MSG = 5 * B


def write_message(msg, coef, cc, ids, scalars, across_ids=None):
    row = ids_row(ids).astype(F32)
    col = to_column(row).astype(I32)
    c4 = coef[:8]
    hi, lo = split(c4)
    low = (c4 - hi.astype(F32) - lo.astype(F32)).astype(BF16)
    parts = jnp.concatenate([hi, lo, low], axis=0)
    ccp = dot2(jnp.where(iota((8, NB), 1) < NCL, c4, 0.0)[:, :NCL], cc[...])
    lane = iota((8, B), 1)
    extra = jnp.zeros((8, B), F32)
    for j, val in enumerate(scalars):
        extra = jnp.where(lane == 64 + j, val, extra)
    if across_ids is None:
        tail = jnp.zeros((8, B), F32)
    else:
        tail = jnp.where(iota((8, B), 0) == 0, row, across_ids)
    none = jnp.zeros((8, B), F32)
    cluster = [jnp.where(lane < NCL, window(ccp, NCL * k, NCL), 0.0) for k in range(NSUB)]
    for k in range(NSUB):
        n = iota((NB, 2 * B), 1)
        onehot = jnp.where((col == n + CHUNK * k) & (n < CHUNK), 1.0, 0.0).astype(BF16)
        y = mm(parts, onehot)
        y = y[:8] + y[8:16] + y[16:24]
        tiles = (
            y[:, :B],
            y[:, B:] + extra,
            jnp.where(lane < NCL, cluster[k], tail),
            cluster[k + 1] if k + 1 < NSUB else none,
            cluster[k - 1] if k > 0 else none,
        )
        for t, x in enumerate(tiles):
            msg[k, :, t * B : (t + 1) * B] = x[:R]


def row_dot(a, b):
    return by_load(jnp.sum(a * b, axis=1, keepdims=True))


STATIC = NB + ROWS
PACK = 80


def k_send_static(
    ids, rhs, cb, kb, signs, links, up, down, even, odd, w_out, v_out, sg_out, idx_out
):
    pos = iota((8, B), 1).astype(BF16)
    moves = []
    for s in range(S):
        for b in range(3):
            q = links[b, s : s + 1, :]
            if b == 0 or (b == 2 and s % 2 == 0):
                hot = jnp.where(iota((B, B), 0) == q, 1.0, 0.0).astype(BF16)
                q = mm_t(pos, hot)[:1].astype(I32)
            idx_out[b, R * s : R * s + R, :] = jnp.broadcast_to(q, (R, B))
            moves.append(q)
    for s in range(S):
        v_out[R * s : R * s + R, :] = rhs[s]
        sg_out[R * s : R * s + R, :] = jnp.broadcast_to(signs[s : s + 1, :].astype(F32), (R, D))
        w_out[KC * s : KC * s + KC, :] = cb[s]
        w_out[NCL + 8 * s : NCL + 8 * s + 8, :] = kb[s]

    def moved(x, s, b):
        q = jnp.broadcast_to(moves[3 * s + b], (x.shape[0], B))
        return jnp.take_along_axis(x[:, b * B : (b + 1) * B], q, axis=1)

    for s in range(S):
        h = s // 2
        side = odd if s % 2 else even
        for x, at, to in ((cb[s], KC * s, KC * h), (kb[s], NCL + 8 * s, 2 * KC + 8 * h)):
            n = x.shape[0]
            up[at : at + n, :] = moved(x, s, 0)
            down[at : at + n, :] = moved(x, s, 1)
            side[to : to + n, :] = moved(x, s, 2)
    write_moved(v_out[...], idx_out, up, down, even, odd, NB, 2 * KC + 16)
    row = ids_row(ids).astype(F32)
    even[72:80, :] = row
    odd[72:80, :] = row


def write_moved(v, idx, up, down, even, odd, at=0, pack_at=0):
    def moved(b):
        return jnp.take_along_axis(v[:, b * B : (b + 1) * B], idx[b], axis=1)

    up[at : at + ROWS, :] = moved(0)
    down[at : at + ROWS, :] = moved(1)
    across = moved(2)
    for h in range(2):
        even[pack_at + R * h : pack_at + R * h + R, :] = across[8 * h : 8 * h + 4]
        odd[pack_at + R * h : pack_at + R * h + R, :] = across[8 * h + 4 : 8 * h + 8]


def k_start(ids, from_next, from_prev, odd_in, even_in, w, v, cc, msg, pw_out, pv_out):
    pw_out[:, 0:B] = from_next[0:NB, :]
    pw_out[:, B : 2 * B] = from_prev[0:NB, :]
    for s in range(S):
        h = s // 2
        side = even_in if s % 2 else odd_in
        pw_out[KC * s : KC * s + KC, 2 * B :] = side[KC * h : KC * h + KC, :]
        at = 2 * KC + 8 * h
        pw_out[NCL + 8 * s : NCL + 8 * s + 8, 2 * B :] = side[at : at + 8, :]
        at = 2 * KC + 16 + R * h
        pv_out[R * s : R * s + R, 2 * B :] = side[at : at + R, :]
    pv_out[:, 0:B] = from_next[NB:STATIC, :]
    pv_out[:, B : 2 * B] = from_prev[NB:STATIC, :]
    lane_even = (iota((8, B), 1) - NCL) // 8 % 2 == 0
    after = pltpu.roll(odd_in[72:80, :], B - 8, 1)
    before = pltpu.roll(even_in[72:80, :], 8, 1)
    x = v[...]
    coef = coefs(x, w[...])
    across_ids = jnp.where(lane_even, after, before)
    write_message(msg, coef, cc, ids, [row_dot(x, x)[:8]], across_ids)


def k_rows(recv, out, csol):
    total = recv[0]
    for k in range(1, NSUB):
        total = total + recv[k]
    own = jnp.where(iota((R, B), 1) < NCL, total[:, 2 * B : 3 * B], 0.0)
    csol[0] = own
    csol[1] = total[:, 3 * B : 4 * B]
    csol[2] = total[:, 4 * B : 5 * B]
    x = jnp.concatenate([total[:, : 2 * B], own], axis=1)
    out[...] = jnp.broadcast_to(x[None], out.shape)


def k_picked(recv, gc, hi_out, lo_out):
    lane = iota((8, B), 1)
    cols = []
    for kind in range(2):
        for half in range(2):
            ids = jnp.zeros((8, B), F32)
            for j in range(4):
                row = recv[4 * half + j, kind : kind + 1, 2 * B : 3 * B]
                row = pltpu.roll(jnp.broadcast_to(row, (8, B)), (32 + 32 * j) % B, 1)
                ids = jnp.where(lane // 32 == j, row, ids)
            cols.append(ids[:1].astype(I32))
    ids = jnp.concatenate(cols, axis=1)
    n = iota((gc.shape[1], 4 * B), 0)
    onehot = jnp.where(n == ids, 1.0, 0.0).astype(BF16)
    gh, gl = split(gc[...])
    zero = jnp.zeros((2 * B - CHUNK, 4 * B), BF16)
    hi_out[0:CHUNK, :] = mm(gh, onehot).astype(BF16)
    hi_out[CHUNK : 2 * B, :] = zero
    lo_out[0:CHUNK, :] = mm(gl, onehot).astype(BF16)
    lo_out[CHUNK : 2 * B, :] = zero


def k_first_rows(recv, gc, out, csol, hi_out, lo_out):
    k_rows(recv, out, csol)
    k_picked(recv, gc, hi_out, lo_out)


def k_global(recv, gh, gl, msg, scal, cacross):
    n_cl = recv.shape[0]
    c = lax.axis_index("cluster")
    total = jnp.sum(recv[:, :, 0 : 2 * B], axis=0)
    total = jnp.concatenate([total, total], axis=0)
    second = total[:, B:]
    lane = iota((8, B), 1)
    x = jnp.concatenate([total[:, :B], jnp.where(lane < 64, second, 0.0)], axis=1)
    xh, xl = split(x)
    y = mm(jnp.concatenate([xh, xl], axis=0), gh[...])
    y = y[:8] + y[8:] + mm(xh, gl[...])

    def pick(kind, k, to):
        at = 8 * 32 * kind + 32 * k
        return pltpu.roll(y[:, at // B * B : at // B * B + B], (to - at) % B, 1)

    none = jnp.zeros((8, B), F32)
    for k in range(NSUB):
        after = pick(0, k + 1, 32) if k + 1 < NSUB else none
        before = pick(0, k - 1, 64) if k > 0 else none
        here = jnp.where(lane < 32, pick(0, k, 0), jnp.where(lane < 64, after, before))
        msg[k] = jnp.where(lane < 96, here, pick(1, k, 96))[:R]
    scal[...] = jnp.concatenate([second, second], axis=0)
    after = recv[jnp.minimum(c + 1, n_cl - 1), :, 2 * B :]
    before = recv[jnp.maximum(c - 1, 0), :, 2 * B :]
    after = pltpu.roll(jnp.concatenate([after, after], axis=0), B - KC, 1)
    before = pltpu.roll(jnp.concatenate([before, before], axis=0), KC, 1)
    both = jnp.where(lane // KC % 2 == 0, after, before)
    cacross[...] = jnp.where(lane < NCL, both, 0.0)[:R]


def four_times(x):
    x = jnp.concatenate([x, x], axis=0)
    return jnp.concatenate([x, x], axis=0)


def corrections(recv, csol, cacross, w, pw):
    total = recv[0]
    for k in range(1, NSUB):
        total = total + recv[k]
    picks = four_times(total)
    tail = iota((ROWS, B), 1) >= NCL

    def sol(cluster, turn):
        p = pltpu.roll(picks, turn, 1) if turn else picks
        return jnp.where(tail, p, four_times(cluster))

    own = spread_back(sol(csol[0], 96), w[...])
    sides = (sol(csol[1], 64), sol(csol[2], 32), sol(cacross[...], 0))
    pi = [spread_back(x, pw[:, b * B : (b + 1) * B]) for b, x in enumerate(sides)]
    return own, jnp.concatenate(pi, axis=1)


def received(from_next, from_prev, odd_in, even_in):
    across = jnp.concatenate(
        [odd_in[0:R, :], even_in[0:R, :], odd_in[R : 2 * R, :], even_in[R : 2 * R, :]], axis=0
    )
    return jnp.concatenate([from_next[...], from_prev[...], across], axis=1)


def paired(n_cl):
    c, k = lax.axis_index("cluster"), lax.axis_index("sub")
    lane = iota((ROWS, D), 1)
    is_even = iota((ROWS, D), 0) // R % 2 == 0
    yes = [
        jnp.where(x, 1.0, 0.0) for x in (k < NSUB - 1, k > 0, c < n_cl - 1, c > 0)
    ]
    across = jnp.where(is_even, yes[2], yes[3])
    return jnp.where(lane < B, yes[0], jnp.where(lane < 2 * B, yes[1], across))


def image_of(d, pd, sg, ops):
    spread = sg * (d + pd)
    low = spread.astype(BF16)
    image = jnp.zeros((ROWS, D), F32)
    row = iota((ROWS, D), 0) // R
    for s in range(S):
        image = jnp.where(row == s, mm(low, ops[s]), image)
    return sg * image, row_dot(spread, image)


def k_first_image(
    recv, csol, cacross, w, pw, v, pv, sg, ops, idx,
    d_out, pd_out, signed_out, curv, up, down, even, odd,
):
    fix, pfix = corrections(recv, csol, cacross, w, pw)
    d = v[...] - fix
    pd = pv[...] - pfix
    d_out[...] = d
    pd_out[...] = pd
    signed, c = image_of(d, pd, sg[...], ops)
    signed_out[...] = signed
    curv[...] = jnp.broadcast_to(c[:8], (8, B))
    write_moved(signed, idx, up, down, even, odd)


def make_product(n_cl):
    def k_product(ids, signed, fn, fp, oi, ei, v, w, cc, curv, ap_out, pap_out, msg):
        pi = received(fn, fp, oi, ei)
        u = signed[...]
        ap = u + pi
        ap_out[...] = ap
        pap_out[...] = pi + paired(n_cl) * u
        scalars = [curv[...][:, :1], row_dot(v[...], ap)[:8], row_dot(ap, ap)[:8]]
        write_message(msg, coefs(ap, w[...]), cc, ids, scalars)

    return k_product


def scalar_at(scal, j):
    return jnp.sum(jnp.where(iota((ROWS, B), 1) == 64 + j, scal, 0.0), axis=1, keepdims=True)


LAST = ROWS + 8


def k_last_image(
    recv, csol, cacross, scal0, scal1, w, pw, v, d, pd, ap, pap, sg, ops, idx,
    r_out, x_out, d_out, signed_out, msg, even, odd, up, down,
):
    fix, pfix = corrections(recv, csol, cacross, w, pw)
    rho = scalar_at(scal0[...], 0)
    s1 = scal1[...]
    step = rho / scalar_at(s1, 0)
    rho_new = rho - 2.0 * step * scalar_at(s1, 1) + step * step * scalar_at(s1, 2)
    beta = rho_new / rho
    ap_ = ap[...]
    d0 = d[...]
    pd0 = pd[...]
    r = v[...] - step * ap_
    r_out[...] = r
    x_out[...] = step * d0
    d1 = d0 - step * (ap_ - fix) + beta * d0
    pd1 = pd0 - step * (pap[...] - pfix) + beta * pd0
    d_out[...] = d1
    signed, c = image_of(d1, pd1, sg[...], ops)
    signed_out[...] = signed
    sq = row_dot(r, r)
    lane = iota((8, B), 1)
    row = iota((8, B), 0)
    both = jnp.where(lane == row, c[:8], jnp.where(lane == row + R, sq[:8], 0.0))
    both = jnp.where(row < R, both, 0.0)
    write_moved(signed, idx, up, down, even, odd)
    msg[...] = jnp.zeros(msg.shape, F32)
    for k in range(NSUB):
        msg[k, ROWS:LAST, :] = both
    k = lax.axis_index("sub")
    msg[jnp.minimum(k + 1, NSUB - 1), 0:ROWS, :] = up[...]
    msg[jnp.maximum(k - 1, 0), 0:ROWS, :] = down[...]


def k_total(recv, out, from_next, from_prev):
    total = recv[0, ROWS:LAST, :]
    for j in range(1, NSUB):
        total = total + recv[j, ROWS:LAST, :]
    line = jnp.sum(total, axis=0, keepdims=True)
    out[...] = jnp.broadcast_to(line[None], out.shape)
    k = lax.axis_index("sub")
    after = recv[jnp.minimum(k + 1, NSUB - 1), 0:ROWS, :]
    before = recv[jnp.maximum(k - 1, 0), 0:ROWS, :]
    from_next[...] = jnp.where(jnp.full((ROWS, B), k, I32) < NSUB - 1, after, 0.0)
    from_prev[...] = jnp.where(jnp.full((ROWS, B), k, I32) > 0, before, 0.0)


def k_finish(recv, signed, fn, fp, oi, ei, x, r, d, x_out, r_out):
    line = jnp.broadcast_to(jnp.sum(recv[...], axis=0), (ROWS, B))
    lane = iota((ROWS, B), 1)
    row = iota((ROWS, B), 0) % R
    curv = jnp.sum(jnp.where(lane == row, line, 0.0), axis=1, keepdims=True)
    rho = jnp.sum(jnp.where(lane == row + R, line, 0.0), axis=1, keepdims=True)
    step = rho / curv
    xn = x[...] + step * d[...]
    rn = r[...] - step * (signed[...] + received(fn, fp, oi, ei))
    for s in range(S):
        x_out[s] = xn[R * s : R * s + R]
        r_out[s] = rn[R * s : R * s + R]


def call(body, outs, *args, smem=(), scratch=()):
    def space(i):
        return pltpu.SMEM if i in smem else pltpu.VMEM

    specs = [pl.BlockSpec(memory_space=space(i)) for i in range(len(args))]
    out_shape = tuple(jax.ShapeDtypeStruct(s, t) for s, t in outs)
    return pl.pallas_call(
        body,
        out_shape=out_shape,
        in_specs=specs,
        out_specs=tuple(pl.BlockSpec(memory_space=pltpu.VMEM) for _ in outs),
        scratch_shapes=scratch,
        name=body.__name__,
        compiler_params=pltpu.CompilerParams(vmem_limit_bytes=VMEM_LIMIT),
    )(*args)


def to_owner(x, axis):
    return lax.all_to_all(x, axis, 0, 0, tiled=True)


def f32(*shape):
    return (shape, F32)


FIELD = f32(ROWS, D)


def sends(rows, pack):
    return (f32(rows, B), f32(rows, B), f32(pack, B), f32(pack, B))


def ahead(n):
    return [(i, i + 1) for i in range(n - 1)]


def back(n):
    return [(i + 1, i) for i in range(n - 1)]


def exchange_across(even, odd, n_cl):
    odd_in = lax.ppermute(odd, "cluster", back(n_cl))
    even_in = lax.ppermute(even, "cluster", ahead(n_cl))
    return odd_in, even_in


def exchange(up, down, even, odd, n_sub, n_cl):
    across = exchange_across(even, odd, n_cl)
    from_prev = lax.ppermute(up, "sub", ahead(n_sub))
    from_next = lax.ppermute(down, "sub", back(n_sub))
    return from_next, from_prev, *across


def local(rhs, operators, signs, links, cb, kb, ids, cluster_coarse, gc):
    n_sub = lax.axis_size("sub")
    n_cl = lax.axis_size("cluster")
    cc = cluster_coarse.reshape(NCL, NSUB * NCL)
    message = f32(NSUB, R, MSG)
    spread_rows = (f32(n_cl, R, D), f32(3, R, B))
    picked = ((2 * B, 4 * B), BF16)
    answer = (f32(NSUB, R, B), f32(ROWS, B), f32(R, B))

    *out, w, v, sg, idx = call(
        k_send_static,
        (*sends(STATIC, PACK), f32(NB, D), FIELD, FIELD, ((3, ROWS, B), I32)),
        ids, rhs, cb, kb, signs, links.transpose(1, 0, 2),
        smem=(0,),
    )
    got = exchange(*out, n_sub, n_cl)
    msg, pw, pv = call(
        k_start, (message, f32(NB, D), FIELD), ids, *got, w, v, cc, smem=(0,)
    )
    rows, csol, gh, gl = call(
        k_first_rows, (*spread_rows, picked, picked), to_owner(msg, "sub"), gc
    )
    to_all, scal0, cacross = call(
        k_global, answer, to_owner(rows, "cluster"), gh, gl
    )
    d, pd, signed, curv, *out = call(
        k_first_image,
        (FIELD, FIELD, FIELD, f32(8, B), *sends(ROWS, 2 * R)),
        to_owner(to_all, "sub"), csol, cacross, w, pw, v, pv, sg, operators, idx,
    )
    got = exchange(*out, n_sub, n_cl)
    ap, pap, msg = call(
        make_product(n_cl),
        (FIELD, FIELD, message),
        ids, signed, *got, v, w, cc, curv, smem=(0,),
    )
    rows, csol = call(k_rows, spread_rows, to_owner(msg, "sub"))
    to_all, scal1, cacross = call(
        k_global, answer, to_owner(rows, "cluster"), gh, gl
    )
    r, x, d1, signed, msg, even, odd = call(
        k_last_image,
        (FIELD, FIELD, FIELD, FIELD, f32(NSUB, LAST, B), f32(2 * R, B), f32(2 * R, B)),
        to_owner(to_all, "sub"), csol, cacross, scal0, scal1,
        w, pw, v, d, pd, ap, pap, sg, operators, idx,
        scratch=(pltpu.VMEM((ROWS, B), F32), pltpu.VMEM((ROWS, B), F32)),
    )
    line, from_next, from_prev = call(
        k_total, (f32(n_cl, 1, B), f32(ROWS, B), f32(ROWS, B)), to_owner(msg, "sub")
    )
    across = exchange_across(even, odd, n_cl)
    out = f32(S, R, D)
    return call(
        k_finish, (out, out), to_owner(line, "cluster"), signed, from_next, from_prev, *across, x, r, d1
    )


def solution(mesh):
    both = ("cluster", "sub")
    in_specs = (
        P(both, None, None),
        P(both, None, None),
        P(both, None),
        P(both, None, None),
        P(both, None, None),
        P(both, None, None),
        P(both, None),
        P("cluster", "sub", None),
        P("sub", None),
    )
    out_specs = (P(both, None, None), P(both, None, None))
    return jax.shard_map(local, mesh=mesh, in_specs=in_specs, out_specs=out_specs, check_vma=False)
```

```python
import jax
import jax.numpy as jnp
from jax import lax
from jax.experimental import pallas as pl
from jax.experimental.pallas import tpu as pltpu
from jax.sharding import Mesh
from jax.sharding import PartitionSpec as P

F32 = jnp.float32
BF16 = jnp.bfloat16
I32 = jnp.int32
R = 4
S = 4
ROWS = R * S
B = 128
D = 384
KC = 24
NB = 128
NCL = S * KC
CHUNK = 192
NSUB = 8
CLUSTER = ("y", "z")
VMEM_LIMIT = 16 * 2**20


def iota(shape, dim):
    return lax.broadcasted_iota(I32, shape, dim)


def split(x):
    hi = x.astype(BF16)
    return hi, (x - hi.astype(F32)).astype(BF16)


def mm(a, b):
    return lax.dot_general(a, b, (((1,), (0,)), ((), ())), preferred_element_type=F32)


def mm_t(a, b):
    return lax.dot_general(a, b, (((1,), (1,)), ((), ())), preferred_element_type=F32)


def dot2(x, w, f=mm):
    n = x.shape[0]
    xh, xl = split(x)
    wh, wl = split(w)
    xs = jnp.concatenate([xh, xl], axis=0)
    both = f(xs, wh)
    return both[:n] + both[n:] + f(xh, wl)


def lanes_of_sub(shape):
    lane = iota(shape, 1)
    return jnp.where(lane < NCL, lane // KC, (lane - NCL) // 8)


def own_mask():
    return iota((ROWS, NB), 0) // R == lanes_of_sub((ROWS, NB))


def by_load(x):
    y = x[:8] + x[8:]
    y = y + pltpu.roll(y, 4, 0)
    return jnp.concatenate([y, y], axis=0)


def coefs(v, w):
    return by_load(jnp.where(own_mask(), dot2(v, w, mm_t), 0.0))


def spread_back(sol, w):
    return dot2(jnp.where(own_mask(), sol, 0.0), w)


def ids_row(ids):
    lane = iota((8, NB), 1)
    row = jnp.full((8, NB), -1, I32)
    for s in range(S):
        for c in range(8):
            row = jnp.where(lane == NCL + 8 * s + c, ids[s, c], row)
    return row


def to_column(row):
    full = jnp.broadcast_to(row[:1], (NB, NB))
    eye = iota((NB, NB), 0) == iota((NB, NB), 1)
    return jnp.sum(jnp.where(eye, full, 0.0), axis=1, keepdims=True)


def window(x, at, width):
    lane = iota((x.shape[0], B), 1)
    tile, off = at // B, at % B
    here = x[:, tile * B : (tile + 1) * B]
    if off:
        here = pltpu.roll(here, B - off, 1)
        if off + width > B:
            after = pltpu.roll(x[:, (tile + 1) * B : (tile + 2) * B], B - off, 1)
            here = jnp.where(lane < B - off, here, after)
    return here


MSG = 5 * B


def write_message(msg, coef, cc, ids, scalars):
    row = ids_row(ids).astype(F32)
    col = to_column(row).astype(I32)
    c4 = coef[:8]
    hi, lo = split(c4)
    low = (c4 - hi.astype(F32) - lo.astype(F32)).astype(BF16)
    parts = jnp.concatenate([hi, lo, low], axis=0)
    ccp = dot2(jnp.where(iota((8, NB), 1) < NCL, c4, 0.0)[:, :NCL], cc[...])
    lane = iota((8, B), 1)
    extra = jnp.zeros((8, B), F32)
    for j, val in enumerate(scalars):
        extra = jnp.where(lane == 64 + j, val, extra)
    none = jnp.zeros((8, B), F32)
    cluster = [jnp.where(lane < NCL, window(ccp, NCL * k, NCL), 0.0) for k in range(NSUB)]
    for k in range(NSUB):
        n = iota((NB, 2 * B), 1)
        onehot = jnp.where((col == n + CHUNK * k) & (n < CHUNK), 1.0, 0.0).astype(BF16)
        y = mm(parts, onehot)
        y = y[:8] + y[8:16] + y[16:24]
        tiles = (
            y[:, :B],
            y[:, B:] + extra,
            jnp.where(lane < NCL, cluster[k], row),
            cluster[k + 1] if k + 1 < NSUB else none,
            cluster[k - 1] if k > 0 else none,
        )
        for t, x in enumerate(tiles):
            msg[k, :, t * B : (t + 1) * B] = x[:R]


def row_dot(a, b):
    return by_load(jnp.sum(a * b, axis=1, keepdims=True))


STATIC = NB + ROWS
PACK = 72


def k_coefs(ids, rhs, cb, kb, cc, msg, w_out, v_out):
    for s in range(S):
        v_out[R * s : R * s + R, :] = rhs[s]
        w_out[KC * s : KC * s + KC, :] = cb[s]
        w_out[NCL + 8 * s : NCL + 8 * s + 8, :] = kb[s]
    v = v_out[...]
    write_message(msg, coefs(v, w_out[...]), cc, ids, [row_dot(v, v)[:8]])


def k_send_static(after, w, v, signs, links, up, down, even, odd, sg_out, idx_out):
    del after
    pos = iota((8, B), 1).astype(BF16)
    moves = []
    for s in range(S):
        sg_out[R * s : R * s + R, :] = jnp.broadcast_to(signs[s : s + 1, :].astype(F32), (R, D))
        for b in range(3):
            q = links[b, s : s + 1, :]
            if b == 0 or (b == 2 and s % 2 == 0):
                hot = jnp.where(iota((B, B), 0) == q, 1.0, 0.0).astype(BF16)
                q = mm_t(pos, hot)[:1].astype(I32)
            idx_out[b, R * s : R * s + R, :] = jnp.broadcast_to(q, (R, B))
            moves.append(q)

    def moved(at, n, s, b):
        q = jnp.broadcast_to(moves[3 * s + b], (n, B))
        return jnp.take_along_axis(w[at : at + n, b * B : (b + 1) * B], q, axis=1)

    for s in range(S):
        h = s // 2
        side = odd if s % 2 else even
        for at, n, to in ((KC * s, KC, KC * h), (NCL + 8 * s, 8, 2 * KC + 8 * h)):
            up[at : at + n, :] = moved(at, n, s, 0)
            down[at : at + n, :] = moved(at, n, s, 1)
            side[to : to + n, :] = moved(at, n, s, 2)
    write_moved(v[...], idx_out, up, down, even, odd, NB, 2 * KC + 16)


def write_moved(v, idx, up, down, even, odd, at=0, pack_at=0):
    def moved(b):
        return jnp.take_along_axis(v[:, b * B : (b + 1) * B], idx[b], axis=1)

    up[at : at + ROWS, :] = moved(0)
    down[at : at + ROWS, :] = moved(1)
    across = moved(2)
    for h in range(2):
        even[pack_at + R * h : pack_at + R * h + R, :] = across[8 * h : 8 * h + 4]
        odd[pack_at + R * h : pack_at + R * h + R, :] = across[8 * h + 4 : 8 * h + 8]


def k_take_static(from_next, from_prev, odd_in, even_in, pw_out, pv_out):
    pw_out[:, 0:B] = from_next[0:NB, :]
    pw_out[:, B : 2 * B] = from_prev[0:NB, :]
    for s in range(S):
        h = s // 2
        side = even_in if s % 2 else odd_in
        pw_out[KC * s : KC * s + KC, 2 * B :] = side[KC * h : KC * h + KC, :]
        at = 2 * KC + 8 * h
        pw_out[NCL + 8 * s : NCL + 8 * s + 8, 2 * B :] = side[at : at + 8, :]
        at = 2 * KC + 16 + R * h
        pv_out[R * s : R * s + R, 2 * B :] = side[at : at + R, :]
    pv_out[:, 0:B] = from_next[NB:STATIC, :]
    pv_out[:, B : 2 * B] = from_prev[NB:STATIC, :]


def member_sum(recv):
    total = recv[0]
    for k in range(1, NSUB):
        total = total + recv[k]
    return total


def k_rows(recv, out, csol):
    total = member_sum(recv)
    own = jnp.where(iota((R, B), 1) < NCL, total[:, 2 * B : 3 * B], 0.0)
    csol[0] = own
    csol[1] = total[:, 3 * B : 4 * B]
    csol[2] = total[:, 4 * B : 5 * B]
    x = jnp.concatenate([total[:, : 2 * B], own], axis=1)
    out[:, :, 0:D] = jnp.broadcast_to(x[None], (out.shape[0], R, D))


def cluster_ids(recv):
    lane = iota((8, B), 1)
    rows = []
    for half in range(2):
        ids = jnp.zeros((8, B), F32)
        for j in range(4):
            row = recv[4 * half + j, 0:1, 2 * B : 3 * B]
            row = pltpu.roll(jnp.broadcast_to(row, (8, B)), (32 + 32 * j) % B, 1)
            ids = jnp.where(lane // 32 == j, row, ids)
        rows.append(ids)
    return rows


def k_first_rows(recv, out, csol, ids_out):
    k_rows(recv, out, csol)
    low, high = cluster_ids(recv)
    ids = jnp.where(iota((8, B), 0) == 0, low, high)
    ids_out[...] = ids
    out[:, :, D:] = jnp.broadcast_to(ids[None, :R], (out.shape[0], R, B))


def k_pass(recv, out):
    y, z = lax.axis_index("y"), lax.axis_index("z")
    n_y, n_z = recv.shape[0], out.shape[0]
    total = jnp.sum(recv[:, :, 0 : 2 * B], axis=0)
    other = jnp.where(z == 0, jnp.minimum(y + 1, n_y - 1), jnp.maximum(y - 1, 0))
    x = jnp.concatenate([total, recv[y, :, 2 * B :], recv[other, :, 2 * B :]], axis=1)
    out[...] = jnp.broadcast_to(x[None], (n_z, *x.shape))


def neighbours(recv, at, wrapped_at):
    z = lax.axis_index("z")
    n_z = recv.shape[0]
    last, first = z == n_z - 1, z == 0
    nxt = recv[jnp.where(last, 0, z + 1)]
    prv = recv[jnp.where(first, n_z - 1, z - 1)]

    def tile(x, use_wrapped):
        plain = x[:, at : at + B]
        wrapped = x[:, wrapped_at : wrapped_at + B]
        x = jnp.where(jnp.full((R, B), use_wrapped.astype(I32), I32) == 1, wrapped, plain)
        return jnp.concatenate([x, x], axis=0)

    return tile(nxt, last), tile(prv, first)


def picked_columns(gc, rows, hi_out, lo_out):
    ids = jnp.concatenate([x[:1].astype(I32) for x in rows], axis=1)
    n = iota((gc.shape[1], ids.shape[1]), 0)
    onehot = jnp.where(n == ids, 1.0, 0.0).astype(BF16)
    gh, gl = split(gc[...])
    zero = jnp.zeros((2 * B - CHUNK, ids.shape[1]), BF16)
    hi_out[0:CHUNK, :] = mm(gh, onehot).astype(BF16)
    hi_out[CHUNK : 2 * B, :] = zero
    lo_out[0:CHUNK, :] = mm(gl, onehot).astype(BF16)
    lo_out[CHUNK : 2 * B, :] = zero


def k_own_columns(ids, gc, hi_out, lo_out):
    picked_columns(gc, [ids[0:1, :], ids[1:2, :]], hi_out, lo_out)


def solve(recv, parts, msg, scal, cacross, stride):
    total = jnp.sum(recv[:, :, 0 : 2 * B], axis=0)
    total = jnp.concatenate([total, total], axis=0)
    second = total[:, B:]
    lane = iota((8, B), 1)
    x = jnp.concatenate([total[:, :B], jnp.where(lane < 64, second, 0.0)], axis=1)
    xh, xl = split(x)
    ys = []
    for gh, gl in parts:
        y = mm(jnp.concatenate([xh, xl], axis=0), gh[...])
        ys.append(y[:8] + y[8:] + mm(xh, gl[...]))

    def pick(kind, k, to):
        at = 32 * k
        return pltpu.roll(ys[kind][:, at // B * B : at // B * B + B], (to - at) % B, 1)

    none = jnp.zeros((8, B), F32)
    for k in range(NSUB):
        after = pick(0, k + 1, 32) if k + 1 < NSUB else none
        before = pick(0, k - 1, 64) if k > 0 else none
        here = jnp.where(lane < 32, pick(0, k, 0), jnp.where(lane < 64, after, before))
        msg[k] = jnp.where(lane < 96, here, pick(1, k, 96))[:R]
    scal[...] = jnp.concatenate([second, second], axis=0)
    after, before = neighbours(recv, 2 * B, 2 * B + stride)
    after = pltpu.roll(after, B - KC, 1)
    before = pltpu.roll(before, KC, 1)
    both = jnp.where(lane // KC % 2 == 0, after, before)
    cacross[...] = jnp.where(lane < NCL, both, 0.0)[:R]


def k_first_global(recv, gc, gh, gl, msg, scal, cacross, ah, al):
    after, before = neighbours(recv, 3 * B, 5 * B)
    lane = iota((8, B), 1)
    after = pltpu.roll(after, B - 8, 1)
    before = pltpu.roll(before, 8, 1)
    ids = jnp.where(lane // 8 % 2 == 0, after, before)
    picked_columns(gc, [ids[0:1], ids[1:2]], ah, al)
    solve(recv, ((gh, gl), (ah, al)), msg, scal, cacross, 2 * B)


def k_global(recv, gh, gl, ah, al, msg, scal, cacross):
    solve(recv, ((gh, gl), (ah, al)), msg, scal, cacross, B)


def four_times(x):
    x = jnp.concatenate([x, x], axis=0)
    return jnp.concatenate([x, x], axis=0)


def corrections(recv, csol, cacross, w, pw):
    picks = four_times(member_sum(recv))
    tail = iota((ROWS, B), 1) >= NCL

    def sol(cluster, turn):
        p = pltpu.roll(picks, turn, 1) if turn else picks
        return jnp.where(tail, p, four_times(cluster))

    own = spread_back(sol(csol[0], 96), w[...])
    sides = (sol(csol[1], 64), sol(csol[2], 32), sol(cacross[...], 0))
    pi = [spread_back(x, pw[:, b * B : (b + 1) * B]) for b, x in enumerate(sides)]
    return own, jnp.concatenate(pi, axis=1)


def received(from_next, from_prev, odd_in, even_in):
    across = jnp.concatenate(
        [odd_in[0:R, :], even_in[0:R, :], odd_in[R : 2 * R, :], even_in[R : 2 * R, :]], axis=0
    )
    return jnp.concatenate([from_next[...], from_prev[...], across], axis=1)


def paired(n_cl):
    c, k = lax.axis_index("y") * lax.axis_size("z") + lax.axis_index("z"), lax.axis_index("sub")
    lane = iota((ROWS, D), 1)
    is_even = iota((ROWS, D), 0) // R % 2 == 0
    yes = [
        jnp.where(x, 1.0, 0.0) for x in (k < NSUB - 1, k > 0, c < n_cl - 1, c > 0)
    ]
    across = jnp.where(is_even, yes[2], yes[3])
    return jnp.where(lane < B, yes[0], jnp.where(lane < 2 * B, yes[1], across))


def image_of(d, pd, sg, ops):
    spread = sg * (d + pd)
    low = spread.astype(BF16)
    image = jnp.zeros((ROWS, D), F32)
    row = iota((ROWS, D), 0) // R
    for s in range(S):
        image = jnp.where(row == s, mm(low, ops[s]), image)
    return sg * image, row_dot(spread, image)


def k_first_image(
    recv, csol, cacross, w, pw, v, pv, sg, ops, idx,
    d_out, pd_out, signed_out, curv, up, down, even, odd,
):
    fix, pfix = corrections(recv, csol, cacross, w, pw)
    d = v[...] - fix
    pd = pv[...] - pfix
    d_out[...] = d
    pd_out[...] = pd
    signed, c = image_of(d, pd, sg[...], ops)
    signed_out[...] = signed
    curv[...] = jnp.broadcast_to(c[:8], (8, B))
    write_moved(signed, idx, up, down, even, odd)


def make_product(n_cl):
    def k_product(ids, signed, fn, fp, oi, ei, v, w, cc, curv, ap_out, pap_out, msg):
        pi = received(fn, fp, oi, ei)
        u = signed[...]
        ap = u + pi
        ap_out[...] = ap
        pap_out[...] = pi + paired(n_cl) * u
        scalars = [curv[...][:, :1], row_dot(v[...], ap)[:8], row_dot(ap, ap)[:8]]
        write_message(msg, coefs(ap, w[...]), cc, ids, scalars)

    return k_product


def scalar_at(scal, j):
    return jnp.sum(jnp.where(iota((ROWS, B), 1) == 64 + j, scal, 0.0), axis=1, keepdims=True)


LAST = ROWS + 8


def k_last_image(
    recv, csol, cacross, scal0, scal1, w, pw, v, d, pd, ap, pap, sg, ops, idx,
    r_out, x_out, d_out, signed_out, msg, even, odd, up, down,
):
    fix, pfix = corrections(recv, csol, cacross, w, pw)
    rho = scalar_at(scal0[...], 0)
    s1 = scal1[...]
    step = rho / scalar_at(s1, 0)
    rho_new = rho - 2.0 * step * scalar_at(s1, 1) + step * step * scalar_at(s1, 2)
    beta = rho_new / rho
    ap_ = ap[...]
    d0 = d[...]
    pd0 = pd[...]
    r = v[...] - step * ap_
    r_out[...] = r
    x_out[...] = step * d0
    d1 = d0 - step * (ap_ - fix) + beta * d0
    pd1 = pd0 - step * (pap[...] - pfix) + beta * pd0
    d_out[...] = d1
    signed, c = image_of(d1, pd1, sg[...], ops)
    signed_out[...] = signed
    sq = row_dot(r, r)
    lane = iota((8, B), 1)
    row = iota((8, B), 0)
    both = jnp.where(lane == row, c[:8], jnp.where(lane == row + R, sq[:8], 0.0))
    both = jnp.where(row < R, both, 0.0)
    write_moved(signed, idx, up, down, even, odd)
    msg[...] = jnp.zeros(msg.shape, F32)
    for k in range(NSUB):
        msg[k, ROWS:LAST, :] = both
    k = lax.axis_index("sub")
    msg[jnp.minimum(k + 1, NSUB - 1), 0:ROWS, :] = up[...]
    msg[jnp.maximum(k - 1, 0), 0:ROWS, :] = down[...]


def k_total(recv, out, from_next, from_prev):
    total = recv[0, ROWS:LAST, :]
    for j in range(1, NSUB):
        total = total + recv[j, ROWS:LAST, :]
    line = jnp.sum(total, axis=0, keepdims=True)
    out[...] = jnp.broadcast_to(line[None], out.shape)
    k = lax.axis_index("sub")
    after = recv[jnp.minimum(k + 1, NSUB - 1), 0:ROWS, :]
    before = recv[jnp.maximum(k - 1, 0), 0:ROWS, :]
    from_next[...] = jnp.where(jnp.full((ROWS, B), k, I32) < NSUB - 1, after, 0.0)
    from_prev[...] = jnp.where(jnp.full((ROWS, B), k, I32) > 0, before, 0.0)


def k_finish(recv, signed, fn, fp, oi, ei, x, r, d, x_out, r_out):
    line = jnp.broadcast_to(jnp.sum(recv[...], axis=0), (ROWS, B))
    lane = iota((ROWS, B), 1)
    row = iota((ROWS, B), 0) % R
    curv = jnp.sum(jnp.where(lane == row, line, 0.0), axis=1, keepdims=True)
    rho = jnp.sum(jnp.where(lane == row + R, line, 0.0), axis=1, keepdims=True)
    step = rho / curv
    xn = x[...] + step * d[...]
    rn = r[...] - step * (signed[...] + received(fn, fp, oi, ei))
    for s in range(S):
        x_out[s] = xn[R * s : R * s + R]
        r_out[s] = rn[R * s : R * s + R]


def call(body, outs, *args, smem=(), scratch=()):
    def space(i):
        return pltpu.SMEM if i in smem else pltpu.VMEM

    specs = [pl.BlockSpec(memory_space=space(i)) for i in range(len(args))]
    out_shape = tuple(jax.ShapeDtypeStruct(s, t) for s, t in outs)
    return pl.pallas_call(
        body,
        out_shape=out_shape,
        in_specs=specs,
        out_specs=tuple(pl.BlockSpec(memory_space=pltpu.VMEM) for _ in outs),
        scratch_shapes=scratch,
        name=body.__name__,
        compiler_params=pltpu.CompilerParams(vmem_limit_bytes=VMEM_LIMIT),
    )(*args)


def to_owner(x, axis):
    return lax.all_to_all(x, axis, 0, 0, tiled=True)


def f32(*shape):
    return (shape, F32)


FIELD = f32(ROWS, D)


def sends(rows, pack):
    return (f32(rows, B), f32(rows, B), f32(pack, B), f32(pack, B))


def ahead(n):
    return [(i, i + 1) for i in range(n - 1)]


def back(n):
    return [(i + 1, i) for i in range(n - 1)]


def exchange_across(even, odd, n_cl):
    odd_in = lax.ppermute(odd, CLUSTER, back(n_cl))
    even_in = lax.ppermute(even, CLUSTER, ahead(n_cl))
    return odd_in, even_in


def exchange(up, down, even, odd, n_sub, n_cl):
    across = exchange_across(even, odd, n_cl)
    from_prev = lax.ppermute(up, "sub", ahead(n_sub))
    from_next = lax.ppermute(down, "sub", back(n_sub))
    return from_next, from_prev, *across


def local(rhs, operators, signs, links, cb, kb, ids, cluster_coarse, gc):
    n_sub = lax.axis_size("sub")
    n_y = lax.axis_size("y")
    n_z = lax.axis_size("z")
    n_cl = n_y * n_z
    cc = cluster_coarse.reshape(NCL, NSUB * NCL)
    message = f32(NSUB, R, MSG)
    picked = ((2 * B, 2 * B), BF16)
    answer = (f32(NSUB, R, B), f32(ROWS, B), f32(R, B))

    msg, w, v = call(
        k_coefs, (message, f32(NB, D), FIELD), ids, rhs, cb, kb, cc, smem=(0,)
    )
    recv = to_owner(msg, "sub")
    rows, csol, all_ids = call(
        k_first_rows, (f32(n_y, R, 4 * B), f32(3, R, B), f32(8, B)), recv
    )
    *out, sg, idx = call(
        k_send_static,
        (*sends(STATIC, PACK), FIELD, ((3, ROWS, B), I32)),
        all_ids, w, v, signs, links.transpose(1, 0, 2),
    )
    got = exchange(*out, n_sub, n_cl)
    pw, pv = call(k_take_static, (f32(NB, D), FIELD), *got)
    gh, gl = call(k_own_columns, (picked, picked), all_ids, gc)
    (rows,) = call(k_pass, (f32(n_z, R, 6 * B),), to_owner(rows, "y"))
    to_all, scal0, cacross, ah, al = call(
        k_first_global, (*answer, picked, picked), to_owner(rows, "z"), gc, gh, gl
    )
    d, pd, signed, curv, *out = call(
        k_first_image,
        (FIELD, FIELD, FIELD, f32(8, B), *sends(ROWS, 2 * R)),
        to_owner(to_all, "sub"), csol, cacross, w, pw, v, pv, sg, operators, idx,
    )
    got = exchange(*out, n_sub, n_cl)
    ap, pap, msg = call(
        make_product(n_cl),
        (FIELD, FIELD, message),
        ids, signed, *got, v, w, cc, curv, smem=(0,),
    )
    rows, csol = call(k_rows, (f32(n_y, R, D), f32(3, R, B)), to_owner(msg, "sub"))
    (rows,) = call(k_pass, (f32(n_z, R, 4 * B),), to_owner(rows, "y"))
    to_all, scal1, cacross = call(k_global, answer, to_owner(rows, "z"), gh, gl, ah, al)
    r, x, d1, signed, msg, even, odd = call(
        k_last_image,
        (FIELD, FIELD, FIELD, FIELD, f32(NSUB, LAST, B), f32(2 * R, B), f32(2 * R, B)),
        to_owner(to_all, "sub"), csol, cacross, scal0, scal1,
        w, pw, v, d, pd, ap, pap, sg, operators, idx,
        scratch=(pltpu.VMEM((ROWS, B), F32), pltpu.VMEM((ROWS, B), F32)),
    )
    line, from_next, from_prev = call(
        k_total, (f32(n_cl, 1, B), f32(ROWS, B), f32(ROWS, B)), to_owner(msg, "sub")
    )
    across = exchange_across(even, odd, n_cl)
    out = f32(S, R, D)
    return call(
        k_finish, (out, out), to_owner(line, CLUSTER), signed, from_next, from_prev, *across, x, r, d1
    )


def solution(mesh):
    n_y, n_z = 8, 12
    torus = Mesh(mesh.devices.reshape(n_y, n_z, NSUB), ("y", "z", "sub"))
    both = ("y", "z", "sub")
    in_specs = (
        P(both, None, None),
        P(both, None, None),
        P(both, None),
        P(both, None, None),
        P(both, None, None),
        P(both, None, None),
        P(both, None),
        P(CLUSTER, "sub", None),
        P("sub", None),
    )
    out_specs = (P(both, None, None), P(both, None, None))
    return jax.shard_map(local, mesh=torus, in_specs=in_specs, out_specs=out_specs, check_vma=False)
```

```python
import jax
import jax.numpy as jnp
from jax import lax
from jax.experimental import pallas as pl
from jax.experimental.pallas import tpu as pltpu
from jax.sharding import Mesh
from jax.sharding import PartitionSpec as P

F32 = jnp.float32
BF16 = jnp.bfloat16
I32 = jnp.int32
R = 4
S = 4
ROWS = R * S
B = 128
D = 384
KC = 24
NB = 128
NCL = S * KC
CHUNK = 192
NSUB = 8
CLUSTER = ("y", "z")
VMEM_LIMIT = 16 * 2**20


def iota(shape, dim):
    return lax.broadcasted_iota(I32, shape, dim)


def pick(flag, a, b):
    return jnp.where(jnp.full(a.shape, flag.astype(I32), I32) == 1, a, b)


def even_member():
    return lax.axis_index("sub") % 2 == 0


def even_cluster():
    return (lax.axis_index("y") * lax.axis_size("z") + lax.axis_index("z")) % 2 == 0


def split(x):
    hi = x.astype(BF16)
    return hi, (x - hi.astype(F32)).astype(BF16)


def mm(a, b):
    return lax.dot_general(a, b, (((1,), (0,)), ((), ())), preferred_element_type=F32)


def mm_t(a, b):
    return lax.dot_general(a, b, (((1,), (1,)), ((), ())), preferred_element_type=F32)


def dot2(x, w, f=mm):
    n = x.shape[0]
    xh, xl = split(x)
    wh, wl = split(w)
    xs = jnp.concatenate([xh, xl], axis=0)
    both = f(xs, wh)
    return both[:n] + both[n:] + f(xh, wl)


def lanes_of_sub(shape):
    lane = iota(shape, 1)
    return jnp.where(lane < NCL, lane // KC, (lane - NCL) // 8)


def own_mask():
    return iota((ROWS, NB), 0) // R == lanes_of_sub((ROWS, NB))


def by_load(x):
    y = x[:8] + x[8:]
    y = y + pltpu.roll(y, 4, 0)
    return jnp.concatenate([y, y], axis=0)


def coefs(v, w):
    return by_load(jnp.where(own_mask(), dot2(v, w, mm_t), 0.0))


def spread_back(sol, w):
    return dot2(jnp.where(own_mask(), sol, 0.0), w)


def ids_row(ids):
    lane = iota((8, NB), 1)
    row = jnp.full((8, NB), -1, I32)
    for s in range(S):
        for c in range(8):
            row = jnp.where(lane == NCL + 8 * s + c, ids[s, c], row)
    return row


def to_column(row):
    full = jnp.broadcast_to(row[:1], (NB, NB))
    eye = iota((NB, NB), 0) == iota((NB, NB), 1)
    return jnp.sum(jnp.where(eye, full, 0.0), axis=1, keepdims=True)


def window(x, at, width):
    lane = iota((x.shape[0], B), 1)
    tile, off = at // B, at % B
    here = x[:, tile * B : (tile + 1) * B]
    if off:
        here = pltpu.roll(here, B - off, 1)
        if off + width > B:
            after = pltpu.roll(x[:, (tile + 1) * B : (tile + 2) * B], B - off, 1)
            here = jnp.where(lane < B - off, here, after)
    return here


MSG = 5 * B


def write_message(msg, coef, cc, ids, scalars):
    row = ids_row(ids).astype(F32)
    col = to_column(row).astype(I32)
    c4 = coef[:8]
    hi, lo = split(c4)
    low = (c4 - hi.astype(F32) - lo.astype(F32)).astype(BF16)
    parts = jnp.concatenate([hi, lo, low], axis=0)
    ccp = dot2(jnp.where(iota((8, NB), 1) < NCL, c4, 0.0)[:, :NCL], cc[...])
    lane = iota((8, B), 1)
    extra = jnp.zeros((8, B), F32)
    for j, val in enumerate(scalars):
        extra = jnp.where(lane == 64 + j, val, extra)
    none = jnp.zeros((8, B), F32)
    cluster = [jnp.where(lane < NCL, window(ccp, NCL * k, NCL), 0.0) for k in range(NSUB)]
    for k in range(NSUB):
        n = iota((NB, 2 * B), 1)
        onehot = jnp.where((col == n + CHUNK * k) & (n < CHUNK), 1.0, 0.0).astype(BF16)
        y = mm(parts, onehot)
        y = y[:8] + y[8:16] + y[16:24]
        tiles = (
            y[:, :B],
            y[:, B:] + extra,
            jnp.where(lane < NCL, cluster[k], row),
            cluster[k + 1] if k + 1 < NSUB else none,
            cluster[k - 1] if k > 0 else none,
        )
        for t, x in enumerate(tiles):
            msg[k, :, t * B : (t + 1) * B] = x[:R]


def row_dot(a, b):
    return by_load(jnp.sum(a * b, axis=1, keepdims=True))


STATIC = NB + ROWS
PACK = 72


def k_coefs(ids, rhs, w, cc, msg, v_out):
    for s in range(S):
        v_out[R * s : R * s + R, :] = rhs[s]
    v = v_out[...]
    write_message(msg, coefs(v, w[...]), cc, ids, [row_dot(v, v)[:8]])


def k_tables(after, signs, links, sg_out, idx_out):
    del after
    pos = iota((8, B), 1).astype(BF16)
    for s in range(S):
        sg_out[R * s : R * s + R, :] = jnp.broadcast_to(signs[s : s + 1, :].astype(F32), (R, D))
        for b in range(3):
            q = links[b, s : s + 1, :]
            if b == 0 or (b == 2 and s % 2 == 0):
                hot = jnp.where(iota((B, B), 0) == q, 1.0, 0.0).astype(BF16)
                q = mm_t(pos, hot)[:1].astype(I32)
            idx_out[b, R * s : R * s + R, :] = jnp.broadcast_to(q, (R, B))


def static_blocks(w, v, idx, b):
    lanes = pl.ds(pl.multiple_of(b * B, B), B)

    def moved(x, q):
        return jnp.take_along_axis(x, jnp.broadcast_to(q, x.shape), axis=1)

    for s in range(S):
        q = idx[b, R * s : R * s + 1, :]
        for at, n in ((KC * s, KC), (NCL + 8 * s, 8)):
            yield s, at, moved(w[at : at + n, lanes], q)
    yield None, NB, moved(v[:, lanes], idx[b])


def send_within(w, v, idx, out, b):
    for _, at, x in static_blocks(w, v, idx, b):
        out[at : at + x.shape[0], :] = x


def k_send_first(after, signs, links, w, v, sg_out, idx_out, out):
    k_tables(after, signs, links, sg_out, idx_out)
    send_within(w, v, idx_out, out, lax.axis_index("sub") % 2)


def k_send_second(after, w, v, idx, out):
    del after
    send_within(w, v, idx, out, 1 - lax.axis_index("sub") % 2)


def k_send_across(after, w, v, idx, first, second):
    del after
    flag = even_cluster()
    blocks = {(s, at): x for s, at, x in static_blocks(w, v, idx, 2)}

    def put(to, even, odd):
        n = even.shape[0]
        first[to : to + n, :] = pick(flag, even, odd)
        second[to : to + n, :] = pick(flag, odd, even)

    for h in range(2):
        s = 2 * h
        put(KC * h, blocks[s, KC * s], blocks[s + 1, KC * (s + 1)])
        put(2 * KC + 8 * h, blocks[s, NCL + 8 * s], blocks[s + 1, NCL + 8 * s + 8])
        x = blocks[None, NB][8 * h : 8 * h + 8]
        put(2 * KC + 16 + R * h, x[:R], x[R:])


def moved_blocks(v, idx):
    up, down, across = (
        jnp.take_along_axis(v[:, b * B : (b + 1) * B], idx[b], axis=1) for b in range(3)
    )
    even = jnp.concatenate([across[0:R], across[8 : 8 + R]], axis=0)
    odd = jnp.concatenate([across[R:8], across[8 + R :]], axis=0)
    return up, down, even, odd


def write_across(even, odd, first, second):
    flag = even_cluster()
    first[...] = pick(flag, even, odd)
    second[...] = pick(flag, odd, even)


def write_moved(v, idx, in1, in2, out1, out2):
    up, down, even, odd = moved_blocks(v, idx)
    flag = even_member()
    in1[...] = pick(flag, up, down)
    in2[...] = pick(flag, down, up)
    write_across(even, odd, out1, out2)


def across_of(out1, out2):
    flag = even_cluster()
    return pick(flag, out1, out2), pick(flag, out2, out1)


def within_of(in1, in2):
    flag = even_member()
    return pick(flag, in1, in2), pick(flag, in2, in1)


def take_static(in1, in2, out1, out2, pw_out, pv_out):
    from_next, from_prev = within_of(in1[...], in2[...])
    odd_in, even_in = across_of(out1[...], out2[...])
    pw_out[:, 0:B] = from_next[0:NB, :]
    pw_out[:, B : 2 * B] = from_prev[0:NB, :]
    for s in range(S):
        h = s // 2
        side = even_in if s % 2 else odd_in
        pw_out[KC * s : KC * s + KC, 2 * B :] = side[KC * h : KC * h + KC, :]
        at = 2 * KC + 8 * h
        pw_out[NCL + 8 * s : NCL + 8 * s + 8, 2 * B :] = side[at : at + 8, :]
        at = 2 * KC + 16 + R * h
        pv_out[R * s : R * s + R, 2 * B :] = side[at : at + R, :]
    pv_out[:, 0:B] = from_next[NB:STATIC, :]
    pv_out[:, B : 2 * B] = from_prev[NB:STATIC, :]


def member_sum(recv):
    total = recv[0]
    for k in range(1, NSUB):
        total = total + recv[k]
    return total


def k_rows(recv, out, csol):
    total = member_sum(recv)
    own = jnp.where(iota((R, B), 1) < NCL, total[:, 2 * B : 3 * B], 0.0)
    csol[0] = own
    csol[1] = total[:, 3 * B : 4 * B]
    csol[2] = total[:, 4 * B : 5 * B]
    x = jnp.concatenate([total[:, : 2 * B], own], axis=1)
    out[:, :, 0:D] = jnp.broadcast_to(x[None], (out.shape[0], R, D))


def cluster_ids(recv):
    lane = iota((8, B), 1)
    rows = []
    for half in range(2):
        ids = jnp.zeros((8, B), F32)
        for j in range(4):
            row = recv[4 * half + j, 0:1, 2 * B : 3 * B]
            row = pltpu.roll(jnp.broadcast_to(row, (8, B)), (32 + 32 * j) % B, 1)
            ids = jnp.where(lane // 32 == j, row, ids)
        rows.append(ids)
    return rows


def k_first_rows(recv, out, csol, ids_out):
    k_rows(recv, out, csol)
    low, high = cluster_ids(recv)
    ids = jnp.where(iota((8, B), 0) == 0, low, high)
    ids_out[...] = ids
    out[:, :, D:] = jnp.broadcast_to(ids[None, :R], (out.shape[0], R, B))


def k_pass(recv, out):
    y, z = lax.axis_index("y"), lax.axis_index("z")
    n_y, n_z = recv.shape[0], out.shape[0]
    total = jnp.sum(recv[:, :, 0 : 2 * B], axis=0)
    other = jnp.where(z == 0, jnp.minimum(y + 1, n_y - 1), jnp.maximum(y - 1, 0))
    x = jnp.concatenate([total, recv[y, :, 2 * B :], recv[other, :, 2 * B :]], axis=1)
    out[...] = jnp.broadcast_to(x[None], (n_z, *x.shape))


def k_first_pass(recv, after, out):
    del after
    k_pass(recv, out)


def neighbours(recv, at, wrapped_at):
    z = lax.axis_index("z")
    n_z = recv.shape[0]
    last, first = z == n_z - 1, z == 0
    nxt = recv[jnp.where(last, 0, z + 1)]
    prv = recv[jnp.where(first, n_z - 1, z - 1)]

    def tile(x, use_wrapped):
        plain = x[:, at : at + B]
        wrapped = x[:, wrapped_at : wrapped_at + B]
        x = jnp.where(jnp.full((R, B), use_wrapped.astype(I32), I32) == 1, wrapped, plain)
        return jnp.concatenate([x, x], axis=0)

    return tile(nxt, last), tile(prv, first)


def picked_columns(gc, rows, hi_out, lo_out):
    ids = jnp.concatenate([x[:1].astype(I32) for x in rows], axis=1)
    n = iota((gc.shape[1], ids.shape[1]), 0)
    onehot = jnp.where(n == ids, 1.0, 0.0).astype(BF16)
    gh, gl = split(gc[...])
    zero = jnp.zeros((2 * B - CHUNK, ids.shape[1]), BF16)
    hi_out[0:CHUNK, :] = mm(gh, onehot).astype(BF16)
    hi_out[CHUNK : 2 * B, :] = zero
    lo_out[0:CHUNK, :] = mm(gl, onehot).astype(BF16)
    lo_out[CHUNK : 2 * B, :] = zero


def k_own_columns(ids, gc, hi_out, lo_out):
    picked_columns(gc, [ids[0:1, :], ids[1:2, :]], hi_out, lo_out)


def solve(recv, parts, msg, scal, cacross, stride):
    total = jnp.sum(recv[:, :, 0 : 2 * B], axis=0)
    total = jnp.concatenate([total, total], axis=0)
    second = total[:, B:]
    lane = iota((8, B), 1)
    x = jnp.concatenate([total[:, :B], jnp.where(lane < 64, second, 0.0)], axis=1)
    xh, xl = split(x)
    ys = []
    for gh, gl in parts:
        y = mm(jnp.concatenate([xh, xl], axis=0), gh[...])
        ys.append(y[:8] + y[8:] + mm(xh, gl[...]))

    def pick(kind, k, to):
        at = 32 * k
        return pltpu.roll(ys[kind][:, at // B * B : at // B * B + B], (to - at) % B, 1)

    none = jnp.zeros((8, B), F32)
    for k in range(NSUB):
        after = pick(0, k + 1, 32) if k + 1 < NSUB else none
        before = pick(0, k - 1, 64) if k > 0 else none
        here = jnp.where(lane < 32, pick(0, k, 0), jnp.where(lane < 64, after, before))
        msg[k] = jnp.where(lane < 96, here, pick(1, k, 96))[:R]
    scal[...] = jnp.concatenate([second, second], axis=0)
    after, before = neighbours(recv, 2 * B, 2 * B + stride)
    after = pltpu.roll(after, B - KC, 1)
    before = pltpu.roll(before, KC, 1)
    both = jnp.where(lane // KC % 2 == 0, after, before)
    cacross[...] = jnp.where(lane < NCL, both, 0.0)[:R]


def k_first_global(recv, gc, gh, gl, odd_after, even_after, msg, scal, cacross, ah, al):
    del odd_after, even_after
    after, before = neighbours(recv, 3 * B, 5 * B)
    lane = iota((8, B), 1)
    after = pltpu.roll(after, B - 8, 1)
    before = pltpu.roll(before, 8, 1)
    ids = jnp.where(lane // 8 % 2 == 0, after, before)
    picked_columns(gc, [ids[0:1], ids[1:2]], ah, al)
    solve(recv, ((gh, gl), (ah, al)), msg, scal, cacross, 2 * B)


def k_global(recv, gh, gl, ah, al, msg, scal, cacross):
    solve(recv, ((gh, gl), (ah, al)), msg, scal, cacross, B)


def four_times(x):
    x = jnp.concatenate([x, x], axis=0)
    return jnp.concatenate([x, x], axis=0)


def corrections(recv, csol, cacross, w, pw):
    picks = four_times(member_sum(recv))
    tail = iota((ROWS, B), 1) >= NCL

    def sol(cluster, turn):
        p = pltpu.roll(picks, turn, 1) if turn else picks
        return jnp.where(tail, p, four_times(cluster))

    own = spread_back(sol(csol[0], 96), w[...])
    sides = (sol(csol[1], 64), sol(csol[2], 32), sol(cacross[...], 0))
    pi = [spread_back(x, pw[:, b * B : (b + 1) * B]) for b, x in enumerate(sides)]
    return own, jnp.concatenate(pi, axis=1)


def received(from_next, from_prev, out1, out2):
    odd_in, even_in = across_of(out1[...], out2[...])
    across = jnp.concatenate([odd_in[0:R], even_in[0:R], odd_in[R:], even_in[R:]], axis=0)
    return jnp.concatenate([from_next, from_prev, across], axis=1)


def paired(n_cl):
    c, k = lax.axis_index("y") * lax.axis_size("z") + lax.axis_index("z"), lax.axis_index("sub")
    lane = iota((ROWS, D), 1)
    is_even = iota((ROWS, D), 0) // R % 2 == 0
    yes = [
        jnp.where(x, 1.0, 0.0) for x in (k < NSUB - 1, k > 0, c < n_cl - 1, c > 0)
    ]
    across = jnp.where(is_even, yes[2], yes[3])
    return jnp.where(lane < B, yes[0], jnp.where(lane < 2 * B, yes[1], across))


def image_of(d, pd, sg, ops):
    spread = sg * (d + pd)
    low = spread.astype(BF16)
    image = jnp.zeros((ROWS, D), F32)
    row = iota((ROWS, D), 0) // R
    for s in range(S):
        image = jnp.where(row == s, mm(low, ops[s]), image)
    return sg * image, row_dot(spread, image)


def k_first_image(
    recv, csol, cacross, in1, in2, out1, out2, w, v, sg, ops, idx,
    pw, pv, d_out, pd_out, signed_out, curv, *outs,
):
    take_static(in1, in2, out1, out2, pw, pv)
    fix, pfix = corrections(recv, csol, cacross, w, pw)
    d = v[...] - fix
    pd = pv[...] - pfix
    d_out[...] = d
    pd_out[...] = pd
    signed, c = image_of(d, pd, sg[...], ops)
    signed_out[...] = signed
    curv[...] = jnp.broadcast_to(c[:8], (8, B))
    write_moved(signed, idx, *outs)


def make_product(n_cl):
    def k_product(ids, signed, in1, in2, out1, out2, v, w, cc, curv, ap_out, pap_out, msg):
        pi = received(*within_of(in1[...], in2[...]), out1, out2)
        u = signed[...]
        ap = u + pi
        ap_out[...] = ap
        pap_out[...] = pi + paired(n_cl) * u
        scalars = [curv[...][:, :1], row_dot(v[...], ap)[:8], row_dot(ap, ap)[:8]]
        write_message(msg, coefs(ap, w[...]), cc, ids, scalars)

    return k_product


def scalar_at(scal, j):
    return jnp.sum(jnp.where(iota((ROWS, B), 1) == 64 + j, scal, 0.0), axis=1, keepdims=True)


LAST = ROWS + 8


def k_last_image(
    recv, csol, cacross, scal0, scal1, w, pw, v, d, pd, ap, pap, sg, ops, idx,
    r_out, x_out, d_out, signed_out, msg, out1, out2,
):
    fix, pfix = corrections(recv, csol, cacross, w, pw)
    rho = scalar_at(scal0[...], 0)
    s1 = scal1[...]
    step = rho / scalar_at(s1, 0)
    rho_new = rho - 2.0 * step * scalar_at(s1, 1) + step * step * scalar_at(s1, 2)
    beta = rho_new / rho
    ap_ = ap[...]
    d0 = d[...]
    pd0 = pd[...]
    r = v[...] - step * ap_
    r_out[...] = r
    x_out[...] = step * d0
    d1 = d0 - step * (ap_ - fix) + beta * d0
    pd1 = pd0 - step * (pap[...] - pfix) + beta * pd0
    d_out[...] = d1
    signed, c = image_of(d1, pd1, sg[...], ops)
    signed_out[...] = signed
    sq = row_dot(r, r)
    lane = iota((8, B), 1)
    row = iota((8, B), 0)
    both = jnp.where(lane == row, c[:8], jnp.where(lane == row + R, sq[:8], 0.0))
    both = jnp.where(row < R, both, 0.0)
    up, down, even, odd = moved_blocks(signed, idx)
    write_across(even, odd, out1, out2)
    msg[...] = jnp.zeros(msg.shape, F32)
    for k in range(NSUB):
        msg[k, ROWS:LAST, :] = both
    k = lax.axis_index("sub")
    msg[jnp.minimum(k + 1, NSUB - 1), 0:ROWS, :] = up
    msg[jnp.maximum(k - 1, 0), 0:ROWS, :] = down


def k_total(recv, out, from_next, from_prev):
    total = recv[0, ROWS:LAST, :]
    for j in range(1, NSUB):
        total = total + recv[j, ROWS:LAST, :]
    line = jnp.sum(total, axis=0, keepdims=True)
    out[...] = jnp.broadcast_to(line[None], out.shape)
    k = lax.axis_index("sub")
    after = recv[jnp.minimum(k + 1, NSUB - 1), 0:ROWS, :]
    before = recv[jnp.maximum(k - 1, 0), 0:ROWS, :]
    from_next[...] = jnp.where(jnp.full((ROWS, B), k, I32) < NSUB - 1, after, 0.0)
    from_prev[...] = jnp.where(jnp.full((ROWS, B), k, I32) > 0, before, 0.0)


def k_finish(recv, signed, fn, fp, out1, out2, x, r, d, x_out, r_out):
    line = jnp.broadcast_to(jnp.sum(recv[...], axis=0), (ROWS, B))
    lane = iota((ROWS, B), 1)
    row = iota((ROWS, B), 0) % R
    curv = jnp.sum(jnp.where(lane == row, line, 0.0), axis=1, keepdims=True)
    rho = jnp.sum(jnp.where(lane == row + R, line, 0.0), axis=1, keepdims=True)
    step = rho / curv
    xn = x[...] + step * d[...]
    rn = r[...] - step * (signed[...] + received(fn[...], fp[...], out1, out2))
    for s in range(S):
        x_out[s] = xn[R * s : R * s + R]
        r_out[s] = rn[R * s : R * s + R]


def call(body, outs, *args, smem=(), scratch=()):
    def space(i):
        return pltpu.SMEM if i in smem else pltpu.VMEM

    specs = [pl.BlockSpec(memory_space=space(i)) for i in range(len(args))]
    out_shape = tuple(jax.ShapeDtypeStruct(s, t) for s, t in outs)
    return pl.pallas_call(
        body,
        out_shape=out_shape,
        in_specs=specs,
        out_specs=tuple(pl.BlockSpec(memory_space=pltpu.VMEM) for _ in outs),
        scratch_shapes=scratch,
        name=body.__name__,
        compiler_params=pltpu.CompilerParams(vmem_limit_bytes=VMEM_LIMIT),
    )(*args)


def to_owner(x, axis):
    return lax.all_to_all(x, axis, 0, 0, tiled=True)


def f32(*shape):
    return (shape, F32)


FIELD = f32(ROWS, D)


SENDS = (f32(ROWS, B), f32(ROWS, B), f32(2 * R, B), f32(2 * R, B))


def swap(x, axis, n, first):
    low = range(0 if first else 1, n - 1, 2)
    return lax.ppermute(x, axis, [p for i in low for p in ((i, i + 1), (i + 1, i))])


def exchange_across(first, second, n_cl):
    return swap(first, CLUSTER, n_cl, True), swap(second, CLUSTER, n_cl, False)


def exchange(in1, in2, out1, out2, n_sub, n_cl):
    across = exchange_across(out1, out2, n_cl)
    return swap(in1, "sub", n_sub, True), swap(in2, "sub", n_sub, False), *across


def local(rhs, operators, signs, links, cb, kb, ids, cluster_coarse, gc):
    n_sub = lax.axis_size("sub")
    n_y = lax.axis_size("y")
    n_z = lax.axis_size("z")
    n_cl = n_y * n_z
    cc = cluster_coarse.reshape(NCL, NSUB * NCL)
    message = f32(NSUB, R, MSG)
    picked = ((2 * B, 2 * B), BF16)
    answer = (f32(NSUB, R, B), f32(ROWS, B), f32(R, B))

    w = jnp.concatenate([cb.reshape(NCL, D), kb.reshape(NB - NCL, D)], axis=0)
    msg, v = call(k_coefs, (message, FIELD), ids, rhs, w, cc, smem=(0,))
    recv = to_owner(msg, "sub")
    rows, csol, all_ids = call(
        k_first_rows, (f32(n_y, R, 4 * B), f32(3, R, B), f32(8, B)), recv
    )
    sg, idx, in1 = call(
        k_send_first,
        (FIELD, ((3, ROWS, B), I32), f32(STATIC, B)),
        all_ids, signs, links.transpose(1, 0, 2), w, v,
    )
    in1 = swap(in1, "sub", n_sub, True)
    recv = to_owner(rows, "y")
    (rows,) = call(k_first_pass, (f32(n_z, R, 6 * B),), recv, in1)
    out = call(k_send_across, (f32(PACK, B), f32(PACK, B)), recv, w, v, idx)
    across = exchange_across(*out, n_cl)
    gh, gl = call(k_own_columns, (picked, picked), all_ids, gc)
    to_all, scal0, cacross, ah, al = call(
        k_first_global, (*answer, picked, picked), to_owner(rows, "z"), gc, gh, gl, *across
    )
    (in2,) = call(k_send_second, (f32(STATIC, B),), to_all, w, v, idx)
    in2 = swap(in2, "sub", n_sub, False)
    pw, pv, d, pd, signed, curv, *out = call(
        k_first_image,
        (f32(NB, D), FIELD, FIELD, FIELD, FIELD, f32(8, B), *SENDS),
        to_owner(to_all, "sub"), csol, cacross, in1, in2, *across,
        w, v, sg, operators, idx,
    )
    got = exchange(*out, n_sub, n_cl)
    ap, pap, msg = call(
        make_product(n_cl),
        (FIELD, FIELD, message),
        ids, signed, *got, v, w, cc, curv, smem=(0,),
    )
    rows, csol = call(k_rows, (f32(n_y, R, D), f32(3, R, B)), to_owner(msg, "sub"))
    (rows,) = call(k_pass, (f32(n_z, R, 4 * B),), to_owner(rows, "y"))
    to_all, scal1, cacross = call(k_global, answer, to_owner(rows, "z"), gh, gl, ah, al)
    r, x, d1, signed, msg, *out = call(
        k_last_image,
        (FIELD, FIELD, FIELD, FIELD, f32(NSUB, LAST, B), f32(2 * R, B), f32(2 * R, B)),
        to_owner(to_all, "sub"), csol, cacross, scal0, scal1,
        w, pw, v, d, pd, ap, pap, sg, operators, idx,
    )
    line, from_next, from_prev = call(
        k_total, (f32(n_cl, 1, B), f32(ROWS, B), f32(ROWS, B)), to_owner(msg, "sub")
    )
    across = exchange_across(*out, n_cl)
    out = f32(S, R, D)
    return call(
        k_finish, (out, out), to_owner(line, CLUSTER), signed, from_next, from_prev, *across, x, r, d1
    )


def solution(mesh):
    n_y, n_z = 8, 12
    torus = Mesh(mesh.devices.reshape(n_y, n_z, NSUB), ("y", "z", "sub"))
    both = ("y", "z", "sub")
    in_specs = (
        P(both, None, None),
        P(both, None, None),
        P(both, None),
        P(both, None, None),
        P(both, None, None),
        P(both, None, None),
        P(both, None),
        P(CLUSTER, "sub", None),
        P("sub", None),
    )
    out_specs = (P(both, None, None), P(both, None, None))
    return jax.shard_map(local, mesh=torus, in_specs=in_specs, out_specs=out_specs, check_vma=False)
```

```python
import jax
import jax.numpy as jnp
from jax import lax
from jax.experimental import pallas as pl
from jax.experimental.pallas import tpu as pltpu
from jax.sharding import Mesh
from jax.sharding import PartitionSpec as P


F32 = jnp.float32
BF16 = jnp.bfloat16
I32 = jnp.int32
R = 4
S = 4
ROWS = R * S
B = 128
D = 384
KC = 24
NB = 128
NCL = S * KC
CHUNK = 192
NSUB = 8
CLUSTER = ("y", "z")
VMEM_LIMIT = 16 * 2**20


def iota(shape, dim):
    return lax.broadcasted_iota(I32, shape, dim)


def pick(flag, a, b):
    return jnp.where(jnp.full(a.shape, flag.astype(I32), I32) == 1, a, b)


def even_member():
    return lax.axis_index("sub") % 2 == 0


def even_cluster():
    return (lax.axis_index("y") * lax.axis_size("z") + lax.axis_index("z")) % 2 == 0


def split(x):
    hi = x.astype(BF16)
    return hi, (x - hi.astype(F32)).astype(BF16)


def mm(a, b):
    return lax.dot_general(a, b, (((1,), (0,)), ((), ())), preferred_element_type=F32)


def mm_t(a, b):
    return lax.dot_general(a, b, (((1,), (1,)), ((), ())), preferred_element_type=F32)


def dot2(x, w, f=mm):
    n = x.shape[0]
    xh, xl = split(x)
    wh, wl = split(w)
    xs = jnp.concatenate([xh, xl], axis=0)
    both = f(xs, wh)
    return both[:n] + both[n:] + f(xh, wl)


def lanes_of_sub(shape):
    lane = iota(shape, 1)
    return jnp.where(lane < NCL, lane // KC, (lane - NCL) // 8)


def own_mask():
    return iota((ROWS, NB), 0) // R == lanes_of_sub((ROWS, NB))


def by_load(x):
    y = x[:8] + x[8:]
    y = y + pltpu.roll(y, 4, 0)
    return jnp.concatenate([y, y], axis=0)


def coefs(v, w):
    return by_load(jnp.where(own_mask(), dot2(v, w, mm_t), 0.0))


def spread_back(sol, w):
    return dot2(jnp.where(own_mask(), sol, 0.0), w)


def ids_row(ids):
    lane = iota((8, NB), 1)
    row = jnp.full((8, NB), -1, I32)
    for s in range(S):
        for c in range(8):
            row = jnp.where(lane == NCL + 8 * s + c, ids[s, c], row)
    return row


def to_column(row):
    full = jnp.broadcast_to(row[:1], (NB, NB))
    eye = iota((NB, NB), 0) == iota((NB, NB), 1)
    return jnp.sum(jnp.where(eye, full, 0.0), axis=1, keepdims=True)


def window(x, at, width):
    lane = iota((x.shape[0], B), 1)
    tile, off = at // B, at % B
    here = x[:, tile * B : (tile + 1) * B]
    if off:
        here = pltpu.roll(here, B - off, 1)
        if off + width > B:
            after = pltpu.roll(x[:, (tile + 1) * B : (tile + 2) * B], B - off, 1)
            here = jnp.where(lane < B - off, here, after)
    return here


MSG = 5 * B


def write_message(msg, coef, cc, ids, scalars):
    row = ids_row(ids).astype(F32)
    col = to_column(row).astype(I32)
    c4 = coef[:8]
    hi, lo = split(c4)
    low = (c4 - hi.astype(F32) - lo.astype(F32)).astype(BF16)
    parts = jnp.concatenate([hi, lo, low], axis=0)
    ccp = dot2(jnp.where(iota((8, NB), 1) < NCL, c4, 0.0)[:, :NCL], cc[...])
    lane = iota((8, B), 1)
    extra = jnp.zeros((8, B), F32)
    for j, val in enumerate(scalars):
        extra = jnp.where(lane == 64 + j, val, extra)
    none = jnp.zeros((8, B), F32)
    cluster = [jnp.where(lane < NCL, window(ccp, NCL * k, NCL), 0.0) for k in range(NSUB)]
    for k in range(NSUB):
        n = iota((NB, 2 * B), 1)
        onehot = jnp.where((col == n + CHUNK * k) & (n < CHUNK), 1.0, 0.0).astype(BF16)
        y = mm(parts, onehot)
        y = y[:8] + y[8:16] + y[16:24]
        tiles = (
            y[:, :B],
            y[:, B:] + extra,
            jnp.where(lane < NCL, cluster[k], row),
            cluster[k + 1] if k + 1 < NSUB else none,
            cluster[k - 1] if k > 0 else none,
        )
        for t, x in enumerate(tiles):
            msg[k, :, t * B : (t + 1) * B] = x[:R]


def row_dot(a, b):
    return by_load(jnp.sum(a * b, axis=1, keepdims=True))


STATIC = NB + ROWS
PACK = 72


def k_coefs(ids, rhs, w, cc, msg, v_out):
    for s in range(S):
        v_out[R * s : R * s + R, :] = rhs[s]
    v = v_out[...]
    write_message(msg, coefs(v, w[...]), cc, ids, [row_dot(v, v)[:8]])


def k_tables(after, signs, links, sg_out, idx_out):
    del after
    pos = iota((8, B), 1).astype(BF16)
    for s in range(S):
        sg_out[R * s : R * s + R, :] = jnp.broadcast_to(signs[s : s + 1, :].astype(F32), (R, D))
        for b in range(3):
            q = links[b, s : s + 1, :]
            if b == 0 or (b == 2 and s % 2 == 0):
                hot = jnp.where(iota((B, B), 0) == q, 1.0, 0.0).astype(BF16)
                q = mm_t(pos, hot)[:1].astype(I32)
            idx_out[b, R * s : R * s + R, :] = jnp.broadcast_to(q, (R, B))


def static_blocks(w, v, idx, b):
    lanes = pl.ds(pl.multiple_of(b * B, B), B)

    def moved(x, q):
        return jnp.take_along_axis(x, jnp.broadcast_to(q, x.shape), axis=1)

    for s in range(S):
        q = idx[b, R * s : R * s + 1, :]
        for at, n in ((KC * s, KC), (NCL + 8 * s, 8)):
            yield s, at, moved(w[at : at + n, lanes], q)
    yield None, NB, moved(v[:, lanes], idx[b])


def send_within(w, v, idx, out, b):
    for _, at, x in static_blocks(w, v, idx, b):
        out[at : at + x.shape[0], :] = x


def k_send_first(after, signs, links, w, v, sg_out, idx_out, out):
    k_tables(after, signs, links, sg_out, idx_out)
    send_within(w, v, idx_out, out, lax.axis_index("sub") % 2)


def k_send_second(after, w, v, idx, out):
    del after
    send_within(w, v, idx, out, 1 - lax.axis_index("sub") % 2)


def k_send_across(after, w, v, idx, first, second):
    del after
    flag = even_cluster()
    blocks = {(s, at): x for s, at, x in static_blocks(w, v, idx, 2)}

    def put(to, even, odd):
        n = even.shape[0]
        first[to : to + n, :] = pick(flag, even, odd)
        second[to : to + n, :] = pick(flag, odd, even)

    for h in range(2):
        s = 2 * h
        put(KC * h, blocks[s, KC * s], blocks[s + 1, KC * (s + 1)])
        put(2 * KC + 8 * h, blocks[s, NCL + 8 * s], blocks[s + 1, NCL + 8 * s + 8])
        x = blocks[None, NB][8 * h : 8 * h + 8]
        put(2 * KC + 16 + R * h, x[:R], x[R:])


def moved_blocks(v, idx):
    up, down, across = (
        jnp.take_along_axis(v[:, b * B : (b + 1) * B], idx[b], axis=1) for b in range(3)
    )
    even = jnp.concatenate([across[0:R], across[8 : 8 + R]], axis=0)
    odd = jnp.concatenate([across[R:8], across[8 + R :]], axis=0)
    return up, down, even, odd


def write_across(even, odd, first, second):
    flag = even_cluster()
    first[...] = pick(flag, even, odd)
    second[...] = pick(flag, odd, even)


def write_moved(v, idx, in1, in2, out1, out2):
    up, down, even, odd = moved_blocks(v, idx)
    flag = even_member()
    in1[...] = pick(flag, up, down)
    in2[...] = pick(flag, down, up)
    write_across(even, odd, out1, out2)


def across_of(out1, out2):
    flag = even_cluster()
    return pick(flag, out1, out2), pick(flag, out2, out1)


def within_of(in1, in2):
    flag = even_member()
    return pick(flag, in1, in2), pick(flag, in2, in1)


def take_static(in1, in2, out1, out2, pw_out, pv_out):
    from_next, from_prev = within_of(in1[...], in2[...])
    odd_in, even_in = across_of(out1[...], out2[...])
    pw_out[:, 0:B] = from_next[0:NB, :]
    pw_out[:, B : 2 * B] = from_prev[0:NB, :]
    for s in range(S):
        h = s // 2
        side = even_in if s % 2 else odd_in
        pw_out[KC * s : KC * s + KC, 2 * B :] = side[KC * h : KC * h + KC, :]
        at = 2 * KC + 8 * h
        pw_out[NCL + 8 * s : NCL + 8 * s + 8, 2 * B :] = side[at : at + 8, :]
        at = 2 * KC + 16 + R * h
        pv_out[R * s : R * s + R, 2 * B :] = side[at : at + R, :]
    pv_out[:, 0:B] = from_next[NB:STATIC, :]
    pv_out[:, B : 2 * B] = from_prev[NB:STATIC, :]


def member_sum(recv):
    total = recv[0]
    for k in range(1, NSUB):
        total = total + recv[k]
    return total


def k_rows(recv, out, csol):
    total = member_sum(recv)
    own = jnp.where(iota((R, B), 1) < NCL, total[:, 2 * B : 3 * B], 0.0)
    csol[0] = own
    csol[1] = total[:, 3 * B : 4 * B]
    csol[2] = total[:, 4 * B : 5 * B]
    x = jnp.concatenate([total[:, : 2 * B], own], axis=1)
    out[:, :, 0:D] = jnp.broadcast_to(x[None], (out.shape[0], R, D))


def cluster_ids(recv):
    lane = iota((8, B), 1)
    rows = []
    for half in range(2):
        ids = jnp.zeros((8, B), F32)
        for j in range(4):
            row = recv[4 * half + j, 0:1, 2 * B : 3 * B]
            row = pltpu.roll(jnp.broadcast_to(row, (8, B)), (32 + 32 * j) % B, 1)
            ids = jnp.where(lane // 32 == j, row, ids)
        rows.append(ids)
    return rows


def k_first_rows(recv, out, csol, ids_out):
    k_rows(recv, out, csol)
    low, high = cluster_ids(recv)
    ids = jnp.where(iota((8, B), 0) == 0, low, high)
    ids_out[...] = ids
    out[:, :, D:] = jnp.broadcast_to(ids[None, :R], (out.shape[0], R, B))


def k_pass(recv, out):
    y, z = lax.axis_index("y"), lax.axis_index("z")
    n_y, n_z = recv.shape[0], out.shape[0]
    total = jnp.sum(recv[:, :, 0 : 2 * B], axis=0)
    other = jnp.where(z == 0, jnp.minimum(y + 1, n_y - 1), jnp.maximum(y - 1, 0))
    x = jnp.concatenate([total, recv[y, :, 2 * B :], recv[other, :, 2 * B :]], axis=1)
    out[...] = jnp.broadcast_to(x[None], (n_z, *x.shape))


def k_first_pass(recv, after, out):
    del after
    k_pass(recv, out)


def neighbours(recv, at, wrapped_at):
    z = lax.axis_index("z")
    n_z = recv.shape[0]
    last, first = z == n_z - 1, z == 0
    nxt = recv[jnp.where(last, 0, z + 1)]
    prv = recv[jnp.where(first, n_z - 1, z - 1)]

    def tile(x, use_wrapped):
        plain = x[:, at : at + B]
        wrapped = x[:, wrapped_at : wrapped_at + B]
        x = jnp.where(jnp.full((R, B), use_wrapped.astype(I32), I32) == 1, wrapped, plain)
        return jnp.concatenate([x, x], axis=0)

    return tile(nxt, last), tile(prv, first)


def picked_columns(gc, rows, hi_out, lo_out):
    ids = jnp.concatenate([x[:1].astype(I32) for x in rows], axis=1)
    n = iota((gc.shape[1], ids.shape[1]), 0)
    onehot = jnp.where(n == ids, 1.0, 0.0).astype(BF16)
    gh, gl = split(gc[...])
    zero = jnp.zeros((2 * B - CHUNK, ids.shape[1]), BF16)
    hi_out[0:CHUNK, :] = mm(gh, onehot).astype(BF16)
    hi_out[CHUNK : 2 * B, :] = zero
    lo_out[0:CHUNK, :] = mm(gl, onehot).astype(BF16)
    lo_out[CHUNK : 2 * B, :] = zero


def k_own_columns(ids, gc, hi_out, lo_out):
    picked_columns(gc, [ids[0:1, :], ids[1:2, :]], hi_out, lo_out)


def solve(recv, parts, msg, scal, cacross, stride):
    total = jnp.sum(recv[:, :, 0 : 2 * B], axis=0)
    total = jnp.concatenate([total, total], axis=0)
    second = total[:, B:]
    lane = iota((8, B), 1)
    x = jnp.concatenate([total[:, :B], jnp.where(lane < 64, second, 0.0)], axis=1)
    xh, xl = split(x)
    ys = []
    for gh, gl in parts:
        y = mm(jnp.concatenate([xh, xl], axis=0), gh[...])
        ys.append(y[:8] + y[8:] + mm(xh, gl[...]))

    def pick(kind, k, to):
        at = 32 * k
        return pltpu.roll(ys[kind][:, at // B * B : at // B * B + B], (to - at) % B, 1)

    none = jnp.zeros((8, B), F32)
    for k in range(NSUB):
        after = pick(0, k + 1, 32) if k + 1 < NSUB else none
        before = pick(0, k - 1, 64) if k > 0 else none
        here = jnp.where(lane < 32, pick(0, k, 0), jnp.where(lane < 64, after, before))
        msg[k] = jnp.where(lane < 96, here, pick(1, k, 96))[:R]
    scal[...] = jnp.concatenate([second, second], axis=0)
    after, before = neighbours(recv, 2 * B, 2 * B + stride)
    after = pltpu.roll(after, B - KC, 1)
    before = pltpu.roll(before, KC, 1)
    both = jnp.where(lane // KC % 2 == 0, after, before)
    cacross[...] = jnp.where(lane < NCL, both, 0.0)[:R]


def k_first_global(recv, gc, gh, gl, odd_after, even_after, msg, scal, cacross, ah, al):
    del odd_after, even_after
    after, before = neighbours(recv, 3 * B, 5 * B)
    lane = iota((8, B), 1)
    after = pltpu.roll(after, B - 8, 1)
    before = pltpu.roll(before, 8, 1)
    ids = jnp.where(lane // 8 % 2 == 0, after, before)
    picked_columns(gc, [ids[0:1], ids[1:2]], ah, al)
    solve(recv, ((gh, gl), (ah, al)), msg, scal, cacross, 2 * B)


def k_global(recv, gh, gl, ah, al, msg, scal, cacross):
    solve(recv, ((gh, gl), (ah, al)), msg, scal, cacross, B)


def four_times(x):
    x = jnp.concatenate([x, x], axis=0)
    return jnp.concatenate([x, x], axis=0)


def corrections(recv, csol, cacross, w, pw):
    picks = four_times(member_sum(recv))
    tail = iota((ROWS, B), 1) >= NCL

    def sol(cluster, turn):
        p = pltpu.roll(picks, turn, 1) if turn else picks
        return jnp.where(tail, p, four_times(cluster))

    own = spread_back(sol(csol[0], 96), w[...])
    sides = (sol(csol[1], 64), sol(csol[2], 32), sol(cacross[...], 0))
    pi = [spread_back(x, pw[:, b * B : (b + 1) * B]) for b, x in enumerate(sides)]
    return own, jnp.concatenate(pi, axis=1)


def received(from_next, from_prev, out1, out2):
    odd_in, even_in = across_of(out1[...], out2[...])
    across = jnp.concatenate([odd_in[0:R], even_in[0:R], odd_in[R:], even_in[R:]], axis=0)
    return jnp.concatenate([from_next, from_prev, across], axis=1)


def paired(n_cl):
    c, k = lax.axis_index("y") * lax.axis_size("z") + lax.axis_index("z"), lax.axis_index("sub")
    lane = iota((ROWS, D), 1)
    is_even = iota((ROWS, D), 0) // R % 2 == 0
    yes = [
        jnp.where(x, 1.0, 0.0) for x in (k < NSUB - 1, k > 0, c < n_cl - 1, c > 0)
    ]
    across = jnp.where(is_even, yes[2], yes[3])
    return jnp.where(lane < B, yes[0], jnp.where(lane < 2 * B, yes[1], across))


def image_of(d, pd, sg, ops):
    spread = sg * (d + pd)
    low = spread.astype(BF16)
    image = jnp.zeros((ROWS, D), F32)
    row = iota((ROWS, D), 0) // R
    for s in range(S):
        image = jnp.where(row == s, mm(low, ops[s]), image)
    return sg * image, row_dot(spread, image)


def k_first_image(
    recv, csol, cacross, in1, in2, out1, out2, w, v, sg, ops, idx,
    pw, pv, d_out, pd_out, signed_out, curv, *outs,
):
    take_static(in1, in2, out1, out2, pw, pv)
    fix, pfix = corrections(recv, csol, cacross, w, pw)
    d = v[...] - fix
    pd = pv[...] - pfix
    d_out[...] = d
    pd_out[...] = pd
    signed, c = image_of(d, pd, sg[...], ops)
    signed_out[...] = signed
    curv[...] = jnp.broadcast_to(c[:8], (8, B))
    write_moved(signed, idx, *outs)


def make_product(n_cl):
    def k_product(ids, signed, in1, in2, out1, out2, v, w, cc, curv, ap_out, pap_out, msg):
        pi = received(*within_of(in1[...], in2[...]), out1, out2)
        u = signed[...]
        ap = u + pi
        ap_out[...] = ap
        pap_out[...] = pi + paired(n_cl) * u
        scalars = [curv[...][:, :1], row_dot(v[...], ap)[:8], row_dot(ap, ap)[:8]]
        write_message(msg, coefs(ap, w[...]), cc, ids, scalars)

    return k_product


def scalar_at(scal, j):
    return jnp.sum(jnp.where(iota((ROWS, B), 1) == 64 + j, scal, 0.0), axis=1, keepdims=True)


LAST = ROWS + 8


def k_last_image(
    recv, csol, cacross, scal0, scal1, w, pw, v, d, pd, ap, pap, sg, ops, idx,
    r_out, x_out, d_out, signed_out, msg, out1, out2,
):
    fix, pfix = corrections(recv, csol, cacross, w, pw)
    rho = scalar_at(scal0[...], 0)
    s1 = scal1[...]
    step = rho / scalar_at(s1, 0)
    rho_new = rho - 2.0 * step * scalar_at(s1, 1) + step * step * scalar_at(s1, 2)
    beta = rho_new / rho
    ap_ = ap[...]
    d0 = d[...]
    pd0 = pd[...]
    r = v[...] - step * ap_
    r_out[...] = r
    x_out[...] = step * d0
    d1 = d0 - step * (ap_ - fix) + beta * d0
    pd1 = pd0 - step * (pap[...] - pfix) + beta * pd0
    d_out[...] = d1
    signed, c = image_of(d1, pd1, sg[...], ops)
    signed_out[...] = signed
    sq = row_dot(r, r)
    lane = iota((8, B), 1)
    row = iota((8, B), 0)
    both = jnp.where(lane == row, c[:8], jnp.where(lane == row + R, sq[:8], 0.0))
    both = jnp.where(row < R, both, 0.0)
    up, down, even, odd = moved_blocks(signed, idx)
    write_across(even, odd, out1, out2)
    msg[...] = jnp.zeros(msg.shape, F32)
    for k in range(NSUB):
        msg[k, ROWS:LAST, :] = both
    k = lax.axis_index("sub")
    msg[jnp.minimum(k + 1, NSUB - 1), 0:ROWS, :] = up
    msg[jnp.maximum(k - 1, 0), 0:ROWS, :] = down


def k_total(recv, out, from_next, from_prev):
    total = recv[0, ROWS:LAST, :]
    for j in range(1, NSUB):
        total = total + recv[j, ROWS:LAST, :]
    line = jnp.sum(total, axis=0, keepdims=True)
    out[...] = jnp.broadcast_to(line[None], out.shape)
    k = lax.axis_index("sub")
    after = recv[jnp.minimum(k + 1, NSUB - 1), 0:ROWS, :]
    before = recv[jnp.maximum(k - 1, 0), 0:ROWS, :]
    from_next[...] = jnp.where(jnp.full((ROWS, B), k, I32) < NSUB - 1, after, 0.0)
    from_prev[...] = jnp.where(jnp.full((ROWS, B), k, I32) > 0, before, 0.0)


def k_finish(recv, signed, fn, fp, out1, out2, x, r, d, x_out, r_out):
    line = jnp.broadcast_to(jnp.sum(recv[...], axis=0), (ROWS, B))
    lane = iota((ROWS, B), 1)
    row = iota((ROWS, B), 0) % R
    curv = jnp.sum(jnp.where(lane == row, line, 0.0), axis=1, keepdims=True)
    rho = jnp.sum(jnp.where(lane == row + R, line, 0.0), axis=1, keepdims=True)
    step = rho / curv
    xn = x[...] + step * d[...]
    rn = r[...] - step * (signed[...] + received(fn[...], fp[...], out1, out2))
    for s in range(S):
        x_out[s] = xn[R * s : R * s + R]
        r_out[s] = rn[R * s : R * s + R]


def call(body, outs, *args, smem=(), scratch=()):
    def space(i):
        return pltpu.SMEM if i in smem else pltpu.VMEM

    specs = [pl.BlockSpec(memory_space=space(i)) for i in range(len(args))]
    out_shape = tuple(jax.ShapeDtypeStruct(s, t) for s, t in outs)
    return pl.pallas_call(
        body,
        out_shape=out_shape,
        in_specs=specs,
        out_specs=tuple(pl.BlockSpec(memory_space=pltpu.VMEM) for _ in outs),
        scratch_shapes=scratch,
        compiler_params=pltpu.CompilerParams(vmem_limit_bytes=VMEM_LIMIT),
    )(*args)


def to_owner(x, axis):
    return lax.all_to_all(x, axis, 0, 0, tiled=True)


def f32(*shape):
    return (shape, F32)


FIELD = f32(ROWS, D)


SENDS = (f32(ROWS, B), f32(ROWS, B), f32(2 * R, B), f32(2 * R, B))


def swap(x, axis, n, first):
    low = range(0 if first else 1, n - 1, 2)
    return lax.ppermute(x, axis, [p for i in low for p in ((i, i + 1), (i + 1, i))])


def exchange_across(first, second, n_cl):
    first = swap(first, CLUSTER, n_cl, True)
    second = swap(second, CLUSTER, n_cl, False)
    return first, second


def exchange(in1, in2, out1, out2, n_sub, n_cl):
    across = exchange_across(out1, out2, n_cl)
    in2 = swap(in2, "sub", n_sub, False)
    in1 = swap(in1, "sub", n_sub, True)
    return in1, in2, *across


def solve_all(rhs, operators, signs, links, cb, kb, ids, cluster_coarse, gc):
    n_sub = lax.axis_size("sub")
    n_y = lax.axis_size("y")
    n_z = lax.axis_size("z")
    n_cl = n_y * n_z
    cc = cluster_coarse.reshape(NCL, NSUB * NCL)
    message = f32(NSUB, R, MSG)
    picked = ((2 * B, 2 * B), BF16)
    answer = (f32(NSUB, R, B), f32(ROWS, B), f32(R, B))

    w = jnp.concatenate([cb.reshape(NCL, D), kb.reshape(NB - NCL, D)], axis=0)
    msg, v = call(k_coefs, (message, FIELD), ids, rhs, w, cc, smem=(0,))
    recv = to_owner(msg, "sub")
    rows, csol, all_ids = call(
        k_first_rows, (f32(n_y, R, 4 * B), f32(3, R, B), f32(8, B)), recv
    )
    sg, idx, in1 = call(
        k_send_first,
        (FIELD, ((3, ROWS, B), I32), f32(STATIC, B)),
        all_ids, signs, links.transpose(1, 0, 2), w, v,
    )
    in1 = swap(in1, "sub", n_sub, True)
    recv = to_owner(rows, "y")
    (rows,) = call(k_first_pass, (f32(n_z, R, 6 * B),), recv, in1)
    out = call(k_send_across, (f32(PACK, B), f32(PACK, B)), recv, w, v, idx)
    across = exchange_across(*out, n_cl)
    gh, gl = call(k_own_columns, (picked, picked), all_ids, gc)
    to_all, scal0, cacross, ah, al = call(
        k_first_global, (*answer, picked, picked), to_owner(rows, "z"), gc, gh, gl, *across
    )
    (in2,) = call(k_send_second, (f32(STATIC, B),), to_all, w, v, idx)
    in2 = swap(in2, "sub", n_sub, False)
    to_all = to_owner(to_all, "sub")
    pw, pv, d, pd, signed, curv, *out = call(
        k_first_image,
        (f32(NB, D), FIELD, FIELD, FIELD, FIELD, f32(8, B), *SENDS),
        to_all, csol, cacross, in1, in2, *across,
        w, v, sg, operators, idx,
    )
    got = exchange(*out, n_sub, n_cl)
    ap, pap, msg = call(
        make_product(n_cl),
        (FIELD, FIELD, message),
        ids, signed, *got, v, w, cc, curv, smem=(0,),
    )
    rows, csol = call(k_rows, (f32(n_y, R, D), f32(3, R, B)), to_owner(msg, "sub"))
    (rows,) = call(k_pass, (f32(n_z, R, 4 * B),), to_owner(rows, "y"))
    to_all, scal1, cacross = call(k_global, answer, to_owner(rows, "z"), gh, gl, ah, al)
    r, x, d1, signed, msg, *out = call(
        k_last_image,
        (FIELD, FIELD, FIELD, FIELD, f32(NSUB, LAST, B), f32(2 * R, B), f32(2 * R, B)),
        to_owner(to_all, "sub"), csol, cacross, scal0, scal1,
        w, pw, v, d, pd, ap, pap, sg, operators, idx,
    )
    line, from_next, from_prev = call(
        k_total, (f32(n_cl, 1, B), f32(ROWS, B), f32(ROWS, B)), to_owner(msg, "sub")
    )
    across = exchange_across(*out, n_cl)
    out = f32(S, R, D)
    return call(
        k_finish, (out, out), to_owner(line, CLUSTER), signed, from_next, from_prev, *across, x, r, d1
    )


def solution(mesh):
    n_y, n_z = 8, 12
    torus = Mesh(mesh.devices.reshape(n_y, n_z, NSUB), ("y", "z", "sub"))
    both = ("y", "z", "sub")
    in_specs = (
        P(both, None, None),
        P(both, None, None),
        P(both, None),
        P(both, None, None),
        P(both, None, None),
        P(both, None, None),
        P(both, None),
        P(CLUSTER, "sub", None),
        P("sub", None),
    )
    out_specs = (P(both, None, None), P(both, None, None))
    return jax.shard_map(solve_all, mesh=torus, in_specs=in_specs, out_specs=out_specs, check_vma=False)
```

```python
import jax
import jax.numpy as jnp
from jax import lax
from jax.experimental import pallas as pl
from jax.experimental.pallas import tpu as pltpu
from jax.sharding import Mesh
from jax.sharding import PartitionSpec as P


F32 = jnp.float32
BF16 = jnp.bfloat16
I32 = jnp.int32
R = 4
S = 4
ROWS = R * S
B = 128
D = 384
KC = 24
NB = 128
NCL = S * KC
CHUNK = 192
NSUB = 8
CLUSTER = ("y", "z")
VMEM_LIMIT = 16 * 2**20


def iota(shape, dim):
    return lax.broadcasted_iota(I32, shape, dim)


def pick(flag, a, b):
    return jnp.where(jnp.full(a.shape, flag.astype(I32), I32) == 1, a, b)


def even_member():
    return lax.axis_index("sub") % 2 == 0


def even_cluster():
    return (lax.axis_index("y") * lax.axis_size("z") + lax.axis_index("z")) % 2 == 0


def split(x):
    hi = x.astype(BF16)
    return hi, (x - hi.astype(F32)).astype(BF16)


def mm(a, b):
    return lax.dot_general(a, b, (((1,), (0,)), ((), ())), preferred_element_type=F32)


def mm_t(a, b):
    return lax.dot_general(a, b, (((1,), (1,)), ((), ())), preferred_element_type=F32)


def dot2(x, w, f=mm):
    n = x.shape[0]
    xh, xl = split(x)
    wh, wl = split(w)
    xs = jnp.concatenate([xh, xl], axis=0)
    both = f(xs, wh)
    return both[:n] + both[n:] + f(xh, wl)


def lanes_of_sub(shape):
    lane = iota(shape, 1)
    return jnp.where(lane < NCL, lane // KC, (lane - NCL) // 8)


def own_mask():
    return iota((ROWS, NB), 0) // R == lanes_of_sub((ROWS, NB))


def by_load(x):
    y = x[:8] + x[8:]
    y = y + pltpu.roll(y, 4, 0)
    return jnp.concatenate([y, y], axis=0)


def coefs(v, w):
    return by_load(jnp.where(own_mask(), dot2(v, w, mm_t), 0.0))


def spread_back(sol, w):
    return dot2(jnp.where(own_mask(), sol, 0.0), w)


def ids_row(ids):
    lane = iota((8, NB), 1)
    row = jnp.full((8, NB), -1, I32)
    for s in range(S):
        for c in range(8):
            row = jnp.where(lane == NCL + 8 * s + c, ids[s, c], row)
    return row


def to_column(row):
    full = jnp.broadcast_to(row[:1], (NB, NB))
    eye = iota((NB, NB), 0) == iota((NB, NB), 1)
    return jnp.sum(jnp.where(eye, full, 0.0), axis=1, keepdims=True)


def window(x, at, width):
    lane = iota((x.shape[0], B), 1)
    tile, off = at // B, at % B
    here = x[:, tile * B : (tile + 1) * B]
    if off:
        here = pltpu.roll(here, B - off, 1)
        if off + width > B:
            after = pltpu.roll(x[:, (tile + 1) * B : (tile + 2) * B], B - off, 1)
            here = jnp.where(lane < B - off, here, after)
    return here


MSG = 5 * B


def write_message(msg, coef, cc, ids, scalars):
    row = ids_row(ids).astype(F32)
    col = to_column(row).astype(I32)
    c4 = coef[:8]
    hi, lo = split(c4)
    low = (c4 - hi.astype(F32) - lo.astype(F32)).astype(BF16)
    parts = jnp.concatenate([hi, lo, low], axis=0)
    ccp = dot2(jnp.where(iota((8, NB), 1) < NCL, c4, 0.0)[:, :NCL], cc[...])
    lane = iota((8, B), 1)
    extra = jnp.zeros((8, B), F32)
    for j, val in enumerate(scalars):
        extra = jnp.where(lane == 64 + j, val, extra)
    none = jnp.zeros((8, B), F32)
    cluster = [jnp.where(lane < NCL, window(ccp, NCL * k, NCL), 0.0) for k in range(NSUB)]
    for k in range(NSUB):
        n = iota((NB, 2 * B), 1)
        onehot = jnp.where((col == n + CHUNK * k) & (n < CHUNK), 1.0, 0.0).astype(BF16)
        y = mm(parts, onehot)
        y = y[:8] + y[8:16] + y[16:24]
        tiles = (
            y[:, :B],
            y[:, B:] + extra,
            jnp.where(lane < NCL, cluster[k], row),
            cluster[k + 1] if k + 1 < NSUB else none,
            cluster[k - 1] if k > 0 else none,
        )
        for t, x in enumerate(tiles):
            msg[k, :, t * B : (t + 1) * B] = x[:R]


def row_dot(a, b):
    return by_load(jnp.sum(a * b, axis=1, keepdims=True))


STATIC = NB + ROWS
PACK = 72


def k_coefs(ids, rhs, w, cc, msg, v_out):
    for s in range(S):
        v_out[R * s : R * s + R, :] = rhs[s]
    v = v_out[...]
    write_message(msg, coefs(v, w[...]), cc, ids, [row_dot(v, v)[:8]])


def k_tables(after, signs, links, sg_out, idx_out):
    del after
    pos = iota((8, B), 1).astype(BF16)
    for s in range(S):
        sg_out[R * s : R * s + R, :] = jnp.broadcast_to(signs[s : s + 1, :].astype(F32), (R, D))
        for b in range(3):
            q = links[b, s : s + 1, :]
            if b == 0 or (b == 2 and s % 2 == 0):
                hot = jnp.where(iota((B, B), 0) == q, 1.0, 0.0).astype(BF16)
                q = mm_t(pos, hot)[:1].astype(I32)
            idx_out[b, R * s : R * s + R, :] = jnp.broadcast_to(q, (R, B))


def static_blocks(w, v, idx, b):
    lanes = pl.ds(pl.multiple_of(b * B, B), B)

    def moved(x, q):
        return jnp.take_along_axis(x, jnp.broadcast_to(q, x.shape), axis=1)

    for s in range(S):
        q = idx[b, R * s : R * s + 1, :]
        for at, n in ((KC * s, KC), (NCL + 8 * s, 8)):
            yield s, at, moved(w[at : at + n, lanes], q)
    yield None, NB, moved(v[:, lanes], idx[b])


def send_within(w, v, idx, out, b):
    for _, at, x in static_blocks(w, v, idx, b):
        out[at : at + x.shape[0], :] = x


def k_send_first(after, signs, links, w, v, sg_out, idx_out, out):
    k_tables(after, signs, links, sg_out, idx_out)
    send_within(w, v, idx_out, out, lax.axis_index("sub") % 2)


def k_send_second(after, w, v, idx, out):
    del after
    send_within(w, v, idx, out, 1 - lax.axis_index("sub") % 2)


def k_send_across(after, w, v, idx, first, second):
    del after
    flag = even_cluster()
    blocks = {(s, at): x for s, at, x in static_blocks(w, v, idx, 2)}

    def put(to, even, odd):
        n = even.shape[0]
        first[to : to + n, :] = pick(flag, even, odd)
        second[to : to + n, :] = pick(flag, odd, even)

    for h in range(2):
        s = 2 * h
        put(KC * h, blocks[s, KC * s], blocks[s + 1, KC * (s + 1)])
        put(2 * KC + 8 * h, blocks[s, NCL + 8 * s], blocks[s + 1, NCL + 8 * s + 8])
        x = blocks[None, NB][8 * h : 8 * h + 8]
        put(2 * KC + 16 + R * h, x[:R], x[R:])


def moved_blocks(v, idx):
    up, down, across = (
        jnp.take_along_axis(v[:, b * B : (b + 1) * B], idx[b], axis=1) for b in range(3)
    )
    even = jnp.concatenate([across[0:R], across[8 : 8 + R]], axis=0)
    odd = jnp.concatenate([across[R:8], across[8 + R :]], axis=0)
    return up, down, even, odd


def write_across(even, odd, first, second):
    flag = even_cluster()
    first[...] = pick(flag, even, odd)
    second[...] = pick(flag, odd, even)


def write_moved(v, idx, in1, in2, out1, out2):
    up, down, even, odd = moved_blocks(v, idx)
    flag = even_member()
    in1[...] = pick(flag, up, down)
    in2[...] = pick(flag, down, up)
    write_across(even, odd, out1, out2)


def across_of(out1, out2):
    flag = even_cluster()
    return pick(flag, out1, out2), pick(flag, out2, out1)


def within_of(in1, in2):
    flag = even_member()
    return pick(flag, in1, in2), pick(flag, in2, in1)


def take_static(in1, in2, out1, out2, pw_out, pv_out):
    from_next, from_prev = within_of(in1[...], in2[...])
    odd_in, even_in = across_of(out1[...], out2[...])
    pw_out[:, 0:B] = from_next[0:NB, :]
    pw_out[:, B : 2 * B] = from_prev[0:NB, :]
    for s in range(S):
        h = s // 2
        side = even_in if s % 2 else odd_in
        pw_out[KC * s : KC * s + KC, 2 * B :] = side[KC * h : KC * h + KC, :]
        at = 2 * KC + 8 * h
        pw_out[NCL + 8 * s : NCL + 8 * s + 8, 2 * B :] = side[at : at + 8, :]
        at = 2 * KC + 16 + R * h
        pv_out[R * s : R * s + R, 2 * B :] = side[at : at + R, :]
    pv_out[:, 0:B] = from_next[NB:STATIC, :]
    pv_out[:, B : 2 * B] = from_prev[NB:STATIC, :]


def member_sum(recv):
    total = recv[0]
    for k in range(1, NSUB):
        total = total + recv[k]
    return total


def k_rows(recv, out, csol):
    total = member_sum(recv)
    own = jnp.where(iota((R, B), 1) < NCL, total[:, 2 * B : 3 * B], 0.0)
    csol[0] = own
    csol[1] = total[:, 3 * B : 4 * B]
    csol[2] = total[:, 4 * B : 5 * B]
    x = jnp.concatenate([total[:, : 2 * B], own], axis=1)
    out[:, :, 0:D] = jnp.broadcast_to(x[None], (out.shape[0], R, D))


def cluster_ids(recv):
    lane = iota((8, B), 1)
    rows = []
    for half in range(2):
        ids = jnp.zeros((8, B), F32)
        for j in range(4):
            row = recv[4 * half + j, 0:1, 2 * B : 3 * B]
            row = pltpu.roll(jnp.broadcast_to(row, (8, B)), (32 + 32 * j) % B, 1)
            ids = jnp.where(lane // 32 == j, row, ids)
        rows.append(ids)
    return rows


def k_first_rows(recv, out, csol, ids_out):
    k_rows(recv, out, csol)
    low, high = cluster_ids(recv)
    ids = jnp.where(iota((8, B), 0) == 0, low, high)
    ids_out[...] = ids
    out[:, :, D:] = jnp.broadcast_to(ids[None, :R], (out.shape[0], R, B))


def k_pass(recv, out):
    y, z = lax.axis_index("y"), lax.axis_index("z")
    n_y, n_z = recv.shape[0], out.shape[0]
    total = jnp.sum(recv[:, :, 0 : 2 * B], axis=0)
    other = jnp.where(z == 0, jnp.minimum(y + 1, n_y - 1), jnp.maximum(y - 1, 0))
    x = jnp.concatenate([total, recv[y, :, 2 * B :], recv[other, :, 2 * B :]], axis=1)
    out[...] = jnp.broadcast_to(x[None], (n_z, *x.shape))


def neighbours(recv, at, wrapped_at):
    z = lax.axis_index("z")
    n_z = recv.shape[0]
    last, first = z == n_z - 1, z == 0
    nxt = recv[jnp.where(last, 0, z + 1)]
    prv = recv[jnp.where(first, n_z - 1, z - 1)]

    def tile(x, use_wrapped):
        plain = x[:, at : at + B]
        wrapped = x[:, wrapped_at : wrapped_at + B]
        x = jnp.where(jnp.full((R, B), use_wrapped.astype(I32), I32) == 1, wrapped, plain)
        return jnp.concatenate([x, x], axis=0)

    return tile(nxt, last), tile(prv, first)


def picked_columns(gc, rows, hi_out, lo_out):
    ids = jnp.concatenate([x[:1].astype(I32) for x in rows], axis=1)
    n = iota((gc.shape[1], ids.shape[1]), 0)
    onehot = jnp.where(n == ids, 1.0, 0.0).astype(BF16)
    gh, gl = split(gc[...])
    zero = jnp.zeros((2 * B - CHUNK, ids.shape[1]), BF16)
    hi_out[0:CHUNK, :] = mm(gh, onehot).astype(BF16)
    hi_out[CHUNK : 2 * B, :] = zero
    lo_out[0:CHUNK, :] = mm(gl, onehot).astype(BF16)
    lo_out[CHUNK : 2 * B, :] = zero


def k_own_columns(ids, gc, hi_out, lo_out):
    picked_columns(gc, [ids[0:1, :], ids[1:2, :]], hi_out, lo_out)


def solve(recv, parts, msg, scal, cacross, stride):
    total = jnp.sum(recv[:, :, 0 : 2 * B], axis=0)
    total = jnp.concatenate([total, total], axis=0)
    second = total[:, B:]
    lane = iota((8, B), 1)
    x = jnp.concatenate([total[:, :B], jnp.where(lane < 64, second, 0.0)], axis=1)
    xh, xl = split(x)
    ys = []
    for gh, gl in parts:
        y = mm(jnp.concatenate([xh, xl], axis=0), gh[...])
        ys.append(y[:8] + y[8:] + mm(xh, gl[...]))

    def pick(kind, k, to):
        at = 32 * k
        return pltpu.roll(ys[kind][:, at // B * B : at // B * B + B], (to - at) % B, 1)

    none = jnp.zeros((8, B), F32)
    for k in range(NSUB):
        after = pick(0, k + 1, 32) if k + 1 < NSUB else none
        before = pick(0, k - 1, 64) if k > 0 else none
        here = jnp.where(lane < 32, pick(0, k, 0), jnp.where(lane < 64, after, before))
        msg[k] = jnp.where(lane < 96, here, pick(1, k, 96))[:R]
    scal[...] = jnp.concatenate([second, second], axis=0)
    after, before = neighbours(recv, 2 * B, 2 * B + stride)
    after = pltpu.roll(after, B - KC, 1)
    before = pltpu.roll(before, KC, 1)
    both = jnp.where(lane // KC % 2 == 0, after, before)
    cacross[...] = jnp.where(lane < NCL, both, 0.0)[:R]


def k_first_global(recv, gc, gh, gl, msg, scal, cacross, ah, al):
    after, before = neighbours(recv, 3 * B, 5 * B)
    lane = iota((8, B), 1)
    after = pltpu.roll(after, B - 8, 1)
    before = pltpu.roll(before, 8, 1)
    ids = jnp.where(lane // 8 % 2 == 0, after, before)
    picked_columns(gc, [ids[0:1], ids[1:2]], ah, al)
    solve(recv, ((gh, gl), (ah, al)), msg, scal, cacross, 2 * B)


def k_global(recv, gh, gl, ah, al, msg, scal, cacross):
    solve(recv, ((gh, gl), (ah, al)), msg, scal, cacross, B)


def four_times(x):
    x = jnp.concatenate([x, x], axis=0)
    return jnp.concatenate([x, x], axis=0)


def corrections(recv, csol, cacross, w, pw):
    picks = four_times(member_sum(recv))
    tail = iota((ROWS, B), 1) >= NCL

    def sol(cluster, turn):
        p = pltpu.roll(picks, turn, 1) if turn else picks
        return jnp.where(tail, p, four_times(cluster))

    own = spread_back(sol(csol[0], 96), w[...])
    sides = (sol(csol[1], 64), sol(csol[2], 32), sol(cacross[...], 0))
    pi = [spread_back(x, pw[:, b * B : (b + 1) * B]) for b, x in enumerate(sides)]
    return own, jnp.concatenate(pi, axis=1)


def received(from_next, from_prev, out1, out2):
    odd_in, even_in = across_of(out1[...], out2[...])
    across = jnp.concatenate([odd_in[0:R], even_in[0:R], odd_in[R:], even_in[R:]], axis=0)
    return jnp.concatenate([from_next, from_prev, across], axis=1)


def paired(n_cl):
    c, k = lax.axis_index("y") * lax.axis_size("z") + lax.axis_index("z"), lax.axis_index("sub")
    lane = iota((ROWS, D), 1)
    is_even = iota((ROWS, D), 0) // R % 2 == 0
    yes = [
        jnp.where(x, 1.0, 0.0) for x in (k < NSUB - 1, k > 0, c < n_cl - 1, c > 0)
    ]
    across = jnp.where(is_even, yes[2], yes[3])
    return jnp.where(lane < B, yes[0], jnp.where(lane < 2 * B, yes[1], across))


def image_of(d, pd, sg, ops):
    spread = sg * (d + pd)
    low = spread.astype(BF16)
    image = jnp.zeros((ROWS, D), F32)
    row = iota((ROWS, D), 0) // R
    for s in range(S):
        image = jnp.where(row == s, mm(low, ops[s]), image)
    return sg * image, row_dot(spread, image)


def k_first_image(
    recv, csol, cacross, in1, in2, out1, out2, w, v, sg, ops, idx,
    pw, pv, d_out, pd_out, signed_out, curv, *outs,
):
    take_static(in1, in2, out1, out2, pw, pv)
    fix, pfix = corrections(recv, csol, cacross, w, pw)
    d = v[...] - fix
    pd = pv[...] - pfix
    d_out[...] = d
    pd_out[...] = pd
    signed, c = image_of(d, pd, sg[...], ops)
    signed_out[...] = signed
    curv[...] = jnp.broadcast_to(c[:8], (8, B))
    write_moved(signed, idx, *outs)


def make_product(n_cl):
    def k_product(ids, signed, in1, in2, out1, out2, v, w, cc, curv, ap_out, pap_out, msg):
        pi = received(*within_of(in1[...], in2[...]), out1, out2)
        u = signed[...]
        ap = u + pi
        ap_out[...] = ap
        pap_out[...] = pi + paired(n_cl) * u
        scalars = [curv[...][:, :1], row_dot(v[...], ap)[:8], row_dot(ap, ap)[:8]]
        write_message(msg, coefs(ap, w[...]), cc, ids, scalars)

    return k_product


def scalar_at(scal, j):
    return jnp.sum(jnp.where(iota((ROWS, B), 1) == 64 + j, scal, 0.0), axis=1, keepdims=True)


def k_last_image(
    recv, csol, cacross, scal0, scal1, w, pw, v, d, pd, ap, pap, sg, ops, idx,
    r_out, x_out, d_out, signed_out, msg, *outs,
):
    fix, pfix = corrections(recv, csol, cacross, w, pw)
    rho = scalar_at(scal0[...], 0)
    s1 = scal1[...]
    step = rho / scalar_at(s1, 0)
    rho_new = rho - 2.0 * step * scalar_at(s1, 1) + step * step * scalar_at(s1, 2)
    beta = rho_new / rho
    ap_ = ap[...]
    d0 = d[...]
    pd0 = pd[...]
    r = v[...] - step * ap_
    r_out[...] = r
    x_out[...] = step * d0
    d1 = d0 - step * (ap_ - fix) + beta * d0
    pd1 = pd0 - step * (pap[...] - pfix) + beta * pd0
    d_out[...] = d1
    signed, c = image_of(d1, pd1, sg[...], ops)
    signed_out[...] = signed
    sq = row_dot(r, r)
    lane = iota((8, B), 1)
    row = iota((8, B), 0)
    both = jnp.where(lane == row, c[:8], jnp.where(lane == row + R, sq[:8], 0.0))
    line = jnp.sum(jnp.where(row < R, both, 0.0), axis=0, keepdims=True)
    msg[...] = jnp.broadcast_to(line[None], msg.shape)
    write_moved(signed, idx, *outs)


def k_total(recv, out):
    out[...] = jnp.broadcast_to(jnp.sum(recv[...], axis=0, keepdims=True), out.shape)


def k_finish(recv, signed, in1, in2, out1, out2, x, r, d, x_out, r_out):
    line = jnp.broadcast_to(jnp.sum(recv[...], axis=0), (ROWS, B))
    lane = iota((ROWS, B), 1)
    row = iota((ROWS, B), 0) % R
    curv = jnp.sum(jnp.where(lane == row, line, 0.0), axis=1, keepdims=True)
    rho = jnp.sum(jnp.where(lane == row + R, line, 0.0), axis=1, keepdims=True)
    step = rho / curv
    xn = x[...] + step * d[...]
    pi = received(*within_of(in1[...], in2[...]), out1, out2)
    rn = r[...] - step * (signed[...] + pi)
    for s in range(S):
        x_out[s] = xn[R * s : R * s + R]
        r_out[s] = rn[R * s : R * s + R]


def call(body, outs, *args, smem=(), scratch=()):
    def space(i):
        return pltpu.SMEM if i in smem else pltpu.VMEM

    specs = [pl.BlockSpec(memory_space=space(i)) for i in range(len(args))]
    out_shape = tuple(jax.ShapeDtypeStruct(s, t) for s, t in outs)
    return pl.pallas_call(
        body,
        out_shape=out_shape,
        in_specs=specs,
        out_specs=tuple(pl.BlockSpec(memory_space=pltpu.VMEM) for _ in outs),
        scratch_shapes=scratch,
        compiler_params=pltpu.CompilerParams(vmem_limit_bytes=VMEM_LIMIT),
    )(*args)


def to_owner(x, axis):
    return lax.all_to_all(x, axis, 0, 0, tiled=True)


def f32(*shape):
    return (shape, F32)


FIELD = f32(ROWS, D)


SENDS = (f32(ROWS, B), f32(ROWS, B), f32(2 * R, B), f32(2 * R, B))


def swap(x, axis, n, first):
    low = range(0 if first else 1, n - 1, 2)
    return lax.ppermute(x, axis, [p for i in low for p in ((i, i + 1), (i + 1, i))])


def exchange_across(first, second, n_cl):
    first = swap(first, CLUSTER, n_cl, True)
    second = swap(second, CLUSTER, n_cl, False)
    return first, second


def exchange(in1, in2, out1, out2, n_sub, n_cl):
    across = exchange_across(out1, out2, n_cl)
    in2 = swap(in2, "sub", n_sub, False)
    in1 = swap(in1, "sub", n_sub, True)
    return in1, in2, *across


def solve_all(rhs, operators, signs, links, cb, kb, ids, cluster_coarse, gc):
    n_sub = lax.axis_size("sub")
    n_y = lax.axis_size("y")
    n_z = lax.axis_size("z")
    n_cl = n_y * n_z
    cc = cluster_coarse.reshape(NCL, NSUB * NCL)
    message = f32(NSUB, R, MSG)
    picked = ((2 * B, 2 * B), BF16)
    answer = (f32(NSUB, R, B), f32(ROWS, B), f32(R, B))

    w = jnp.concatenate([cb.reshape(NCL, D), kb.reshape(NB - NCL, D)], axis=0)
    msg, v = call(k_coefs, (message, FIELD), ids, rhs, w, cc, smem=(0,))
    recv = to_owner(msg, "sub")
    rows, csol, all_ids = call(
        k_first_rows, (f32(n_y, R, 4 * B), f32(3, R, B), f32(8, B)), recv
    )
    sg, idx, in1 = call(
        k_send_first,
        (FIELD, ((3, ROWS, B), I32), f32(STATIC, B)),
        all_ids, signs, links.transpose(1, 0, 2), w, v,
    )
    recv = to_owner(rows, "y")
    in1 = swap(in1, "sub", n_sub, True)
    (rows,) = call(k_pass, (f32(n_z, R, 6 * B),), recv)
    recv_z = to_owner(rows, "z")
    out = call(k_send_across, (f32(PACK, B), f32(PACK, B)), recv, w, v, idx)
    across = exchange_across(*out, n_cl)
    gh, gl = call(k_own_columns, (picked, picked), all_ids, gc)
    to_all, scal0, cacross, ah, al = call(
        k_first_global, (*answer, picked, picked), recv_z, gc, gh, gl
    )
    (in2,) = call(k_send_second, (f32(STATIC, B),), to_all, w, v, idx)
    in2 = swap(in2, "sub", n_sub, False)
    to_all = to_owner(to_all, "sub")
    pw, pv, d, pd, signed, curv, *out = call(
        k_first_image,
        (f32(NB, D), FIELD, FIELD, FIELD, FIELD, f32(8, B), *SENDS),
        to_all, csol, cacross, in1, in2, *across,
        w, v, sg, operators, idx,
    )
    got = exchange(*out, n_sub, n_cl)
    ap, pap, msg = call(
        make_product(n_cl),
        (FIELD, FIELD, message),
        ids, signed, *got, v, w, cc, curv, smem=(0,),
    )
    rows, csol = call(k_rows, (f32(n_y, R, D), f32(3, R, B)), to_owner(msg, "sub"))
    (rows,) = call(k_pass, (f32(n_z, R, 4 * B),), to_owner(rows, "y"))
    to_all, scal1, cacross = call(k_global, answer, to_owner(rows, "z"), gh, gl, ah, al)
    r, x, d1, signed, line, *out = call(
        k_last_image,
        (FIELD, FIELD, FIELD, FIELD, f32(n_y * n_sub, 1, B), *SENDS),
        to_owner(to_all, "sub"), csol, cacross, scal0, scal1,
        w, pw, v, d, pd, ap, pap, sg, operators, idx,
    )
    line = to_owner(line, ("y", "sub"))
    (line,) = call(k_total, (f32(n_z, 1, B),), line)
    line = to_owner(line, "z")
    got = exchange(*out, n_sub, n_cl)
    out = f32(S, R, D)
    return call(k_finish, (out, out), line, signed, *got, x, r, d1)


def solution(mesh):
    n_y, n_z = 8, 12
    torus = Mesh(mesh.devices.reshape(n_y, n_z, NSUB), ("y", "z", "sub"))
    both = ("y", "z", "sub")
    in_specs = (
        P(both, None, None),
        P(both, None, None),
        P(both, None),
        P(both, None, None),
        P(both, None, None),
        P(both, None, None),
        P(both, None),
        P(CLUSTER, "sub", None),
        P("sub", None),
    )
    out_specs = (P(both, None, None), P(both, None, None))
    return jax.shard_map(solve_all, mesh=torus, in_specs=in_specs, out_specs=out_specs, check_vma=False)
```

```python
import jax
import jax.numpy as jnp
from jax import lax
from jax.experimental import pallas as pl
from jax.experimental.pallas import tpu as pltpu
from jax.sharding import Mesh
from jax.sharding import PartitionSpec as P


F32 = jnp.float32
BF16 = jnp.bfloat16
I32 = jnp.int32
R = 4
S = 4
ROWS = R * S
B = 128
D = 384
KC = 24
NB = 128
NCL = S * KC
CHUNK = 192
NSUB = 8
CLUSTER = ("y", "z")
VMEM_LIMIT = 16 * 2**20


def iota(shape, dim):
    return lax.broadcasted_iota(I32, shape, dim)


def pick(flag, a, b):
    return jnp.where(jnp.full(a.shape, flag.astype(I32), I32) == 1, a, b)


def even_member():
    return lax.axis_index("sub") % 2 == 0


def even_cluster():
    return (lax.axis_index("y") * lax.axis_size("z") + lax.axis_index("z")) % 2 == 0


def split(x):
    hi = x.astype(BF16)
    return hi, (x - hi.astype(F32)).astype(BF16)


def mm(a, b):
    return lax.dot_general(a, b, (((1,), (0,)), ((), ())), preferred_element_type=F32)


def mm_t(a, b):
    return lax.dot_general(a, b, (((1,), (1,)), ((), ())), preferred_element_type=F32)


def dot2(x, w, f=mm):
    n = x.shape[0]
    xh, xl = split(x)
    wh, wl = split(w)
    xs = jnp.concatenate([xh, xl], axis=0)
    both = f(xs, wh)
    return both[:n] + both[n:] + f(xh, wl)


def lanes_of_sub(shape):
    lane = iota(shape, 1)
    return jnp.where(lane < NCL, lane // KC, (lane - NCL) // 8)


def own_mask():
    return iota((ROWS, NB), 0) // R == lanes_of_sub((ROWS, NB))


def by_load(x):
    y = x[:8] + x[8:]
    y = y + pltpu.roll(y, 4, 0)
    return jnp.concatenate([y, y], axis=0)


def coefs(v, w):
    return by_load(jnp.where(own_mask(), dot2(v, w, mm_t), 0.0))


def spread_back(sol, w):
    return dot2(jnp.where(own_mask(), sol, 0.0), w)


def ids_row(ids):
    lane = iota((8, NB), 1)
    row = jnp.full((8, NB), -1, I32)
    for s in range(S):
        for c in range(8):
            row = jnp.where(lane == NCL + 8 * s + c, ids[s, c], row)
    return row


def to_column(row):
    full = jnp.broadcast_to(row[:1], (NB, NB))
    eye = iota((NB, NB), 0) == iota((NB, NB), 1)
    return jnp.sum(jnp.where(eye, full, 0.0), axis=1, keepdims=True)


def window(x, at, width):
    lane = iota((x.shape[0], B), 1)
    tile, off = at // B, at % B
    here = x[:, tile * B : (tile + 1) * B]
    if off:
        here = pltpu.roll(here, B - off, 1)
        if off + width > B:
            after = pltpu.roll(x[:, (tile + 1) * B : (tile + 2) * B], B - off, 1)
            here = jnp.where(lane < B - off, here, after)
    return here


MSG = 5 * B


def clustered(c4, cc):
    return dot2(jnp.where(iota((8, NB), 1) < NCL, c4, 0.0)[:, :NCL], cc)


def marked(scalars):
    lane = iota((8, B), 1)
    extra = jnp.zeros((8, B), F32)
    for j, val in enumerate(scalars):
        extra = jnp.where(lane == 64 + j, val, extra)
    return extra


def write_message(msg, c4, ccp, row, scalars=()):
    col = to_column(row).astype(I32)
    hi, lo = split(c4)
    low = (c4 - hi.astype(F32) - lo.astype(F32)).astype(BF16)
    parts = jnp.concatenate([hi, lo, low], axis=0)
    lane = iota((8, B), 1)
    extra = marked(scalars)
    none = jnp.zeros((8, B), F32)
    cluster = [jnp.where(lane < NCL, window(ccp, NCL * k, NCL), 0.0) for k in range(NSUB)]
    for k in range(NSUB):
        n = iota((NB, 2 * B), 1)
        onehot = jnp.where((col == n + CHUNK * k) & (n < CHUNK), 1.0, 0.0).astype(BF16)
        y = mm(parts, onehot)
        y = y[:8] + y[8:16] + y[16:24]
        tiles = (
            y[:, :B],
            y[:, B:] + extra,
            jnp.where(lane < NCL, cluster[k], row),
            cluster[k + 1] if k + 1 < NSUB else none,
            cluster[k - 1] if k > 0 else none,
        )
        for t, x in enumerate(tiles):
            msg[k, :, t * B : (t + 1) * B] = x[:R]


def row_dot(a, b):
    return by_load(jnp.sum(a * b, axis=1, keepdims=True))


STATIC = NB + ROWS
WITHIN = STATIC + NCL * 6
PACK = 72


def k_coefs(ids, rhs, w, cc, msg, v_out):
    for s in range(S):
        v_out[R * s : R * s + R, :] = rhs[s]
    v = v_out[...]
    c4 = coefs(v, w[...])[:8]
    row = ids_row(ids).astype(F32)
    write_message(msg, c4, clustered(c4, cc[...]), row, [row_dot(v, v)[:8]])


def k_tables(after, signs, links, sg_out, idx_out):
    del after
    pos = iota((8, B), 1).astype(BF16)
    for s in range(S):
        sg_out[R * s : R * s + R, :] = jnp.broadcast_to(signs[s : s + 1, :].astype(F32), (R, D))
        for b in range(3):
            q = links[b, s : s + 1, :]
            if b == 0 or (b == 2 and s % 2 == 0):
                hot = jnp.where(iota((B, B), 0) == q, 1.0, 0.0).astype(BF16)
                q = mm_t(pos, hot)[:1].astype(I32)
            idx_out[b, R * s : R * s + R, :] = jnp.broadcast_to(q, (R, B))


def static_blocks(w, v, idx, b):
    lanes = pl.ds(pl.multiple_of(b * B, B), B)

    def moved(x, q):
        return jnp.take_along_axis(x, jnp.broadcast_to(q, x.shape), axis=1)

    for s in range(S):
        q = idx[b, R * s : R * s + 1, :]
        for at, n in ((KC * s, KC), (NCL + 8 * s, 8)):
            yield s, at, moved(w[at : at + n, lanes], q)
    yield None, NB, moved(v[:, lanes], idx[b])


def send_within(w, v, cc, idx, out, b):
    for _, at, x in static_blocks(w, v, idx, b):
        out[at : at + x.shape[0], :] = x
    for j in range(6):
        out[STATIC + NCL * j : STATIC + NCL * j + NCL, :] = cc[:, j * B : (j + 1) * B]


def coarse_rows(x):
    return jnp.concatenate([x[STATIC + NCL * j : STATIC + NCL * j + NCL, :] for j in range(6)], axis=1)


def k_send_first(after, signs, links, w, v, cc, sg_out, idx_out, out):
    k_tables(after, signs, links, sg_out, idx_out)
    send_within(w, v, cc, idx_out, out, lax.axis_index("sub") % 2)


def k_send_rest(after, w, v, cc, idx, first, second, within):
    del after
    send_within(w, v, cc, idx, within, 1 - lax.axis_index("sub") % 2)
    flag = even_cluster()
    blocks = {(s, at): x for s, at, x in static_blocks(w, v, idx, 2)}

    def put(to, even, odd):
        n = even.shape[0]
        first[to : to + n, :] = pick(flag, even, odd)
        second[to : to + n, :] = pick(flag, odd, even)

    for h in range(2):
        s = 2 * h
        put(KC * h, blocks[s, KC * s], blocks[s + 1, KC * (s + 1)])
        put(2 * KC + 8 * h, blocks[s, NCL + 8 * s], blocks[s + 1, NCL + 8 * s + 8])
        x = blocks[None, NB][8 * h : 8 * h + 8]
        put(2 * KC + 16 + R * h, x[:R], x[R:])


def moved_blocks(v, idx):
    up, down, across = (
        jnp.take_along_axis(v[:, b * B : (b + 1) * B], idx[b], axis=1) for b in range(3)
    )
    even = jnp.concatenate([across[0:R], across[8 : 8 + R]], axis=0)
    odd = jnp.concatenate([across[R:8], across[8 + R :]], axis=0)
    return up, down, even, odd


def write_across(even, odd, first, second):
    flag = even_cluster()
    first[...] = pick(flag, even, odd)
    second[...] = pick(flag, odd, even)


def write_moved(v, idx, in1, in2, out1, out2):
    up, down, even, odd = moved_blocks(v, idx)
    flag = even_member()
    in1[...] = pick(flag, up, down)
    in2[...] = pick(flag, down, up)
    write_across(even, odd, out1, out2)


def across_of(out1, out2):
    flag = even_cluster()
    return pick(flag, out1, out2), pick(flag, out2, out1)


def within_of(in1, in2):
    flag = even_member()
    return pick(flag, in1, in2), pick(flag, in2, in1)


def take_static(in1, in2, out1, out2, pw_out, pv_out):
    from_next, from_prev = within_of(in1[0:STATIC, :], in2[0:STATIC, :])
    odd_in, even_in = across_of(out1[...], out2[...])
    pw_out[:, 0:B] = from_next[0:NB, :]
    pw_out[:, B : 2 * B] = from_prev[0:NB, :]
    for s in range(S):
        h = s // 2
        side = even_in if s % 2 else odd_in
        pw_out[KC * s : KC * s + KC, 2 * B :] = side[KC * h : KC * h + KC, :]
        at = 2 * KC + 8 * h
        pw_out[NCL + 8 * s : NCL + 8 * s + 8, 2 * B :] = side[at : at + 8, :]
        at = 2 * KC + 16 + R * h
        pv_out[R * s : R * s + R, 2 * B :] = side[at : at + R, :]
    pv_out[:, 0:B] = from_next[NB:STATIC, :]
    pv_out[:, B : 2 * B] = from_prev[NB:STATIC, :]


def member_sum(recv):
    total = recv[0]
    for k in range(1, NSUB):
        total = total + recv[k]
    return total


def k_rows(recv, out, csol, scalars=()):
    total = recv[0, :, 0:MSG]
    for k in range(1, NSUB):
        total = total + recv[k, :, 0:MSG]
    own = jnp.where(iota((R, B), 1) < NCL, total[:, 2 * B : 3 * B], 0.0)
    csol[0] = own
    csol[1] = total[:, 3 * B : 4 * B]
    csol[2] = total[:, 4 * B : 5 * B]
    second = total[:, B : 2 * B] + marked(scalars)[:R]
    x = jnp.concatenate([total[:, :B], second, own], axis=1)
    out[:, :, 0:D] = jnp.broadcast_to(x[None], (out.shape[0], R, D))


def cluster_ids(recv):
    lane = iota((8, B), 1)
    rows = []
    for half in range(2):
        ids = jnp.zeros((8, B), F32)
        for j in range(4):
            row = recv[4 * half + j, 0:1, 2 * B : 3 * B]
            row = pltpu.roll(jnp.broadcast_to(row, (8, B)), (32 + 32 * j) % B, 1)
            ids = jnp.where(lane // 32 == j, row, ids)
        rows.append(ids)
    return rows


def k_first_rows(recv, out, csol, ids_out):
    k_rows(recv, out, csol)
    low, high = cluster_ids(recv)
    ids = jnp.where(iota((8, B), 0) == 0, low, high)
    ids_out[...] = ids
    out[:, :, D:] = jnp.broadcast_to(ids[None, :R], (out.shape[0], R, B))


def k_pass(recv, out):
    y, z = lax.axis_index("y"), lax.axis_index("z")
    n_y, n_z = recv.shape[0], out.shape[0]
    total = jnp.sum(recv[:, :, 0 : 2 * B], axis=0)
    other = jnp.where(z == 0, jnp.minimum(y + 1, n_y - 1), jnp.maximum(y - 1, 0))
    x = jnp.concatenate([total, recv[y, :, 2 * B :], recv[other, :, 2 * B :]], axis=1)
    out[...] = jnp.broadcast_to(x[None], (n_z, *x.shape))


def neighbours(recv, at, wrapped_at):
    z = lax.axis_index("z")
    n_z = recv.shape[0]
    last, first = z == n_z - 1, z == 0
    nxt = recv[jnp.where(last, 0, z + 1)]
    prv = recv[jnp.where(first, n_z - 1, z - 1)]

    def tile(x, use_wrapped):
        plain = x[:, at : at + B]
        wrapped = x[:, wrapped_at : wrapped_at + B]
        x = jnp.where(jnp.full((R, B), use_wrapped.astype(I32), I32) == 1, wrapped, plain)
        return jnp.concatenate([x, x], axis=0)

    return tile(nxt, last), tile(prv, first)


def picked_columns(gc, rows, hi_out, lo_out):
    ids = jnp.concatenate([x[:1].astype(I32) for x in rows], axis=1)
    n = iota((gc.shape[1], ids.shape[1]), 0)
    onehot = jnp.where(n == ids, 1.0, 0.0).astype(BF16)
    gh, gl = split(gc[...])
    zero = jnp.zeros((2 * B - CHUNK, ids.shape[1]), BF16)
    hi_out[0:CHUNK, :] = mm(gh, onehot).astype(BF16)
    hi_out[CHUNK : 2 * B, :] = zero
    lo_out[0:CHUNK, :] = mm(gl, onehot).astype(BF16)
    lo_out[CHUNK : 2 * B, :] = zero


def k_own_columns(ids, gc, hi_out, lo_out):
    picked_columns(gc, [ids[0:1, :], ids[1:2, :]], hi_out, lo_out)


def solve(recv, parts, msg, scal, cacross, stride):
    total = jnp.sum(recv[:, :, 0 : 2 * B], axis=0)
    total = jnp.concatenate([total, total], axis=0)
    second = total[:, B:]
    lane = iota((8, B), 1)
    x = jnp.concatenate([total[:, :B], jnp.where(lane < 64, second, 0.0)], axis=1)
    xh, xl = split(x)
    ys = []
    for gh, gl in parts:
        y = mm(jnp.concatenate([xh, xl], axis=0), gh[...])
        ys.append(y[:8] + y[8:] + mm(xh, gl[...]))

    def picked(kind, k, to):
        at = 32 * k
        return pltpu.roll(ys[kind][:, at // B * B : at // B * B + B], (to - at) % B, 1)

    none = jnp.zeros((8, B), F32)
    for k in range(NSUB):
        after = picked(0, k + 1, 32) if k + 1 < NSUB else none
        before = picked(0, k - 1, 64) if k > 0 else none
        here = jnp.where(lane < 32, picked(0, k, 0), jnp.where(lane < 64, after, before))
        msg[k, :, 0:B] = jnp.where(lane < 96, here, picked(1, k, 96))[:R]
        if msg.shape[2] > B:
            msg[k, :, B : 2 * B] = second[:R]
    scal[...] = jnp.concatenate([second, second], axis=0)
    after, before = neighbours(recv, 2 * B, 2 * B + stride)
    after = pltpu.roll(after, B - KC, 1)
    before = pltpu.roll(before, KC, 1)
    both = jnp.where(lane // KC % 2 == 0, after, before)
    cacross[...] = jnp.where(lane < NCL, both, 0.0)[:R]


def k_first_global(recv, gc, gh, gl, msg, scal, cacross, ah, al):
    after, before = neighbours(recv, 3 * B, 5 * B)
    lane = iota((8, B), 1)
    after = pltpu.roll(after, B - 8, 1)
    before = pltpu.roll(before, 8, 1)
    ids = jnp.where(lane // 8 % 2 == 0, after, before)
    picked_columns(gc, [ids[0:1], ids[1:2]], ah, al)
    solve(recv, ((gh, gl), (ah, al)), msg, scal, cacross, 2 * B)


def k_global(recv, gh, gl, ah, al, msg, scal, cacross):
    solve(recv, ((gh, gl), (ah, al)), msg, scal, cacross, B)


def four_times(x):
    x = jnp.concatenate([x, x], axis=0)
    return jnp.concatenate([x, x], axis=0)


def corrections(recv, csol, cacross, w, pw):
    picks = four_times(member_sum(recv)[:, :B])
    tail = iota((ROWS, B), 1) >= NCL

    def sol(cluster, turn):
        p = pltpu.roll(picks, turn, 1) if turn else picks
        return jnp.where(tail, p, four_times(cluster))

    own = spread_back(sol(csol[0], 96), w[...])
    sides = (sol(csol[1], 64), sol(csol[2], 32), sol(cacross[...], 0))
    pi = [spread_back(x, pw[:, b * B : (b + 1) * B]) for b, x in enumerate(sides)]
    return own, jnp.concatenate(pi, axis=1)


def across_received(out1, out2):
    odd_in, even_in = across_of(out1[...], out2[...])
    return jnp.concatenate([odd_in[0:R], even_in[0:R], odd_in[R:], even_in[R:]], axis=0)


def received(from_next, from_prev, out1, out2):
    return jnp.concatenate([from_next, from_prev, across_received(out1, out2)], axis=1)


def paired(n_cl):
    c, k = lax.axis_index("y") * lax.axis_size("z") + lax.axis_index("z"), lax.axis_index("sub")
    lane = iota((ROWS, D), 1)
    is_even = iota((ROWS, D), 0) // R % 2 == 0
    yes = [
        jnp.where(x, 1.0, 0.0) for x in (k < NSUB - 1, k > 0, c < n_cl - 1, c > 0)
    ]
    across = jnp.where(is_even, yes[2], yes[3])
    return jnp.where(lane < B, yes[0], jnp.where(lane < 2 * B, yes[1], across))


def image_of(d, pd, sg, ops):
    spread = sg * (d + pd)
    low = spread.astype(BF16)
    image = jnp.zeros((ROWS, D), F32)
    row = iota((ROWS, D), 0) // R
    for s in range(S):
        image = jnp.where(row == s, mm(low, ops[s]), image)
    return sg * image, row_dot(spread, image)


def k_first_image(
    recv, csol, cacross, in1, in2, out1, out2, w, v, sg, ops, idx,
    pw, pv, d_out, pd_out, signed_out, curv, up_out, down_out, *outs,
):
    take_static(in1, in2, out1, out2, pw, pv)
    fix, pfix = corrections(recv, csol, cacross, w, pw)
    d = v[...] - fix
    pd = pv[...] - pfix
    d_out[...] = d
    pd_out[...] = pd
    signed, c = image_of(d, pd, sg[...], ops)
    signed_out[...] = signed
    curv[...] = jnp.broadcast_to(c[:8], (8, B))
    up, down, even, odd = moved_blocks(signed, idx)
    up_out[...] = up
    down_out[...] = down
    write_across(even, odd, *outs)


def member_ids(all_ids, member, to):
    row = jnp.zeros((8, B), F32)
    which = jnp.full((8, B), member, I32)
    for j in range(NSUB):
        x = jnp.broadcast_to(all_ids[j // 4 : j // 4 + 1, :], (8, B))
        row = jnp.where(which == j, pltpu.roll(x, (to - 32 * (j % 4)) % B, 1), row)
    return row


def k_product(
    ids, signed, up, down, out1, out2, static1, static2, w, pw, cc, all_ids, across_out, msg
):
    k = lax.axis_index("sub")
    odd_k = k % 2
    across = across_received(out1, out2)
    across_out[...] = across
    u = signed[...]
    known = jnp.concatenate([u[:, : 2 * B], u[:, 2 * B :] + across], axis=1)
    own = coefs(known, w[...])[:8]

    def towards(b):
        lanes = pl.ds(pl.multiple_of(b * B, B), B)
        return coefs(signed[:, lanes], pw[:, lanes])[:8]

    first, second = towards(odd_k), towards(1 - odd_k)
    ccp = (
        clustered(own, cc[...])
        + clustered(first, coarse_rows(static1))
        + clustered(second, coarse_rows(static2))
    )
    lane = iota((8, B), 1)
    other = jnp.clip(k - 1 + 2 * odd_k, 0, NSUB - 1)

    def lanes_of(c96, c64, c32, rest):
        return jnp.where(
            lane >= 96, c96, jnp.where(lane >= 64, c64, jnp.where(lane >= 32, c32, rest))
        )

    c4 = lanes_of(own, pltpu.roll(first, B - 32, 1), pltpu.roll(second, B - 64, 1), 0.0)
    row = lanes_of(
        ids_row(ids).astype(F32),
        member_ids(all_ids, k + 1 - 2 * odd_k, 64),
        member_ids(all_ids, other, 32),
        -1.0,
    )
    write_message(msg, c4, ccp, row)
    after, before = jnp.minimum(k + 1, NSUB - 1), jnp.maximum(k - 1, 0)
    for s in range(S):
        at = MSG + B * s
        msg[after, :, at : at + B] = up[R * s : R * s + R, :]
        msg[before, :, at : at + B] = down[R * s : R * s + R, :]


def make_joined(n_cl):
    def k_joined(recv, signed, across, curv, v, out, csol, ap_out, pap_out):
        k = lax.axis_index("sub")

        def block(member, there):
            x = [recv[member, :, MSG + B * s : MSG + B * s + B] for s in range(S)]
            x = jnp.concatenate(x, axis=0)
            return pick(there, x, jnp.zeros_like(x))

        from_next = block(jnp.minimum(k + 1, NSUB - 1), k < NSUB - 1)
        from_prev = block(jnp.maximum(k - 1, 0), k > 0)
        u = signed[...]
        pi = jnp.concatenate([from_next, from_prev, across[...]], axis=1)
        ap = u + pi
        ap_out[...] = ap
        pap_out[...] = pi + paired(n_cl) * u
        scalars = [curv[...][:, :1], row_dot(v[...], ap)[:8], row_dot(ap, ap)[:8]]
        k_rows(recv, out, csol, scalars)

    return k_joined


def scalar_at(scal, j):
    return jnp.sum(jnp.where(iota((ROWS, B), 1) == 64 + j, scal, 0.0), axis=1, keepdims=True)


def k_last_image(
    recv, csol, cacross, scal0, w, pw, v, d, pd, ap, pap, sg, ops, idx,
    r_out, x_out, d_out, signed_out, msg, *outs,
):
    fix, pfix = corrections(recv, csol, cacross, w, pw)
    rho = scalar_at(scal0[...], 0)
    s1 = four_times(member_sum(recv)[:, B : 2 * B])
    step = rho / scalar_at(s1, 0)
    rho_new = rho - 2.0 * step * scalar_at(s1, 1) + step * step * scalar_at(s1, 2)
    beta = rho_new / rho
    ap_ = ap[...]
    d0 = d[...]
    pd0 = pd[...]
    r = v[...] - step * ap_
    r_out[...] = r
    x_out[...] = step * d0
    d1 = d0 - step * (ap_ - fix) + beta * d0
    pd1 = pd0 - step * (pap[...] - pfix) + beta * pd0
    d_out[...] = d1
    signed, c = image_of(d1, pd1, sg[...], ops)
    signed_out[...] = signed
    sq = row_dot(r, r)
    lane = iota((8, B), 1)
    row = iota((8, B), 0)
    both = jnp.where(lane == row, c[:8], jnp.where(lane == row + R, sq[:8], 0.0))
    line = jnp.sum(jnp.where(row < R, both, 0.0), axis=0, keepdims=True)
    msg[...] = jnp.broadcast_to(line[None], msg.shape)
    write_moved(signed, idx, *outs)


def k_total(recv, out):
    out[...] = jnp.broadcast_to(jnp.sum(recv[...], axis=0, keepdims=True), out.shape)


def k_finish(recv, signed, in1, in2, out1, out2, x, r, d, x_out, r_out):
    line = jnp.broadcast_to(jnp.sum(recv[...], axis=0), (ROWS, B))
    lane = iota((ROWS, B), 1)
    row = iota((ROWS, B), 0) % R
    curv = jnp.sum(jnp.where(lane == row, line, 0.0), axis=1, keepdims=True)
    rho = jnp.sum(jnp.where(lane == row + R, line, 0.0), axis=1, keepdims=True)
    step = rho / curv
    xn = x[...] + step * d[...]
    pi = received(*within_of(in1[...], in2[...]), out1, out2)
    rn = r[...] - step * (signed[...] + pi)
    for s in range(S):
        x_out[s] = xn[R * s : R * s + R]
        r_out[s] = rn[R * s : R * s + R]


def call(body, outs, *args, smem=(), scratch=()):
    def space(i):
        return pltpu.SMEM if i in smem else pltpu.VMEM

    specs = [pl.BlockSpec(memory_space=space(i)) for i in range(len(args))]
    out_shape = tuple(jax.ShapeDtypeStruct(s, t) for s, t in outs)
    return pl.pallas_call(
        body,
        out_shape=out_shape,
        in_specs=specs,
        out_specs=tuple(pl.BlockSpec(memory_space=pltpu.VMEM) for _ in outs),
        scratch_shapes=scratch,
        compiler_params=pltpu.CompilerParams(vmem_limit_bytes=VMEM_LIMIT),
    )(*args)


def to_owner(x, axis):
    return lax.all_to_all(x, axis, 0, 0, tiled=True)


def f32(*shape):
    return (shape, F32)


FIELD = f32(ROWS, D)


SENDS = (f32(ROWS, B), f32(ROWS, B), f32(2 * R, B), f32(2 * R, B))


def swap(x, axis, n, first):
    low = range(0 if first else 1, n - 1, 2)
    return lax.ppermute(x, axis, [p for i in low for p in ((i, i + 1), (i + 1, i))])


def exchange_across(first, second, n_cl):
    first = swap(first, CLUSTER, n_cl, True)
    second = swap(second, CLUSTER, n_cl, False)
    return first, second


def exchange(in1, in2, out1, out2, n_sub, n_cl):
    across = exchange_across(out1, out2, n_cl)
    in2 = swap(in2, "sub", n_sub, False)
    in1 = swap(in1, "sub", n_sub, True)
    return in1, in2, *across


def solve_all(rhs, operators, signs, links, cb, kb, ids, cluster_coarse, gc):
    n_sub = lax.axis_size("sub")
    n_y = lax.axis_size("y")
    n_z = lax.axis_size("z")
    n_cl = n_y * n_z
    cc = cluster_coarse.reshape(NCL, NSUB * NCL)
    message = f32(NSUB, R, MSG)
    picked = ((2 * B, 2 * B), BF16)
    answer = (f32(NSUB, R, B), f32(ROWS, B), f32(R, B))

    w = jnp.concatenate([cb.reshape(NCL, D), kb.reshape(NB - NCL, D)], axis=0)
    msg, v = call(k_coefs, (message, FIELD), ids, rhs, w, cc, smem=(0,))
    recv = to_owner(msg, "sub")
    rows, csol, all_ids = call(
        k_first_rows, (f32(n_y, R, 4 * B), f32(3, R, B), f32(8, B)), recv
    )
    sg, idx, in1 = call(
        k_send_first,
        (FIELD, ((3, ROWS, B), I32), f32(WITHIN, B)),
        all_ids, signs, links.transpose(1, 0, 2), w, v, cc,
    )
    recv = to_owner(rows, "y")
    in1 = swap(in1, "sub", n_sub, True)
    (rows,) = call(k_pass, (f32(n_z, R, 6 * B),), recv)
    recv_z = to_owner(rows, "z")
    *out, in2 = call(k_send_rest, (f32(PACK, B), f32(PACK, B), f32(WITHIN, B)), recv, w, v, cc, idx)
    across = exchange_across(*out, n_cl)
    in2 = swap(in2, "sub", n_sub, False)
    gh, gl = call(k_own_columns, (picked, picked), all_ids, gc)
    to_all, scal0, cacross, ah, al = call(
        k_first_global, (*answer, picked, picked), recv_z, gc, gh, gl
    )
    to_all = to_owner(to_all, "sub")
    pw, pv, d, pd, signed, curv, up, down, *out = call(
        k_first_image,
        (f32(NB, D), FIELD, FIELD, FIELD, FIELD, f32(8, B), *SENDS),
        to_all, csol, cacross, in1, in2, *across,
        w, v, sg, operators, idx,
    )
    got = exchange_across(*out, n_cl)
    across, msg = call(
        k_product,
        (f32(ROWS, B), f32(NSUB, R, MSG + S * B)),
        ids, signed, up, down, *got, in1, in2, w, pw, cc, all_ids, smem=(0,),
    )
    rows, csol, ap, pap = call(
        make_joined(n_cl),
        (f32(n_y, R, D), f32(3, R, B), FIELD, FIELD),
        to_owner(msg, "sub"), signed, across, curv, v,
    )
    (rows,) = call(k_pass, (f32(n_z, R, 4 * B),), to_owner(rows, "y"))
    to_all, _, cacross = call(
        k_global,
        (f32(NSUB, R, 2 * B), f32(ROWS, B), f32(R, B)),
        to_owner(rows, "z"), gh, gl, ah, al,
    )
    r, x, d1, signed, line, *out = call(
        k_last_image,
        (FIELD, FIELD, FIELD, FIELD, f32(n_y * n_sub, 1, B), *SENDS),
        to_owner(to_all, "sub"), csol, cacross, scal0,
        w, pw, v, d, pd, ap, pap, sg, operators, idx,
    )
    line = to_owner(line, ("y", "sub"))
    (line,) = call(k_total, (f32(n_z, 1, B),), line)
    line = to_owner(line, "z")
    got = exchange(*out, n_sub, n_cl)
    out = f32(S, R, D)
    return call(k_finish, (out, out), line, signed, *got, x, r, d1)


def solution(mesh):
    n_y, n_z = 8, 12
    torus = Mesh(mesh.devices.reshape(n_y, n_z, NSUB), ("y", "z", "sub"))
    both = ("y", "z", "sub")
    in_specs = (
        P(both, None, None),
        P(both, None, None),
        P(both, None),
        P(both, None, None),
        P(both, None, None),
        P(both, None, None),
        P(both, None),
        P(CLUSTER, "sub", None),
        P("sub", None),
    )
    out_specs = (P(both, None, None), P(both, None, None))
    return jax.shard_map(solve_all, mesh=torus, in_specs=in_specs, out_specs=out_specs, check_vma=False)
```

```python
import jax
import jax.numpy as jnp
from jax import lax
from jax.experimental import pallas as pl
from jax.experimental.pallas import tpu as pltpu
from jax.sharding import Mesh
from jax.sharding import PartitionSpec as P


F32 = jnp.float32
BF16 = jnp.bfloat16
I32 = jnp.int32
R = 4
S = 4
ROWS = R * S
B = 128
D = 384
KC = 24
NB = 128
NCL = S * KC
CHUNK = 192
NSUB = 8
CLUSTER = ("y", "z")
VMEM_LIMIT = 16 * 2**20


def iota(shape, dim):
    return lax.broadcasted_iota(I32, shape, dim)


def pick(flag, a, b):
    return jnp.where(jnp.full(a.shape, flag.astype(I32), I32) == 1, a, b)


def even_member():
    return lax.axis_index("sub") % 2 == 0


def even_cluster():
    return (lax.axis_index("y") * lax.axis_size("z") + lax.axis_index("z")) % 2 == 0


def split(x):
    hi = x.astype(BF16)
    return hi, (x - hi.astype(F32)).astype(BF16)


def mm(a, b):
    return lax.dot_general(a, b, (((1,), (0,)), ((), ())), preferred_element_type=F32)


def mm_t(a, b):
    return lax.dot_general(a, b, (((1,), (1,)), ((), ())), preferred_element_type=F32)


def dot2(x, w, f=mm):
    n = x.shape[0]
    xh, xl = split(x)
    wh, wl = split(w)
    xs = jnp.concatenate([xh, xl], axis=0)
    both = f(xs, wh)
    return both[:n] + both[n:] + f(xh, wl)


def lanes_of_sub(shape):
    lane = iota(shape, 1)
    return jnp.where(lane < NCL, lane // KC, (lane - NCL) // 8)


def own_mask():
    return iota((ROWS, NB), 0) // R == lanes_of_sub((ROWS, NB))


def by_load(x):
    y = x[:8] + x[8:]
    y = y + pltpu.roll(y, 4, 0)
    return jnp.concatenate([y, y], axis=0)


def coefs(v, w):
    return by_load(jnp.where(own_mask(), dot2(v, w, mm_t), 0.0))


def spread_back(sol, w):
    return dot2(jnp.where(own_mask(), sol, 0.0), w)


def ids_row(ids):
    lane = iota((8, NB), 1)
    row = jnp.full((8, NB), -1, I32)
    for s in range(S):
        for c in range(8):
            row = jnp.where(lane == NCL + 8 * s + c, ids[s, c], row)
    return row


def to_column(row):
    full = jnp.broadcast_to(row[:1], (NB, NB))
    eye = iota((NB, NB), 0) == iota((NB, NB), 1)
    return jnp.sum(jnp.where(eye, full, 0.0), axis=1, keepdims=True)


def window(x, at, width):
    lane = iota((x.shape[0], B), 1)
    tile, off = at // B, at % B
    here = x[:, tile * B : (tile + 1) * B]
    if off:
        here = pltpu.roll(here, B - off, 1)
        if off + width > B:
            after = pltpu.roll(x[:, (tile + 1) * B : (tile + 2) * B], B - off, 1)
            here = jnp.where(lane < B - off, here, after)
    return here


MSG = 5 * B


def clustered(c4, cc):
    return dot2(jnp.where(iota((8, NB), 1) < NCL, c4, 0.0)[:, :NCL], cc)


def marked(scalars):
    lane = iota((8, B), 1)
    extra = jnp.zeros((8, B), F32)
    for j, val in enumerate(scalars):
        extra = jnp.where(lane == 64 + j, val, extra)
    return extra


def write_message(msg, c4, ccp, row, scalars=()):
    col = to_column(row).astype(I32)
    hi, lo = split(c4)
    low = (c4 - hi.astype(F32) - lo.astype(F32)).astype(BF16)
    parts = jnp.concatenate([hi, lo, low], axis=0)
    lane = iota((8, B), 1)
    extra = marked(scalars)
    none = jnp.zeros((8, B), F32)
    cluster = [jnp.where(lane < NCL, window(ccp, NCL * k, NCL), 0.0) for k in range(NSUB)]
    for k in range(NSUB):
        n = iota((NB, 2 * B), 1)
        onehot = jnp.where((col == n + CHUNK * k) & (n < CHUNK), 1.0, 0.0).astype(BF16)
        y = mm(parts, onehot)
        y = y[:8] + y[8:16] + y[16:24]
        tiles = (
            y[:, :B],
            y[:, B:] + extra,
            jnp.where(lane < NCL, cluster[k], row),
            cluster[k + 1] if k + 1 < NSUB else none,
            cluster[k - 1] if k > 0 else none,
        )
        for t, x in enumerate(tiles):
            msg[k, :, t * B : (t + 1) * B] = x[:R]


def row_dot(a, b):
    return by_load(jnp.sum(a * b, axis=1, keepdims=True))


STATIC = NB + ROWS
WITHIN = STATIC + NCL * 6
PACK = 72


def k_coefs(ids, rhs, w, cc, msg, v_out):
    for s in range(S):
        v_out[R * s : R * s + R, :] = rhs[s]
    v = v_out[...]
    c4 = coefs(v, w[...])[:8]
    row = ids_row(ids).astype(F32)
    write_message(msg, c4, clustered(c4, cc[...]), row, [row_dot(v, v)[:8]])


def k_tables(after, signs, links, sg_out, idx_out):
    del after
    pos = iota((8, B), 1).astype(BF16)
    for s in range(S):
        sg_out[R * s : R * s + R, :] = jnp.broadcast_to(signs[s : s + 1, :].astype(F32), (R, D))
        for b in range(3):
            q = links[b, s : s + 1, :]
            if b == 0 or (b == 2 and s % 2 == 0):
                hot = jnp.where(iota((B, B), 0) == q, 1.0, 0.0).astype(BF16)
                q = mm_t(pos, hot)[:1].astype(I32)
            idx_out[b, R * s : R * s + R, :] = jnp.broadcast_to(q, (R, B))


def static_blocks(w, v, idx, b):
    lanes = pl.ds(pl.multiple_of(b * B, B), B)

    def moved(x, q):
        return jnp.take_along_axis(x, jnp.broadcast_to(q, x.shape), axis=1)

    for s in range(S):
        q = idx[b, R * s : R * s + 1, :]
        for at, n in ((KC * s, KC), (NCL + 8 * s, 8)):
            yield s, at, moved(w[at : at + n, lanes], q)
    yield None, NB, moved(v[:, lanes], idx[b])


def send_within(w, v, cc, idx, out, b):
    for _, at, x in static_blocks(w, v, idx, b):
        out[at : at + x.shape[0], :] = x
    for j in range(6):
        out[STATIC + NCL * j : STATIC + NCL * j + NCL, :] = cc[:, j * B : (j + 1) * B]


def coarse_rows(x):
    return jnp.concatenate([x[STATIC + NCL * j : STATIC + NCL * j + NCL, :] for j in range(6)], axis=1)


def k_send_first(after, signs, links, w, v, cc, sg_out, idx_out, first, second):
    k_tables(after, signs, links, sg_out, idx_out)
    odd = lax.axis_index("sub") % 2
    send_within(w, v, cc, idx_out, first, odd)
    send_within(w, v, cc, idx_out, second, 1 - odd)


def k_send_across(after, w, v, idx, first, second):
    del after
    flag = even_cluster()
    blocks = {(s, at): x for s, at, x in static_blocks(w, v, idx, 2)}

    def put(to, even, odd):
        n = even.shape[0]
        first[to : to + n, :] = pick(flag, even, odd)
        second[to : to + n, :] = pick(flag, odd, even)

    for h in range(2):
        s = 2 * h
        put(KC * h, blocks[s, KC * s], blocks[s + 1, KC * (s + 1)])
        put(2 * KC + 8 * h, blocks[s, NCL + 8 * s], blocks[s + 1, NCL + 8 * s + 8])
        x = blocks[None, NB][8 * h : 8 * h + 8]
        put(2 * KC + 16 + R * h, x[:R], x[R:])


def moved_blocks(v, idx):
    up, down, across = (
        jnp.take_along_axis(v[:, b * B : (b + 1) * B], idx[b], axis=1) for b in range(3)
    )
    even = jnp.concatenate([across[0:R], across[8 : 8 + R]], axis=0)
    odd = jnp.concatenate([across[R:8], across[8 + R :]], axis=0)
    return up, down, even, odd


def write_across(even, odd, first, second):
    flag = even_cluster()
    first[...] = pick(flag, even, odd)
    second[...] = pick(flag, odd, even)


def write_moved(v, idx, in1, in2, out1, out2):
    up, down, even, odd = moved_blocks(v, idx)
    flag = even_member()
    in1[...] = pick(flag, up, down)
    in2[...] = pick(flag, down, up)
    write_across(even, odd, out1, out2)


def across_of(out1, out2):
    flag = even_cluster()
    return pick(flag, out1, out2), pick(flag, out2, out1)


def within_of(in1, in2):
    flag = even_member()
    return pick(flag, in1, in2), pick(flag, in2, in1)


def take_static(in1, in2, out1, out2, pw_out, pv_out):
    from_next, from_prev = within_of(in1[0:STATIC, :], in2[0:STATIC, :])
    odd_in, even_in = across_of(out1[...], out2[...])
    pw_out[:, 0:B] = from_next[0:NB, :]
    pw_out[:, B : 2 * B] = from_prev[0:NB, :]
    for s in range(S):
        h = s // 2
        side = even_in if s % 2 else odd_in
        pw_out[KC * s : KC * s + KC, 2 * B :] = side[KC * h : KC * h + KC, :]
        at = 2 * KC + 8 * h
        pw_out[NCL + 8 * s : NCL + 8 * s + 8, 2 * B :] = side[at : at + 8, :]
        at = 2 * KC + 16 + R * h
        pv_out[R * s : R * s + R, 2 * B :] = side[at : at + R, :]
    pv_out[:, 0:B] = from_next[NB:STATIC, :]
    pv_out[:, B : 2 * B] = from_prev[NB:STATIC, :]


def member_sum(recv):
    total = recv[0]
    for k in range(1, NSUB):
        total = total + recv[k]
    return total


def k_rows(recv, out, csol, scalars=()):
    total = recv[0, :, 0:MSG]
    for k in range(1, NSUB):
        total = total + recv[k, :, 0:MSG]
    own = jnp.where(iota((R, B), 1) < NCL, total[:, 2 * B : 3 * B], 0.0)
    csol[0] = own
    csol[1] = total[:, 3 * B : 4 * B]
    csol[2] = total[:, 4 * B : 5 * B]
    second = total[:, B : 2 * B] + marked(scalars)[:R]
    x = jnp.concatenate([total[:, :B], second, own], axis=1)
    out[:, :, 0:D] = jnp.broadcast_to(x[None], (out.shape[0], R, D))


def cluster_ids(recv):
    lane = iota((8, B), 1)
    rows = []
    for half in range(2):
        ids = jnp.zeros((8, B), F32)
        for j in range(4):
            row = recv[4 * half + j, 0:1, 2 * B : 3 * B]
            row = pltpu.roll(jnp.broadcast_to(row, (8, B)), (32 + 32 * j) % B, 1)
            ids = jnp.where(lane // 32 == j, row, ids)
        rows.append(ids)
    return rows


def k_first_rows(recv, out, csol, ids_out):
    k_rows(recv, out, csol)
    low, high = cluster_ids(recv)
    ids = jnp.where(iota((8, B), 0) == 0, low, high)
    ids_out[...] = ids
    out[:, :, D:] = jnp.broadcast_to(ids[None, :R], (out.shape[0], R, B))


def k_pass(recv, out):
    y, z = lax.axis_index("y"), lax.axis_index("z")
    n_y, n_z = recv.shape[0], out.shape[0]
    total = jnp.sum(recv[:, :, 0 : 2 * B], axis=0)
    other = jnp.where(z == 0, jnp.minimum(y + 1, n_y - 1), jnp.maximum(y - 1, 0))
    x = jnp.concatenate([total, recv[y, :, 2 * B :], recv[other, :, 2 * B :]], axis=1)
    out[...] = jnp.broadcast_to(x[None], (n_z, *x.shape))


def neighbours(recv, at, wrapped_at):
    z = lax.axis_index("z")
    n_z = recv.shape[0]
    last, first = z == n_z - 1, z == 0
    nxt = recv[jnp.where(last, 0, z + 1)]
    prv = recv[jnp.where(first, n_z - 1, z - 1)]

    def tile(x, use_wrapped):
        plain = x[:, at : at + B]
        wrapped = x[:, wrapped_at : wrapped_at + B]
        x = jnp.where(jnp.full((R, B), use_wrapped.astype(I32), I32) == 1, wrapped, plain)
        return jnp.concatenate([x, x], axis=0)

    return tile(nxt, last), tile(prv, first)


def picked_columns(gc, rows, hi_out, lo_out):
    ids = jnp.concatenate([x[:1].astype(I32) for x in rows], axis=1)
    n = iota((gc.shape[1], ids.shape[1]), 0)
    onehot = jnp.where(n == ids, 1.0, 0.0).astype(BF16)
    gh, gl = split(gc[...])
    zero = jnp.zeros((2 * B - CHUNK, ids.shape[1]), BF16)
    hi_out[0:CHUNK, :] = mm(gh, onehot).astype(BF16)
    hi_out[CHUNK : 2 * B, :] = zero
    lo_out[0:CHUNK, :] = mm(gl, onehot).astype(BF16)
    lo_out[CHUNK : 2 * B, :] = zero


def solve(recv, parts, msg, scal, cacross, stride):
    total = jnp.sum(recv[:, :, 0 : 2 * B], axis=0)
    total = jnp.concatenate([total, total], axis=0)
    second = total[:, B:]
    lane = iota((8, B), 1)
    x = jnp.concatenate([total[:, :B], jnp.where(lane < 64, second, 0.0)], axis=1)
    xh, xl = split(x)
    ys = []
    for gh, gl in parts:
        y = mm(jnp.concatenate([xh, xl], axis=0), gh[...])
        ys.append(y[:8] + y[8:] + mm(xh, gl[...]))

    def picked(kind, k, to):
        at = 32 * k
        return pltpu.roll(ys[kind][:, at // B * B : at // B * B + B], (to - at) % B, 1)

    none = jnp.zeros((8, B), F32)
    for k in range(NSUB):
        after = picked(0, k + 1, 32) if k + 1 < NSUB else none
        before = picked(0, k - 1, 64) if k > 0 else none
        here = jnp.where(lane < 32, picked(0, k, 0), jnp.where(lane < 64, after, before))
        msg[k, :, 0:B] = jnp.where(lane < 96, here, picked(1, k, 96))[:R]
        if msg.shape[2] > B:
            msg[k, :, B : 2 * B] = second[:R]
    scal[...] = jnp.concatenate([second, second], axis=0)
    after, before = neighbours(recv, 2 * B, 2 * B + stride)
    after = pltpu.roll(after, B - KC, 1)
    before = pltpu.roll(before, KC, 1)
    both = jnp.where(lane // KC % 2 == 0, after, before)
    cacross[...] = jnp.where(lane < NCL, both, 0.0)[:R]


def k_first_global(recv, own, gc, msg, scal, cacross, gh, gl, ah, al):
    picked_columns(gc, [own[0:1, :], own[1:2, :]], gh, gl)
    after, before = neighbours(recv, 3 * B, 5 * B)
    lane = iota((8, B), 1)
    after = pltpu.roll(after, B - 8, 1)
    before = pltpu.roll(before, 8, 1)
    ids = jnp.where(lane // 8 % 2 == 0, after, before)
    picked_columns(gc, [ids[0:1], ids[1:2]], ah, al)
    solve(recv, ((gh, gl), (ah, al)), msg, scal, cacross, 2 * B)


def k_global(recv, gh, gl, ah, al, msg, scal, cacross):
    solve(recv, ((gh, gl), (ah, al)), msg, scal, cacross, B)


def four_times(x):
    x = jnp.concatenate([x, x], axis=0)
    return jnp.concatenate([x, x], axis=0)


def corrections(recv, csol, cacross, w, pw):
    picks = four_times(member_sum(recv)[:, :B])
    tail = iota((ROWS, B), 1) >= NCL

    def sol(cluster, turn):
        p = pltpu.roll(picks, turn, 1) if turn else picks
        return jnp.where(tail, p, four_times(cluster))

    own = spread_back(sol(csol[0], 96), w[...])
    sides = (sol(csol[1], 64), sol(csol[2], 32), sol(cacross[...], 0))
    pi = [spread_back(x, pw[:, b * B : (b + 1) * B]) for b, x in enumerate(sides)]
    return own, jnp.concatenate(pi, axis=1)


def across_received(out1, out2):
    odd_in, even_in = across_of(out1[...], out2[...])
    return jnp.concatenate([odd_in[0:R], even_in[0:R], odd_in[R:], even_in[R:]], axis=0)


def received(from_next, from_prev, out1, out2):
    return jnp.concatenate([from_next, from_prev, across_received(out1, out2)], axis=1)


def paired(n_cl):
    c, k = lax.axis_index("y") * lax.axis_size("z") + lax.axis_index("z"), lax.axis_index("sub")
    lane = iota((ROWS, D), 1)
    is_even = iota((ROWS, D), 0) // R % 2 == 0
    yes = [
        jnp.where(x, 1.0, 0.0) for x in (k < NSUB - 1, k > 0, c < n_cl - 1, c > 0)
    ]
    across = jnp.where(is_even, yes[2], yes[3])
    return jnp.where(lane < B, yes[0], jnp.where(lane < 2 * B, yes[1], across))


def image_of(d, pd, sg, ops):
    spread = sg * (d + pd)
    low = spread.astype(BF16)
    image = jnp.zeros((ROWS, D), F32)
    row = iota((ROWS, D), 0) // R
    for s in range(S):
        image = jnp.where(row == s, mm(low, ops[s]), image)
    return sg * image, row_dot(spread, image)


def k_first_image(
    recv, csol, cacross, in1, in2, out1, out2, w, v, sg, ops, idx,
    pw, pv, d_out, pd_out, signed_out, curv, up_out, down_out, *outs,
):
    take_static(in1, in2, out1, out2, pw, pv)
    fix, pfix = corrections(recv, csol, cacross, w, pw)
    d = v[...] - fix
    pd = pv[...] - pfix
    d_out[...] = d
    pd_out[...] = pd
    signed, c = image_of(d, pd, sg[...], ops)
    signed_out[...] = signed
    curv[...] = jnp.broadcast_to(c[:8], (8, B))
    up, down, even, odd = moved_blocks(signed, idx)
    up_out[...] = up
    down_out[...] = down
    write_across(even, odd, *outs)


def member_ids(all_ids, member, to):
    row = jnp.zeros((8, B), F32)
    which = jnp.full((8, B), member, I32)
    for j in range(NSUB):
        x = jnp.broadcast_to(all_ids[j // 4 : j // 4 + 1, :], (8, B))
        row = jnp.where(which == j, pltpu.roll(x, (to - 32 * (j % 4)) % B, 1), row)
    return row


def k_product(
    ids, signed, up, down, out1, out2, static1, static2, w, pw, cc, all_ids, across_out, msg
):
    k = lax.axis_index("sub")
    odd_k = k % 2
    across = across_received(out1, out2)
    across_out[...] = across
    u = signed[...]
    known = jnp.concatenate([u[:, : 2 * B], u[:, 2 * B :] + across], axis=1)
    own = coefs(known, w[...])[:8]

    def towards(b):
        lanes = pl.ds(pl.multiple_of(b * B, B), B)
        return coefs(signed[:, lanes], pw[:, lanes])[:8]

    first, second = towards(odd_k), towards(1 - odd_k)
    ccp = (
        clustered(own, cc[...])
        + clustered(first, coarse_rows(static1))
        + clustered(second, coarse_rows(static2))
    )
    lane = iota((8, B), 1)
    other = jnp.clip(k - 1 + 2 * odd_k, 0, NSUB - 1)

    def lanes_of(c96, c64, c32, rest):
        return jnp.where(
            lane >= 96, c96, jnp.where(lane >= 64, c64, jnp.where(lane >= 32, c32, rest))
        )

    c4 = lanes_of(own, pltpu.roll(first, B - 32, 1), pltpu.roll(second, B - 64, 1), 0.0)
    row = lanes_of(
        ids_row(ids).astype(F32),
        member_ids(all_ids, k + 1 - 2 * odd_k, 64),
        member_ids(all_ids, other, 32),
        -1.0,
    )
    write_message(msg, c4, ccp, row)
    after, before = jnp.minimum(k + 1, NSUB - 1), jnp.maximum(k - 1, 0)
    for s in range(S):
        at = MSG + B * s
        msg[after, :, at : at + B] = up[R * s : R * s + R, :]
        msg[before, :, at : at + B] = down[R * s : R * s + R, :]


def make_joined(n_cl):
    def k_joined(recv, signed, across, curv, v, out, csol, ap_out, pap_out):
        k = lax.axis_index("sub")

        def block(member, there):
            x = [recv[member, :, MSG + B * s : MSG + B * s + B] for s in range(S)]
            x = jnp.concatenate(x, axis=0)
            return pick(there, x, jnp.zeros_like(x))

        from_next = block(jnp.minimum(k + 1, NSUB - 1), k < NSUB - 1)
        from_prev = block(jnp.maximum(k - 1, 0), k > 0)
        u = signed[...]
        pi = jnp.concatenate([from_next, from_prev, across[...]], axis=1)
        ap = u + pi
        ap_out[...] = ap
        pap_out[...] = pi + paired(n_cl) * u
        scalars = [curv[...][:, :1], row_dot(v[...], ap)[:8], row_dot(ap, ap)[:8]]
        k_rows(recv, out, csol, scalars)

    return k_joined


def scalar_at(scal, j):
    return jnp.sum(jnp.where(iota((ROWS, B), 1) == 64 + j, scal, 0.0), axis=1, keepdims=True)


def k_last_image(
    recv, csol, cacross, scal0, w, pw, v, d, pd, ap, pap, sg, ops, idx,
    r_out, x_out, d_out, signed_out, msg, *outs,
):
    fix, pfix = corrections(recv, csol, cacross, w, pw)
    rho = scalar_at(scal0[...], 0)
    s1 = four_times(member_sum(recv)[:, B : 2 * B])
    step = rho / scalar_at(s1, 0)
    rho_new = rho - 2.0 * step * scalar_at(s1, 1) + step * step * scalar_at(s1, 2)
    beta = rho_new / rho
    ap_ = ap[...]
    d0 = d[...]
    pd0 = pd[...]
    r = v[...] - step * ap_
    r_out[...] = r
    x_out[...] = step * d0
    d1 = d0 - step * (ap_ - fix) + beta * d0
    pd1 = pd0 - step * (pap[...] - pfix) + beta * pd0
    d_out[...] = d1
    signed, c = image_of(d1, pd1, sg[...], ops)
    signed_out[...] = signed
    sq = row_dot(r, r)
    lane = iota((8, B), 1)
    row = iota((8, B), 0)
    both = jnp.where(lane == row, c[:8], jnp.where(lane == row + R, sq[:8], 0.0))
    line = jnp.sum(jnp.where(row < R, both, 0.0), axis=0, keepdims=True)
    msg[...] = jnp.broadcast_to(line[None], msg.shape)
    write_moved(signed, idx, *outs)


def k_total(recv, out):
    out[...] = jnp.broadcast_to(jnp.sum(recv[...], axis=0, keepdims=True), out.shape)


def k_finish(recv, signed, in1, in2, out1, out2, x, r, d, x_out, r_out):
    line = jnp.broadcast_to(jnp.sum(recv[...], axis=0), (ROWS, B))
    lane = iota((ROWS, B), 1)
    row = iota((ROWS, B), 0) % R
    curv = jnp.sum(jnp.where(lane == row, line, 0.0), axis=1, keepdims=True)
    rho = jnp.sum(jnp.where(lane == row + R, line, 0.0), axis=1, keepdims=True)
    step = rho / curv
    xn = x[...] + step * d[...]
    pi = received(*within_of(in1[...], in2[...]), out1, out2)
    rn = r[...] - step * (signed[...] + pi)
    for s in range(S):
        x_out[s] = xn[R * s : R * s + R]
        r_out[s] = rn[R * s : R * s + R]


def call(body, outs, *args, smem=(), scratch=()):
    def space(i):
        return pltpu.SMEM if i in smem else pltpu.VMEM

    specs = [pl.BlockSpec(memory_space=space(i)) for i in range(len(args))]
    out_shape = tuple(jax.ShapeDtypeStruct(s, t) for s, t in outs)
    return pl.pallas_call(
        body,
        out_shape=out_shape,
        in_specs=specs,
        out_specs=tuple(pl.BlockSpec(memory_space=pltpu.VMEM) for _ in outs),
        scratch_shapes=scratch,
        compiler_params=pltpu.CompilerParams(vmem_limit_bytes=VMEM_LIMIT),
    )(*args)


def to_owner(x, axis):
    return lax.all_to_all(x, axis, 0, 0, tiled=True)


def f32(*shape):
    return (shape, F32)


FIELD = f32(ROWS, D)


SENDS = (f32(ROWS, B), f32(ROWS, B), f32(2 * R, B), f32(2 * R, B))


def swap(x, axis, n, first):
    low = range(0 if first else 1, n - 1, 2)
    return lax.ppermute(x, axis, [p for i in low for p in ((i, i + 1), (i + 1, i))])


def exchange_across(first, second, n_cl):
    first = swap(first, CLUSTER, n_cl, True)
    second = swap(second, CLUSTER, n_cl, False)
    return first, second


def exchange(in1, in2, out1, out2, n_sub, n_cl):
    across = exchange_across(out1, out2, n_cl)
    in2 = swap(in2, "sub", n_sub, False)
    in1 = swap(in1, "sub", n_sub, True)
    return in1, in2, *across


def solve_all(rhs, operators, signs, links, cb, kb, ids, cluster_coarse, gc):
    n_sub = lax.axis_size("sub")
    n_y = lax.axis_size("y")
    n_z = lax.axis_size("z")
    n_cl = n_y * n_z
    cc = cluster_coarse.reshape(NCL, NSUB * NCL)
    message = f32(NSUB, R, MSG)
    picked = ((2 * B, 2 * B), BF16)
    answer = (f32(NSUB, R, B), f32(ROWS, B), f32(R, B))

    w = jnp.concatenate([cb.reshape(NCL, D), kb.reshape(NB - NCL, D)], axis=0)
    msg, v = call(k_coefs, (message, FIELD), ids, rhs, w, cc, smem=(0,))
    recv = to_owner(msg, "sub")
    rows, csol, all_ids = call(
        k_first_rows, (f32(n_y, R, 4 * B), f32(3, R, B), f32(8, B)), recv
    )
    sg, idx, in1, in2 = call(
        k_send_first,
        (FIELD, ((3, ROWS, B), I32), f32(WITHIN, B), f32(WITHIN, B)),
        all_ids, signs, links.transpose(1, 0, 2), w, v, cc,
    )
    recv = to_owner(rows, "y")
    in1 = swap(in1, "sub", n_sub, True)
    in2 = swap(in2, "sub", n_sub, False)
    (rows,) = call(k_pass, (f32(n_z, R, 6 * B),), recv)
    recv_z = to_owner(rows, "z")
    out = call(k_send_across, (f32(PACK, B), f32(PACK, B)), recv, w, v, idx)
    across = exchange_across(*out, n_cl)
    to_all, scal0, cacross, gh, gl, ah, al = call(
        k_first_global, (*answer, picked, picked, picked, picked), recv_z, all_ids, gc
    )
    to_all = to_owner(to_all, "sub")
    pw, pv, d, pd, signed, curv, up, down, *out = call(
        k_first_image,
        (f32(NB, D), FIELD, FIELD, FIELD, FIELD, f32(8, B), *SENDS),
        to_all, csol, cacross, in1, in2, *across,
        w, v, sg, operators, idx,
    )
    got = exchange_across(*out, n_cl)
    across, msg = call(
        k_product,
        (f32(ROWS, B), f32(NSUB, R, MSG + S * B)),
        ids, signed, up, down, *got, in1, in2, w, pw, cc, all_ids, smem=(0,),
    )
    rows, csol, ap, pap = call(
        make_joined(n_cl),
        (f32(n_y, R, D), f32(3, R, B), FIELD, FIELD),
        to_owner(msg, "sub"), signed, across, curv, v,
    )
    (rows,) = call(k_pass, (f32(n_z, R, 4 * B),), to_owner(rows, "y"))
    to_all, _, cacross = call(
        k_global,
        (f32(NSUB, R, 2 * B), f32(ROWS, B), f32(R, B)),
        to_owner(rows, "z"), gh, gl, ah, al,
    )
    r, x, d1, signed, line, *out = call(
        k_last_image,
        (FIELD, FIELD, FIELD, FIELD, f32(n_y * n_sub, 1, B), *SENDS),
        to_owner(to_all, "sub"), csol, cacross, scal0,
        w, pw, v, d, pd, ap, pap, sg, operators, idx,
    )
    line = to_owner(line, ("y", "sub"))
    (line,) = call(k_total, (f32(n_z, 1, B),), line)
    line = to_owner(line, "z")
    got = exchange(*out, n_sub, n_cl)
    out = f32(S, R, D)
    return call(k_finish, (out, out), line, signed, *got, x, r, d1)


def solution(mesh):
    n_y, n_z = 8, 12
    torus = Mesh(mesh.devices.reshape(n_y, n_z, NSUB), ("y", "z", "sub"))
    both = ("y", "z", "sub")
    in_specs = (
        P(both, None, None),
        P(both, None, None),
        P(both, None),
        P(both, None, None),
        P(both, None, None),
        P(both, None, None),
        P(both, None),
        P(CLUSTER, "sub", None),
        P("sub", None),
    )
    out_specs = (P(both, None, None), P(both, None, None))
    return jax.shard_map(solve_all, mesh=torus, in_specs=in_specs, out_specs=out_specs, check_vma=False)
```

```python
import jax
import jax.numpy as jnp
from jax import lax
from jax.experimental import pallas as pl
from jax.experimental.pallas import tpu as pltpu
from jax.sharding import Mesh
from jax.sharding import PartitionSpec as P


F32 = jnp.float32
BF16 = jnp.bfloat16
I32 = jnp.int32
R = 4
S = 4
ROWS = R * S
B = 128
D = 384
KC = 24
NB = 128
NCL = S * KC
CHUNK = 192
NSUB = 8
CLUSTER = ("y", "z")
VMEM_LIMIT = 16 * 2**20


def iota(shape, dim):
    return lax.broadcasted_iota(I32, shape, dim)


def pick(flag, a, b):
    return jnp.where(jnp.full(a.shape, flag.astype(I32), I32) == 1, a, b)


def even_member():
    return lax.axis_index("sub") % 2 == 0


def even_cluster():
    return (lax.axis_index("y") * lax.axis_size("z") + lax.axis_index("z")) % 2 == 0


def split(x):
    hi = x.astype(BF16)
    return hi, (x - hi.astype(F32)).astype(BF16)


def mm(a, b):
    return lax.dot_general(a, b, (((1,), (0,)), ((), ())), preferred_element_type=F32)


def mm_t(a, b):
    return lax.dot_general(a, b, (((1,), (1,)), ((), ())), preferred_element_type=F32)


def dot2(x, w, f=mm):
    n = x.shape[0]
    xh, xl = split(x)
    wh, wl = split(w)
    xs = jnp.concatenate([xh, xl], axis=0)
    both = f(xs, wh)
    return both[:n] + both[n:] + f(xh, wl)


def lanes_of_sub(shape):
    lane = iota(shape, 1)
    return jnp.where(lane < NCL, lane // KC, (lane - NCL) // 8)


def own_mask():
    return iota((ROWS, NB), 0) // R == lanes_of_sub((ROWS, NB))


def by_load(x):
    y = x[:8] + x[8:]
    y = y + pltpu.roll(y, 4, 0)
    return jnp.concatenate([y, y], axis=0)


def coefs(v, w):
    return by_load(jnp.where(own_mask(), dot2(v, w, mm_t), 0.0))


def spread_back(sol, w):
    return dot2(jnp.where(own_mask(), sol, 0.0), w)


def ids_row(ids):
    lane = iota((8, NB), 1)
    row = jnp.full((8, NB), -1, I32)
    for s in range(S):
        for c in range(8):
            row = jnp.where(lane == NCL + 8 * s + c, ids[s, c], row)
    return row


def to_column(row):
    full = jnp.broadcast_to(row[:1], (NB, NB))
    eye = iota((NB, NB), 0) == iota((NB, NB), 1)
    return jnp.sum(jnp.where(eye, full, 0.0), axis=1, keepdims=True)


def window(x, at, width):
    lane = iota((x.shape[0], B), 1)
    tile, off = at // B, at % B
    here = x[:, tile * B : (tile + 1) * B]
    if off:
        here = pltpu.roll(here, B - off, 1)
        if off + width > B:
            after = pltpu.roll(x[:, (tile + 1) * B : (tile + 2) * B], B - off, 1)
            here = jnp.where(lane < B - off, here, after)
    return here


MSG = 5 * B


def clustered(c4, cc):
    return dot2(jnp.where(iota((8, NB), 1) < NCL, c4, 0.0)[:, :NCL], cc)


def marked(scalars):
    lane = iota((8, B), 1)
    extra = jnp.zeros((8, B), F32)
    for j, val in enumerate(scalars):
        extra = jnp.where(lane == 64 + j, val, extra)
    return extra


def write_message(msg, c4, ccp, row, scalars=()):
    col = to_column(row).astype(I32)
    hi, lo = split(c4)
    low = (c4 - hi.astype(F32) - lo.astype(F32)).astype(BF16)
    parts = jnp.concatenate([hi, lo, low], axis=0)
    lane = iota((8, B), 1)
    extra = marked(scalars)
    none = jnp.zeros((8, B), F32)
    cluster = [jnp.where(lane < NCL, window(ccp, NCL * k, NCL), 0.0) for k in range(NSUB)]
    for k in range(NSUB):
        n = iota((NB, 2 * B), 1)
        onehot = jnp.where((col == n + CHUNK * k) & (n < CHUNK), 1.0, 0.0).astype(BF16)
        y = mm(parts, onehot)
        y = y[:8] + y[8:16] + y[16:24]
        tiles = (
            y[:, :B],
            y[:, B:] + extra,
            jnp.where(lane < NCL, cluster[k], row),
            cluster[k + 1] if k + 1 < NSUB else none,
            cluster[k - 1] if k > 0 else none,
        )
        for t, x in enumerate(tiles):
            msg[k, :, t * B : (t + 1) * B] = x[:R]


def row_dot(a, b):
    return by_load(jnp.sum(a * b, axis=1, keepdims=True))


STATIC = NB + ROWS
WITHIN = STATIC + NCL * 6
PACK = 72


def k_coefs(ids, rhs, w, cc, msg, v_out):
    for s in range(S):
        v_out[R * s : R * s + R, :] = rhs[s]
    v = v_out[...]
    c4 = coefs(v, w[...])[:8]
    row = ids_row(ids).astype(F32)
    write_message(msg, c4, clustered(c4, cc[...]), row, [row_dot(v, v)[:8]])


def k_tables(after, signs, links, sg_out, idx_out):
    del after
    pos = iota((8, B), 1).astype(BF16)
    for s in range(S):
        sg_out[R * s : R * s + R, :] = jnp.broadcast_to(signs[s : s + 1, :].astype(F32), (R, D))
        for b in range(3):
            q = links[b, s : s + 1, :]
            if b == 0 or (b == 2 and s % 2 == 0):
                hot = jnp.where(iota((B, B), 0) == q, 1.0, 0.0).astype(BF16)
                q = mm_t(pos, hot)[:1].astype(I32)
            idx_out[b, R * s : R * s + R, :] = jnp.broadcast_to(q, (R, B))


def static_blocks(w, v, idx, b):
    lanes = pl.ds(pl.multiple_of(b * B, B), B)

    def moved(x, q):
        return jnp.take_along_axis(x, jnp.broadcast_to(q, x.shape), axis=1)

    for s in range(S):
        q = idx[b, R * s : R * s + 1, :]
        for at, n in ((KC * s, KC), (NCL + 8 * s, 8)):
            yield s, at, moved(w[at : at + n, lanes], q)
    yield None, NB, moved(v[:, lanes], idx[b])


def send_within(w, v, cc, idx, out, b):
    for _, at, x in static_blocks(w, v, idx, b):
        out[at : at + x.shape[0], :] = x
    for j in range(6):
        out[STATIC + NCL * j : STATIC + NCL * j + NCL, :] = cc[:, j * B : (j + 1) * B]


def coarse_rows(x):
    return jnp.concatenate([x[STATIC + NCL * j : STATIC + NCL * j + NCL, :] for j in range(6)], axis=1)


def k_send_static(after, signs, links, w, v, cc, sg_out, idx_out, within, out1, out2):
    k_tables(after, signs, links, sg_out, idx_out)
    send_within(w, v, cc, idx_out, within, 1 - lax.axis_index("sub") % 2)
    send_across(w, v, idx_out, out1, out2)


def k_send_chip(after, w, v, cc, idx, within):
    del after
    send_within(w, v, cc, idx, within, lax.axis_index("sub") % 2)


def send_across(w, v, idx, first, second):
    flag = even_cluster()
    blocks = {(s, at): x for s, at, x in static_blocks(w, v, idx, 2)}

    def put(to, even, odd):
        n = even.shape[0]
        first[to : to + n, :] = pick(flag, even, odd)
        second[to : to + n, :] = pick(flag, odd, even)

    for h in range(2):
        s = 2 * h
        put(KC * h, blocks[s, KC * s], blocks[s + 1, KC * (s + 1)])
        put(2 * KC + 8 * h, blocks[s, NCL + 8 * s], blocks[s + 1, NCL + 8 * s + 8])
        x = blocks[None, NB][8 * h : 8 * h + 8]
        put(2 * KC + 16 + R * h, x[:R], x[R:])


def moved_blocks(v, idx):
    up, down, across = (
        jnp.take_along_axis(v[:, b * B : (b + 1) * B], idx[b], axis=1) for b in range(3)
    )
    even = jnp.concatenate([across[0:R], across[8 : 8 + R]], axis=0)
    odd = jnp.concatenate([across[R:8], across[8 + R :]], axis=0)
    return up, down, even, odd


def write_across(even, odd, first, second):
    flag = even_cluster()
    first[...] = pick(flag, even, odd)
    second[...] = pick(flag, odd, even)


def write_moved(v, idx, in1, in2, out1, out2):
    up, down, even, odd = moved_blocks(v, idx)
    flag = even_member()
    in1[...] = pick(flag, up, down)
    in2[...] = pick(flag, down, up)
    write_across(even, odd, out1, out2)


def across_of(out1, out2):
    flag = even_cluster()
    return pick(flag, out1, out2), pick(flag, out2, out1)


def within_of(in1, in2):
    flag = even_member()
    return pick(flag, in1, in2), pick(flag, in2, in1)


def take_static(in1, in2, out1, out2, pw_out, pv_out):
    from_next, from_prev = within_of(in1[0:STATIC, :], in2[0:STATIC, :])
    odd_in, even_in = across_of(out1[...], out2[...])
    pw_out[:, 0:B] = from_next[0:NB, :]
    pw_out[:, B : 2 * B] = from_prev[0:NB, :]
    for s in range(S):
        h = s // 2
        side = even_in if s % 2 else odd_in
        pw_out[KC * s : KC * s + KC, 2 * B :] = side[KC * h : KC * h + KC, :]
        at = 2 * KC + 8 * h
        pw_out[NCL + 8 * s : NCL + 8 * s + 8, 2 * B :] = side[at : at + 8, :]
        at = 2 * KC + 16 + R * h
        pv_out[R * s : R * s + R, 2 * B :] = side[at : at + R, :]
    pv_out[:, 0:B] = from_next[NB:STATIC, :]
    pv_out[:, B : 2 * B] = from_prev[NB:STATIC, :]


def member_sum(recv):
    total = recv[0]
    for k in range(1, NSUB):
        total = total + recv[k]
    return total


def k_rows(recv, out, csol, scalars=()):
    total = recv[0, :, 0:MSG]
    for k in range(1, NSUB):
        total = total + recv[k, :, 0:MSG]
    own = jnp.where(iota((R, B), 1) < NCL, total[:, 2 * B : 3 * B], 0.0)
    csol[0] = own
    csol[1] = total[:, 3 * B : 4 * B]
    csol[2] = total[:, 4 * B : 5 * B]
    second = total[:, B : 2 * B] + marked(scalars)[:R]
    x = jnp.concatenate([total[:, :B], second, own], axis=1)
    out[:, :, 0:D] = jnp.broadcast_to(x[None], (out.shape[0], R, D))


def cluster_ids(recv):
    lane = iota((8, B), 1)
    rows = []
    for half in range(2):
        ids = jnp.zeros((8, B), F32)
        for j in range(4):
            row = recv[4 * half + j, 0:1, 2 * B : 3 * B]
            row = pltpu.roll(jnp.broadcast_to(row, (8, B)), (32 + 32 * j) % B, 1)
            ids = jnp.where(lane // 32 == j, row, ids)
        rows.append(ids)
    return rows


def k_first_rows(recv, out, csol, ids_out):
    k_rows(recv, out, csol)
    low, high = cluster_ids(recv)
    ids = jnp.where(iota((8, B), 0) == 0, low, high)
    ids_out[...] = ids
    out[:, :, D:] = jnp.broadcast_to(ids[None, :R], (out.shape[0], R, B))


def k_pass(recv, out):
    y, z = lax.axis_index("y"), lax.axis_index("z")
    n_y, n_z = recv.shape[0], out.shape[0]
    total = jnp.sum(recv[:, :, 0 : 2 * B], axis=0)
    other = jnp.where(z == 0, jnp.minimum(y + 1, n_y - 1), jnp.maximum(y - 1, 0))
    x = jnp.concatenate([total, recv[y, :, 2 * B :], recv[other, :, 2 * B :]], axis=1)
    out[...] = jnp.broadcast_to(x[None], (n_z, *x.shape))


def neighbours(recv, at, wrapped_at):
    z = lax.axis_index("z")
    n_z = recv.shape[0]
    last, first = z == n_z - 1, z == 0
    nxt = recv[jnp.where(last, 0, z + 1)]
    prv = recv[jnp.where(first, n_z - 1, z - 1)]

    def tile(x, use_wrapped):
        plain = x[:, at : at + B]
        wrapped = x[:, wrapped_at : wrapped_at + B]
        x = jnp.where(jnp.full((R, B), use_wrapped.astype(I32), I32) == 1, wrapped, plain)
        return jnp.concatenate([x, x], axis=0)

    return tile(nxt, last), tile(prv, first)


def picked_columns(gc, rows, hi_out, lo_out):
    ids = jnp.concatenate([x[:1].astype(I32) for x in rows], axis=1)
    n = iota((gc.shape[1], ids.shape[1]), 0)
    onehot = jnp.where(n == ids, 1.0, 0.0).astype(BF16)
    gh, gl = split(gc[...])
    zero = jnp.zeros((2 * B - CHUNK, ids.shape[1]), BF16)
    hi_out[0:CHUNK, :] = mm(gh, onehot).astype(BF16)
    hi_out[CHUNK : 2 * B, :] = zero
    lo_out[0:CHUNK, :] = mm(gl, onehot).astype(BF16)
    lo_out[CHUNK : 2 * B, :] = zero


def solve(recv, parts, msg, cacross, stride):
    total = jnp.sum(recv[:, :, 0 : 2 * B], axis=0)
    total = jnp.concatenate([total, total], axis=0)
    second = total[:, B:]
    lane = iota((8, B), 1)
    x = jnp.concatenate([total[:, :B], jnp.where(lane < 64, second, 0.0)], axis=1)
    xh, xl = split(x)
    ys = []
    for gh, gl in parts:
        y = mm(jnp.concatenate([xh, xl], axis=0), gh[...])
        ys.append(y[:8] + y[8:] + mm(xh, gl[...]))

    def picked(kind, k, to):
        at = 32 * k
        return pltpu.roll(ys[kind][:, at // B * B : at // B * B + B], (to - at) % B, 1)

    none = jnp.zeros((8, B), F32)
    for k in range(NSUB):
        after = picked(0, k + 1, 32) if k + 1 < NSUB else none
        before = picked(0, k - 1, 64) if k > 0 else none
        here = jnp.where(lane < 32, picked(0, k, 0), jnp.where(lane < 64, after, before))
        msg[k, :, 0:B] = jnp.where(lane < 96, here, picked(1, k, 96))[:R]
        if msg.shape[2] > B:
            msg[k, :, B : 2 * B] = second[:R]
    after, before = neighbours(recv, 2 * B, 2 * B + stride)
    after = pltpu.roll(after, B - KC, 1)
    before = pltpu.roll(before, KC, 1)
    both = jnp.where(lane // KC % 2 == 0, after, before)
    cacross[...] = jnp.where(lane < NCL, both, 0.0)[:R]
    return second


def k_first_global(recv, own, gc, msg, scal, cacross, gh, gl, ah, al):
    picked_columns(gc, [own[0:1, :], own[1:2, :]], gh, gl)
    after, before = neighbours(recv, 3 * B, 5 * B)
    lane = iota((8, B), 1)
    after = pltpu.roll(after, B - 8, 1)
    before = pltpu.roll(before, 8, 1)
    ids = jnp.where(lane // 8 % 2 == 0, after, before)
    picked_columns(gc, [ids[0:1], ids[1:2]], ah, al)
    second = solve(recv, ((gh, gl), (ah, al)), msg, cacross, 2 * B)
    scal[...] = jnp.concatenate([second, second], axis=0)


def k_global(recv, gh, gl, ah, al, msg, cacross):
    solve(recv, ((gh, gl), (ah, al)), msg, cacross, B)


def four_times(x):
    x = jnp.concatenate([x, x], axis=0)
    return jnp.concatenate([x, x], axis=0)


def corrections(recv, csol, cacross, w, pw):
    picks = four_times(member_sum(recv)[:, :B])
    tail = iota((ROWS, B), 1) >= NCL

    def sol(cluster, turn):
        p = pltpu.roll(picks, turn, 1) if turn else picks
        return jnp.where(tail, p, four_times(cluster))

    own = spread_back(sol(csol[0], 96), w[...])
    sides = (sol(csol[1], 64), sol(csol[2], 32), sol(cacross[...], 0))
    pi = [spread_back(x, pw[:, b * B : (b + 1) * B]) for b, x in enumerate(sides)]
    return own, jnp.concatenate(pi, axis=1)


def across_received(out1, out2):
    odd_in, even_in = across_of(out1[...], out2[...])
    return jnp.concatenate([odd_in[0:R], even_in[0:R], odd_in[R:], even_in[R:]], axis=0)


def received(from_next, from_prev, out1, out2):
    return jnp.concatenate([from_next, from_prev, across_received(out1, out2)], axis=1)


def paired(n_cl):
    c, k = lax.axis_index("y") * lax.axis_size("z") + lax.axis_index("z"), lax.axis_index("sub")
    lane = iota((ROWS, D), 1)
    is_even = iota((ROWS, D), 0) // R % 2 == 0
    yes = [
        jnp.where(x, 1.0, 0.0) for x in (k < NSUB - 1, k > 0, c < n_cl - 1, c > 0)
    ]
    across = jnp.where(is_even, yes[2], yes[3])
    return jnp.where(lane < B, yes[0], jnp.where(lane < 2 * B, yes[1], across))


def image_of(d, pd, sg, ops):
    spread = sg * (d + pd)
    low = spread.astype(BF16)
    image = jnp.zeros((ROWS, D), F32)
    row = iota((ROWS, D), 0) // R
    for s in range(S):
        image = jnp.where(row == s, mm(low, ops[s]), image)
    return sg * image, row_dot(spread, image)


def k_first_image(
    recv, csol, cacross, in1, in2, out1, out2, w, v, sg, ops, idx,
    pw, pv, d_out, pd_out, signed_out, curv, up_out, down_out, *outs,
):
    take_static(in1, in2, out1, out2, pw, pv)
    fix, pfix = corrections(recv, csol, cacross, w, pw)
    d = v[...] - fix
    pd = pv[...] - pfix
    d_out[...] = d
    pd_out[...] = pd
    signed, c = image_of(d, pd, sg[...], ops)
    signed_out[...] = signed
    curv[...] = jnp.broadcast_to(c[:8], (8, B))
    up, down, even, odd = moved_blocks(signed, idx)
    up_out[...] = up
    down_out[...] = down
    write_across(even, odd, *outs)


def member_ids(all_ids, member, to):
    row = jnp.zeros((8, B), F32)
    which = jnp.full((8, B), member, I32)
    for j in range(NSUB):
        x = jnp.broadcast_to(all_ids[j // 4 : j // 4 + 1, :], (8, B))
        row = jnp.where(which == j, pltpu.roll(x, (to - 32 * (j % 4)) % B, 1), row)
    return row


def k_product(
    ids, signed, up, down, out1, out2, static1, static2, w, pw, cc, all_ids, across_out, msg
):
    k = lax.axis_index("sub")
    odd_k = k % 2
    across = across_received(out1, out2)
    across_out[...] = across
    u = signed[...]
    known = jnp.concatenate([u[:, : 2 * B], u[:, 2 * B :] + across], axis=1)
    own = coefs(known, w[...])[:8]

    def towards(b):
        lanes = pl.ds(pl.multiple_of(b * B, B), B)
        return coefs(signed[:, lanes], pw[:, lanes])[:8]

    first, second = towards(odd_k), towards(1 - odd_k)
    ccp = (
        clustered(own, cc[...])
        + clustered(first, coarse_rows(static1))
        + clustered(second, coarse_rows(static2))
    )
    lane = iota((8, B), 1)
    other = jnp.clip(k - 1 + 2 * odd_k, 0, NSUB - 1)

    def lanes_of(c96, c64, c32, rest):
        return jnp.where(
            lane >= 96, c96, jnp.where(lane >= 64, c64, jnp.where(lane >= 32, c32, rest))
        )

    c4 = lanes_of(own, pltpu.roll(first, B - 32, 1), pltpu.roll(second, B - 64, 1), 0.0)
    row = lanes_of(
        ids_row(ids).astype(F32),
        member_ids(all_ids, k + 1 - 2 * odd_k, 64),
        member_ids(all_ids, other, 32),
        -1.0,
    )
    write_message(msg, c4, ccp, row)
    after, before = jnp.minimum(k + 1, NSUB - 1), jnp.maximum(k - 1, 0)
    for s in range(S):
        at = MSG + B * s
        msg[after, :, at : at + B] = up[R * s : R * s + R, :]
        msg[before, :, at : at + B] = down[R * s : R * s + R, :]


def make_joined(n_cl):
    def k_joined(recv, signed, across, curv, v, out, csol, ap_out, pap_out):
        k = lax.axis_index("sub")

        def block(member, there):
            x = [recv[member, :, MSG + B * s : MSG + B * s + B] for s in range(S)]
            x = jnp.concatenate(x, axis=0)
            return pick(there, x, jnp.zeros_like(x))

        from_next = block(jnp.minimum(k + 1, NSUB - 1), k < NSUB - 1)
        from_prev = block(jnp.maximum(k - 1, 0), k > 0)
        u = signed[...]
        pi = jnp.concatenate([from_next, from_prev, across[...]], axis=1)
        ap = u + pi
        ap_out[...] = ap
        pap_out[...] = pi + paired(n_cl) * u
        scalars = [curv[...][:, :1], row_dot(v[...], ap)[:8], row_dot(ap, ap)[:8]]
        k_rows(recv, out, csol, scalars)

    return k_joined


def scalar_at(scal, j):
    return jnp.sum(jnp.where(iota((ROWS, B), 1) == 64 + j, scal, 0.0), axis=1, keepdims=True)


def k_last_image(
    recv, csol, cacross, scal0, w, pw, v, d, pd, ap, pap, sg, ops, idx,
    r_out, x_out, d_out, signed_out, msg, *outs,
):
    fix, pfix = corrections(recv, csol, cacross, w, pw)
    rho = scalar_at(scal0[...], 0)
    s1 = four_times(member_sum(recv)[:, B : 2 * B])
    step = rho / scalar_at(s1, 0)
    rho_new = rho - 2.0 * step * scalar_at(s1, 1) + step * step * scalar_at(s1, 2)
    beta = rho_new / rho
    ap_ = ap[...]
    d0 = d[...]
    pd0 = pd[...]
    r = v[...] - step * ap_
    r_out[...] = r
    x_out[...] = step * d0
    d1 = d0 - step * (ap_ - fix) + beta * d0
    pd1 = pd0 - step * (pap[...] - pfix) + beta * pd0
    d_out[...] = d1
    signed, c = image_of(d1, pd1, sg[...], ops)
    signed_out[...] = signed
    sq = row_dot(r, r)
    lane = iota((8, B), 1)
    row = iota((8, B), 0)
    both = jnp.where(lane == row, c[:8], jnp.where(lane == row + R, sq[:8], 0.0))
    line = jnp.sum(jnp.where(row < R, both, 0.0), axis=0, keepdims=True)
    msg[...] = jnp.broadcast_to(line[None], msg.shape)
    write_moved(signed, idx, *outs)


def k_total(recv, out):
    out[...] = jnp.broadcast_to(jnp.sum(recv[...], axis=0, keepdims=True), out.shape)


def k_finish(recv, signed, in1, in2, out1, out2, x, r, d, x_out, r_out):
    line = jnp.broadcast_to(jnp.sum(recv[...], axis=0), (ROWS, B))
    lane = iota((ROWS, B), 1)
    row = iota((ROWS, B), 0) % R
    curv = jnp.sum(jnp.where(lane == row, line, 0.0), axis=1, keepdims=True)
    rho = jnp.sum(jnp.where(lane == row + R, line, 0.0), axis=1, keepdims=True)
    step = rho / curv
    xn = x[...] + step * d[...]
    pi = received(*within_of(in1[...], in2[...]), out1, out2)
    rn = r[...] - step * (signed[...] + pi)
    for s in range(S):
        x_out[s] = xn[R * s : R * s + R]
        r_out[s] = rn[R * s : R * s + R]


def call(body, outs, *args, smem=(), scratch=()):
    def space(i):
        return pltpu.SMEM if i in smem else pltpu.VMEM

    specs = [pl.BlockSpec(memory_space=space(i)) for i in range(len(args))]
    out_shape = tuple(jax.ShapeDtypeStruct(s, t) for s, t in outs)
    return pl.pallas_call(
        body,
        out_shape=out_shape,
        in_specs=specs,
        out_specs=tuple(pl.BlockSpec(memory_space=pltpu.VMEM) for _ in outs),
        scratch_shapes=scratch,
        compiler_params=pltpu.CompilerParams(vmem_limit_bytes=VMEM_LIMIT),
    )(*args)


def to_owner(x, axis):
    return lax.all_to_all(x, axis, 0, 0, tiled=True)


def f32(*shape):
    return (shape, F32)


FIELD = f32(ROWS, D)


SENDS = (f32(ROWS, B), f32(ROWS, B), f32(2 * R, B), f32(2 * R, B))


def swap(x, axis, n, first):
    low = range(0 if first else 1, n - 1, 2)
    return lax.ppermute(x, axis, [p for i in low for p in ((i, i + 1), (i + 1, i))])


def exchange_across(first, second, n_cl):
    first = swap(first, CLUSTER, n_cl, True)
    second = swap(second, CLUSTER, n_cl, False)
    return first, second


def exchange(in1, in2, out1, out2, n_sub, n_cl):
    across = exchange_across(out1, out2, n_cl)
    in2 = swap(in2, "sub", n_sub, False)
    in1 = swap(in1, "sub", n_sub, True)
    return in1, in2, *across


def solve_all(rhs, operators, signs, links, cb, kb, ids, cluster_coarse, gc):
    n_sub = lax.axis_size("sub")
    n_y = lax.axis_size("y")
    n_z = lax.axis_size("z")
    n_cl = n_y * n_z
    cc = cluster_coarse.reshape(NCL, NSUB * NCL)
    message = f32(NSUB, R, MSG)
    picked = ((2 * B, 2 * B), BF16)
    answer = (f32(NSUB, R, B), f32(ROWS, B), f32(R, B))

    w = jnp.concatenate([cb.reshape(NCL, D), kb.reshape(NB - NCL, D)], axis=0)
    msg, v = call(k_coefs, (message, FIELD), ids, rhs, w, cc, smem=(0,))
    recv = to_owner(msg, "sub")
    rows, csol, all_ids = call(
        k_first_rows, (f32(n_y, R, 4 * B), f32(3, R, B), f32(8, B)), recv
    )
    recv = to_owner(rows, "y")
    (rows,) = call(k_pass, (f32(n_z, R, 6 * B),), recv)
    recv_z = to_owner(rows, "z")
    sg, idx, in2, *out = call(
        k_send_static,
        (
            FIELD, ((3, ROWS, B), I32), f32(WITHIN, B), f32(PACK, B), f32(PACK, B),
        ),
        recv, signs, links.transpose(1, 0, 2), w, v, cc,
    )
    across = exchange_across(*out, n_cl)
    in2 = swap(in2, "sub", n_sub, False)
    (in1,) = call(k_send_chip, (f32(WITHIN, B),), recv_z, w, v, cc, idx)
    in1 = swap(in1, "sub", n_sub, True)
    to_all, scal0, cacross, gh, gl, ah, al = call(
        k_first_global, (*answer, picked, picked, picked, picked), recv_z, all_ids, gc
    )
    to_all = to_owner(to_all, "sub")
    pw, pv, d, pd, signed, curv, up, down, *out = call(
        k_first_image,
        (f32(NB, D), FIELD, FIELD, FIELD, FIELD, f32(8, B), *SENDS),
        to_all, csol, cacross, in1, in2, *across,
        w, v, sg, operators, idx,
    )
    got = exchange_across(*out, n_cl)
    across, msg = call(
        k_product,
        (f32(ROWS, B), f32(NSUB, R, MSG + S * B)),
        ids, signed, up, down, *got, in1, in2, w, pw, cc, all_ids, smem=(0,),
    )
    rows, csol, ap, pap = call(
        make_joined(n_cl),
        (f32(n_y, R, D), f32(3, R, B), FIELD, FIELD),
        to_owner(msg, "sub"), signed, across, curv, v,
    )
    (rows,) = call(k_pass, (f32(n_z, R, 4 * B),), to_owner(rows, "y"))
    to_all, cacross = call(
        k_global,
        (f32(NSUB, R, 2 * B), f32(R, B)),
        to_owner(rows, "z"), gh, gl, ah, al,
    )
    r, x, d1, signed, line, *out = call(
        k_last_image,
        (FIELD, FIELD, FIELD, FIELD, f32(n_y * n_sub, 1, B), *SENDS),
        to_owner(to_all, "sub"), csol, cacross, scal0,
        w, pw, v, d, pd, ap, pap, sg, operators, idx,
    )
    line = to_owner(line, ("y", "sub"))
    (line,) = call(k_total, (f32(n_z, 1, B),), line)
    line = to_owner(line, "z")
    got = exchange(*out, n_sub, n_cl)
    out = f32(S, R, D)
    return call(k_finish, (out, out), line, signed, *got, x, r, d1)


def solution(mesh):
    n_y, n_z = 8, 12
    torus = Mesh(mesh.devices.reshape(n_y, n_z, NSUB), ("y", "z", "sub"))
    both = ("y", "z", "sub")
    in_specs = (
        P(both, None, None),
        P(both, None, None),
        P(both, None),
        P(both, None, None),
        P(both, None, None),
        P(both, None, None),
        P(both, None),
        P(CLUSTER, "sub", None),
        P("sub", None),
    )
    out_specs = (P(both, None, None), P(both, None, None))
    return jax.shard_map(solve_all, mesh=torus, in_specs=in_specs, out_specs=out_specs, check_vma=False)
```

```python
import jax
import jax.numpy as jnp
from jax import lax
from jax.experimental import pallas as pl
from jax.experimental.pallas import tpu as pltpu
from jax.sharding import Mesh
from jax.sharding import PartitionSpec as P


F32 = jnp.float32
BF16 = jnp.bfloat16
I32 = jnp.int32
R = 4
S = 4
ROWS = R * S
B = 128
D = 384
KC = 24
NB = 128
NCL = S * KC
CHUNK = 192
NSUB = 8
CLUSTER = ("y", "z")
VMEM_LIMIT = 16 * 2**20


def iota(shape, dim):
    return lax.broadcasted_iota(I32, shape, dim)


def pick(flag, a, b):
    return jnp.where(jnp.full(a.shape, flag.astype(I32), I32) == 1, a, b)


def even_member():
    return lax.axis_index("sub") % 2 == 0


def even_cluster():
    return (lax.axis_index("y") * lax.axis_size("z") + lax.axis_index("z")) % 2 == 0


def split(x):
    hi = x.astype(BF16)
    return hi, (x - hi.astype(F32)).astype(BF16)


def mm(a, b):
    return lax.dot_general(a, b, (((1,), (0,)), ((), ())), preferred_element_type=F32)


def mm_t(a, b):
    return lax.dot_general(a, b, (((1,), (1,)), ((), ())), preferred_element_type=F32)


def dot2(x, w, f=mm):
    n = x.shape[0]
    xh, xl = split(x)
    wh, wl = split(w)
    xs = jnp.concatenate([xh, xl], axis=0)
    both = f(xs, wh)
    return both[:n] + both[n:] + f(xh, wl)


def lanes_of_sub(shape):
    lane = iota(shape, 1)
    return jnp.where(lane < NCL, lane // KC, (lane - NCL) // 8)


def own_mask():
    return iota((ROWS, NB), 0) // R == lanes_of_sub((ROWS, NB))


def by_load(x):
    y = x[:8] + x[8:]
    y = y + pltpu.roll(y, 4, 0)
    return jnp.concatenate([y, y], axis=0)


def coefs(v, w):
    return by_load(jnp.where(own_mask(), dot2(v, w, mm_t), 0.0))


def spread_back(sol, w):
    return dot2(jnp.where(own_mask(), sol, 0.0), w)


def ids_row(ids):
    lane = iota((8, NB), 1)
    row = jnp.full((8, NB), -1, I32)
    for s in range(S):
        for c in range(8):
            row = jnp.where(lane == NCL + 8 * s + c, ids[s, c], row)
    return row


def to_column(row):
    full = jnp.broadcast_to(row[:1], (NB, NB))
    eye = iota((NB, NB), 0) == iota((NB, NB), 1)
    return jnp.sum(jnp.where(eye, full, 0.0), axis=1, keepdims=True)


def window(x, at, width):
    lane = iota((x.shape[0], B), 1)
    tile, off = at // B, at % B
    here = x[:, tile * B : (tile + 1) * B]
    if off:
        here = pltpu.roll(here, B - off, 1)
        if off + width > B:
            after = pltpu.roll(x[:, (tile + 1) * B : (tile + 2) * B], B - off, 1)
            here = jnp.where(lane < B - off, here, after)
    return here


MSG = 5 * B


def clustered(c4, cc):
    return dot2(jnp.where(iota((8, NB), 1) < NCL, c4, 0.0)[:, :NCL], cc)


def marked(scalars):
    lane = iota((8, B), 1)
    extra = jnp.zeros((8, B), F32)
    for j, val in enumerate(scalars):
        extra = jnp.where(lane == 64 + j, val, extra)
    return extra


def write_message(msg, c4, ccp, row, scalars=()):
    col = to_column(row).astype(I32)
    hi, lo = split(c4)
    low = (c4 - hi.astype(F32) - lo.astype(F32)).astype(BF16)
    parts = jnp.concatenate([hi, lo, low], axis=0)
    lane = iota((8, B), 1)
    extra = marked(scalars)
    none = jnp.zeros((8, B), F32)
    cluster = [jnp.where(lane < NCL, window(ccp, NCL * k, NCL), 0.0) for k in range(NSUB)]
    for k in range(NSUB):
        n = iota((NB, 2 * B), 1)
        onehot = jnp.where((col == n + CHUNK * k) & (n < CHUNK), 1.0, 0.0).astype(BF16)
        y = mm(parts, onehot)
        y = y[:8] + y[8:16] + y[16:24]
        tiles = (
            y[:, :B],
            y[:, B:] + extra,
            jnp.where(lane < NCL, cluster[k], row),
            cluster[k + 1] if k + 1 < NSUB else none,
            cluster[k - 1] if k > 0 else none,
        )
        for t, x in enumerate(tiles):
            msg[k, :, t * B : (t + 1) * B] = x[:R]


def row_dot(a, b):
    return by_load(jnp.sum(a * b, axis=1, keepdims=True))


STATIC = NB + ROWS
WITHIN = STATIC + NCL * 6
PACK = 72


def k_coefs(ids, rhs, w, cc, msg, v_out):
    for s in range(S):
        v_out[R * s : R * s + R, :] = rhs[s]
    v = v_out[...]
    c4 = coefs(v, w[...])[:8]
    row = ids_row(ids).astype(F32)
    write_message(msg, c4, clustered(c4, cc[...]), row, [row_dot(v, v)[:8]])


def k_tables(after, signs, links, sg_out, idx_out):
    del after
    pos = iota((8, B), 1).astype(BF16)
    for s in range(S):
        sg_out[R * s : R * s + R, :] = jnp.broadcast_to(signs[s : s + 1, :].astype(F32), (R, D))
        for b in range(3):
            q = links[b, s : s + 1, :]
            if b == 0 or (b == 2 and s % 2 == 0):
                hot = jnp.where(iota((B, B), 0) == q, 1.0, 0.0).astype(BF16)
                q = mm_t(pos, hot)[:1].astype(I32)
            idx_out[b, R * s : R * s + R, :] = jnp.broadcast_to(q, (R, B))


def static_blocks(w, v, idx, b):
    lanes = pl.ds(pl.multiple_of(b * B, B), B)

    def moved(x, q):
        return jnp.take_along_axis(x, jnp.broadcast_to(q, x.shape), axis=1)

    for s in range(S):
        q = idx[b, R * s : R * s + 1, :]
        for at, n in ((KC * s, KC), (NCL + 8 * s, 8)):
            yield s, at, moved(w[at : at + n, lanes], q)
    yield None, NB, moved(v[:, lanes], idx[b])


def send_within(w, v, cc, idx, out, b):
    for _, at, x in static_blocks(w, v, idx, b):
        out[at : at + x.shape[0], :] = x
    for j in range(6):
        out[STATIC + NCL * j : STATIC + NCL * j + NCL, :] = cc[:, j * B : (j + 1) * B]


def coarse_rows(x):
    return jnp.concatenate([x[STATIC + NCL * j : STATIC + NCL * j + NCL, :] for j in range(6)], axis=1)


def k_send_static(
    after, signs, links, w, v, cc, sg_out, idx_out, first, second, out1, out2
):
    k_tables(after, signs, links, sg_out, idx_out)
    odd = lax.axis_index("sub") % 2
    send_within(w, v, cc, idx_out, first, odd)
    send_within(w, v, cc, idx_out, second, 1 - odd)
    send_across(w, v, idx_out, out1, out2)


def send_across(w, v, idx, first, second):
    flag = even_cluster()
    blocks = {(s, at): x for s, at, x in static_blocks(w, v, idx, 2)}

    def put(to, even, odd):
        n = even.shape[0]
        first[to : to + n, :] = pick(flag, even, odd)
        second[to : to + n, :] = pick(flag, odd, even)

    for h in range(2):
        s = 2 * h
        put(KC * h, blocks[s, KC * s], blocks[s + 1, KC * (s + 1)])
        put(2 * KC + 8 * h, blocks[s, NCL + 8 * s], blocks[s + 1, NCL + 8 * s + 8])
        x = blocks[None, NB][8 * h : 8 * h + 8]
        put(2 * KC + 16 + R * h, x[:R], x[R:])


def moved_blocks(v, idx):
    up, down, across = (
        jnp.take_along_axis(v[:, b * B : (b + 1) * B], idx[b], axis=1) for b in range(3)
    )
    even = jnp.concatenate([across[0:R], across[8 : 8 + R]], axis=0)
    odd = jnp.concatenate([across[R:8], across[8 + R :]], axis=0)
    return up, down, even, odd


def write_across(even, odd, first, second):
    flag = even_cluster()
    first[...] = pick(flag, even, odd)
    second[...] = pick(flag, odd, even)


def write_moved(v, idx, in1, in2, out1, out2):
    up, down, even, odd = moved_blocks(v, idx)
    flag = even_member()
    in1[...] = pick(flag, up, down)
    in2[...] = pick(flag, down, up)
    write_across(even, odd, out1, out2)


def across_of(out1, out2):
    flag = even_cluster()
    return pick(flag, out1, out2), pick(flag, out2, out1)


def within_of(in1, in2):
    flag = even_member()
    return pick(flag, in1, in2), pick(flag, in2, in1)


def take_static(in1, in2, out1, out2, pw_out, pv_out):
    from_next, from_prev = within_of(in1[0:STATIC, :], in2[0:STATIC, :])
    odd_in, even_in = across_of(out1[...], out2[...])
    pw_out[:, 0:B] = from_next[0:NB, :]
    pw_out[:, B : 2 * B] = from_prev[0:NB, :]
    for s in range(S):
        h = s // 2
        side = even_in if s % 2 else odd_in
        pw_out[KC * s : KC * s + KC, 2 * B :] = side[KC * h : KC * h + KC, :]
        at = 2 * KC + 8 * h
        pw_out[NCL + 8 * s : NCL + 8 * s + 8, 2 * B :] = side[at : at + 8, :]
        at = 2 * KC + 16 + R * h
        pv_out[R * s : R * s + R, 2 * B :] = side[at : at + R, :]
    pv_out[:, 0:B] = from_next[NB:STATIC, :]
    pv_out[:, B : 2 * B] = from_prev[NB:STATIC, :]


def member_sum(recv):
    total = recv[0]
    for k in range(1, NSUB):
        total = total + recv[k]
    return total


def k_rows(recv, out, csol, scalars=()):
    total = recv[0, :, 0:MSG]
    for k in range(1, NSUB):
        total = total + recv[k, :, 0:MSG]
    own = jnp.where(iota((R, B), 1) < NCL, total[:, 2 * B : 3 * B], 0.0)
    csol[0] = own
    csol[1] = total[:, 3 * B : 4 * B]
    csol[2] = total[:, 4 * B : 5 * B]
    second = total[:, B : 2 * B] + marked(scalars)[:R]
    x = jnp.concatenate([total[:, :B], second, own], axis=1)
    out[:, :, 0:D] = jnp.broadcast_to(x[None], (out.shape[0], R, D))


def cluster_ids(recv):
    lane = iota((8, B), 1)
    rows = []
    for half in range(2):
        ids = jnp.zeros((8, B), F32)
        for j in range(4):
            row = recv[4 * half + j, 0:1, 2 * B : 3 * B]
            row = pltpu.roll(jnp.broadcast_to(row, (8, B)), (32 + 32 * j) % B, 1)
            ids = jnp.where(lane // 32 == j, row, ids)
        rows.append(ids)
    return rows


def k_first_rows(recv, out, csol, ids_out):
    k_rows(recv, out, csol)
    low, high = cluster_ids(recv)
    ids = jnp.where(iota((8, B), 0) == 0, low, high)
    ids_out[...] = ids
    out[:, :, D:] = jnp.broadcast_to(ids[None, :R], (out.shape[0], R, B))


def k_pass(recv, out):
    y, z = lax.axis_index("y"), lax.axis_index("z")
    n_y, n_z = recv.shape[0], out.shape[0]
    total = jnp.sum(recv[:, :, 0 : 2 * B], axis=0)
    other = jnp.where(z == 0, jnp.minimum(y + 1, n_y - 1), jnp.maximum(y - 1, 0))
    x = jnp.concatenate([total, recv[y, :, 2 * B :], recv[other, :, 2 * B :]], axis=1)
    out[...] = jnp.broadcast_to(x[None], (n_z, *x.shape))


def neighbours(recv, at, wrapped_at):
    z = lax.axis_index("z")
    n_z = recv.shape[0]
    last, first = z == n_z - 1, z == 0
    nxt = recv[jnp.where(last, 0, z + 1)]
    prv = recv[jnp.where(first, n_z - 1, z - 1)]

    def tile(x, use_wrapped):
        plain = x[:, at : at + B]
        wrapped = x[:, wrapped_at : wrapped_at + B]
        x = jnp.where(jnp.full((R, B), use_wrapped.astype(I32), I32) == 1, wrapped, plain)
        return jnp.concatenate([x, x], axis=0)

    return tile(nxt, last), tile(prv, first)


def picked_columns(gc, rows, hi_out, lo_out):
    ids = jnp.concatenate([x[:1].astype(I32) for x in rows], axis=1)
    n = iota((gc.shape[1], ids.shape[1]), 0)
    onehot = jnp.where(n == ids, 1.0, 0.0).astype(BF16)
    gh, gl = split(gc[...])
    zero = jnp.zeros((2 * B - CHUNK, ids.shape[1]), BF16)
    hi_out[0:CHUNK, :] = mm(gh, onehot).astype(BF16)
    hi_out[CHUNK : 2 * B, :] = zero
    lo_out[0:CHUNK, :] = mm(gl, onehot).astype(BF16)
    lo_out[CHUNK : 2 * B, :] = zero


def solve(recv, parts, msg, cacross, stride):
    total = jnp.sum(recv[:, :, 0 : 2 * B], axis=0)
    total = jnp.concatenate([total, total], axis=0)
    second = total[:, B:]
    lane = iota((8, B), 1)
    x = jnp.concatenate([total[:, :B], jnp.where(lane < 64, second, 0.0)], axis=1)
    xh, xl = split(x)
    ys = []
    for gh, gl in parts:
        y = mm(jnp.concatenate([xh, xl], axis=0), gh[...])
        ys.append(y[:8] + y[8:] + mm(xh, gl[...]))

    def picked(kind, k, to):
        at = 32 * k
        return pltpu.roll(ys[kind][:, at // B * B : at // B * B + B], (to - at) % B, 1)

    none = jnp.zeros((8, B), F32)
    for k in range(NSUB):
        after = picked(0, k + 1, 32) if k + 1 < NSUB else none
        before = picked(0, k - 1, 64) if k > 0 else none
        here = jnp.where(lane < 32, picked(0, k, 0), jnp.where(lane < 64, after, before))
        msg[k, :, 0:B] = jnp.where(lane < 96, here, picked(1, k, 96))[:R]
        if msg.shape[2] > B:
            msg[k, :, B : 2 * B] = second[:R]
    after, before = neighbours(recv, 2 * B, 2 * B + stride)
    after = pltpu.roll(after, B - KC, 1)
    before = pltpu.roll(before, KC, 1)
    both = jnp.where(lane // KC % 2 == 0, after, before)
    cacross[...] = jnp.where(lane < NCL, both, 0.0)[:R]
    return second


def k_first_global(recv, own, gc, msg, scal, cacross, gh, gl, ah, al):
    picked_columns(gc, [own[0:1, :], own[1:2, :]], gh, gl)
    after, before = neighbours(recv, 3 * B, 5 * B)
    lane = iota((8, B), 1)
    after = pltpu.roll(after, B - 8, 1)
    before = pltpu.roll(before, 8, 1)
    ids = jnp.where(lane // 8 % 2 == 0, after, before)
    picked_columns(gc, [ids[0:1], ids[1:2]], ah, al)
    second = solve(recv, ((gh, gl), (ah, al)), msg, cacross, 2 * B)
    scal[...] = jnp.concatenate([second, second], axis=0)


def k_global(recv, gh, gl, ah, al, msg, cacross):
    solve(recv, ((gh, gl), (ah, al)), msg, cacross, B)


def four_times(x):
    x = jnp.concatenate([x, x], axis=0)
    return jnp.concatenate([x, x], axis=0)


def corrections(recv, csol, cacross, w, pw):
    picks = four_times(member_sum(recv)[:, :B])
    tail = iota((ROWS, B), 1) >= NCL

    def sol(cluster, turn):
        p = pltpu.roll(picks, turn, 1) if turn else picks
        return jnp.where(tail, p, four_times(cluster))

    own = spread_back(sol(csol[0], 96), w[...])
    sides = (sol(csol[1], 64), sol(csol[2], 32), sol(cacross[...], 0))
    pi = [spread_back(x, pw[:, b * B : (b + 1) * B]) for b, x in enumerate(sides)]
    return own, jnp.concatenate(pi, axis=1)


def across_received(out1, out2):
    odd_in, even_in = across_of(out1[...], out2[...])
    return jnp.concatenate([odd_in[0:R], even_in[0:R], odd_in[R:], even_in[R:]], axis=0)


def received(from_next, from_prev, out1, out2):
    return jnp.concatenate([from_next, from_prev, across_received(out1, out2)], axis=1)


def paired(n_cl):
    c, k = lax.axis_index("y") * lax.axis_size("z") + lax.axis_index("z"), lax.axis_index("sub")
    lane = iota((ROWS, D), 1)
    is_even = iota((ROWS, D), 0) // R % 2 == 0
    yes = [
        jnp.where(x, 1.0, 0.0) for x in (k < NSUB - 1, k > 0, c < n_cl - 1, c > 0)
    ]
    across = jnp.where(is_even, yes[2], yes[3])
    return jnp.where(lane < B, yes[0], jnp.where(lane < 2 * B, yes[1], across))


def image_of(d, pd, sg, ops):
    spread = sg * (d + pd)
    low = spread.astype(BF16)
    image = jnp.zeros((ROWS, D), F32)
    row = iota((ROWS, D), 0) // R
    for s in range(S):
        image = jnp.where(row == s, mm(low, ops[s]), image)
    return sg * image, row_dot(spread, image)


def k_first_image(
    recv, csol, cacross, in1, in2, out1, out2, w, v, sg, ops, idx,
    pw, pv, d_out, pd_out, signed_out, curv, up_out, down_out, *outs,
):
    take_static(in1, in2, out1, out2, pw, pv)
    fix, pfix = corrections(recv, csol, cacross, w, pw)
    d = v[...] - fix
    pd = pv[...] - pfix
    d_out[...] = d
    pd_out[...] = pd
    signed, c = image_of(d, pd, sg[...], ops)
    signed_out[...] = signed
    curv[...] = jnp.broadcast_to(c[:8], (8, B))
    up, down, even, odd = moved_blocks(signed, idx)
    up_out[...] = up
    down_out[...] = down
    write_across(even, odd, *outs)


def member_ids(all_ids, member, to):
    row = jnp.zeros((8, B), F32)
    which = jnp.full((8, B), member, I32)
    for j in range(NSUB):
        x = jnp.broadcast_to(all_ids[j // 4 : j // 4 + 1, :], (8, B))
        row = jnp.where(which == j, pltpu.roll(x, (to - 32 * (j % 4)) % B, 1), row)
    return row


def k_product(
    ids, signed, up, down, out1, out2, static1, static2, w, pw, cc, all_ids, across_out, msg
):
    k = lax.axis_index("sub")
    odd_k = k % 2
    across = across_received(out1, out2)
    across_out[...] = across
    u = signed[...]
    known = jnp.concatenate([u[:, : 2 * B], u[:, 2 * B :] + across], axis=1)
    own = coefs(known, w[...])[:8]

    def towards(b):
        lanes = pl.ds(pl.multiple_of(b * B, B), B)
        return coefs(signed[:, lanes], pw[:, lanes])[:8]

    first, second = towards(odd_k), towards(1 - odd_k)
    ccp = (
        clustered(own, cc[...])
        + clustered(first, coarse_rows(static1))
        + clustered(second, coarse_rows(static2))
    )
    lane = iota((8, B), 1)
    other = jnp.clip(k - 1 + 2 * odd_k, 0, NSUB - 1)

    def lanes_of(c96, c64, c32, rest):
        return jnp.where(
            lane >= 96, c96, jnp.where(lane >= 64, c64, jnp.where(lane >= 32, c32, rest))
        )

    c4 = lanes_of(own, pltpu.roll(first, B - 32, 1), pltpu.roll(second, B - 64, 1), 0.0)
    row = lanes_of(
        ids_row(ids).astype(F32),
        member_ids(all_ids, k + 1 - 2 * odd_k, 64),
        member_ids(all_ids, other, 32),
        -1.0,
    )
    write_message(msg, c4, ccp, row)
    after, before = jnp.minimum(k + 1, NSUB - 1), jnp.maximum(k - 1, 0)
    for s in range(S):
        at = MSG + B * s
        msg[after, :, at : at + B] = up[R * s : R * s + R, :]
        msg[before, :, at : at + B] = down[R * s : R * s + R, :]


def make_joined(n_cl):
    def k_joined(recv, signed, across, curv, v, out, csol, ap_out, pap_out):
        k = lax.axis_index("sub")

        def block(member, there):
            x = [recv[member, :, MSG + B * s : MSG + B * s + B] for s in range(S)]
            x = jnp.concatenate(x, axis=0)
            return pick(there, x, jnp.zeros_like(x))

        from_next = block(jnp.minimum(k + 1, NSUB - 1), k < NSUB - 1)
        from_prev = block(jnp.maximum(k - 1, 0), k > 0)
        u = signed[...]
        pi = jnp.concatenate([from_next, from_prev, across[...]], axis=1)
        ap = u + pi
        ap_out[...] = ap
        pap_out[...] = pi + paired(n_cl) * u
        scalars = [curv[...][:, :1], row_dot(v[...], ap)[:8], row_dot(ap, ap)[:8]]
        k_rows(recv, out, csol, scalars)

    return k_joined


def scalar_at(scal, j):
    return jnp.sum(jnp.where(iota((ROWS, B), 1) == 64 + j, scal, 0.0), axis=1, keepdims=True)


def k_last_image(
    recv, csol, cacross, scal0, w, pw, v, d, pd, ap, pap, sg, ops, idx,
    r_out, x_out, d_out, signed_out, msg, *outs,
):
    fix, pfix = corrections(recv, csol, cacross, w, pw)
    rho = scalar_at(scal0[...], 0)
    s1 = four_times(member_sum(recv)[:, B : 2 * B])
    step = rho / scalar_at(s1, 0)
    rho_new = rho - 2.0 * step * scalar_at(s1, 1) + step * step * scalar_at(s1, 2)
    beta = rho_new / rho
    ap_ = ap[...]
    d0 = d[...]
    pd0 = pd[...]
    r = v[...] - step * ap_
    r_out[...] = r
    x_out[...] = step * d0
    d1 = d0 - step * (ap_ - fix) + beta * d0
    pd1 = pd0 - step * (pap[...] - pfix) + beta * pd0
    d_out[...] = d1
    signed, c = image_of(d1, pd1, sg[...], ops)
    signed_out[...] = signed
    sq = row_dot(r, r)
    lane = iota((8, B), 1)
    row = iota((8, B), 0)
    both = jnp.where(lane == row, c[:8], jnp.where(lane == row + R, sq[:8], 0.0))
    line = jnp.sum(jnp.where(row < R, both, 0.0), axis=0, keepdims=True)
    msg[...] = jnp.broadcast_to(line[None], msg.shape)
    write_moved(signed, idx, *outs)


def k_total(recv, out):
    out[...] = jnp.broadcast_to(jnp.sum(recv[...], axis=0, keepdims=True), out.shape)


def k_finish(recv, signed, in1, in2, out1, out2, x, r, d, x_out, r_out):
    line = jnp.broadcast_to(jnp.sum(recv[...], axis=0), (ROWS, B))
    lane = iota((ROWS, B), 1)
    row = iota((ROWS, B), 0) % R
    curv = jnp.sum(jnp.where(lane == row, line, 0.0), axis=1, keepdims=True)
    rho = jnp.sum(jnp.where(lane == row + R, line, 0.0), axis=1, keepdims=True)
    step = rho / curv
    xn = x[...] + step * d[...]
    pi = received(*within_of(in1[...], in2[...]), out1, out2)
    rn = r[...] - step * (signed[...] + pi)
    for s in range(S):
        x_out[s] = xn[R * s : R * s + R]
        r_out[s] = rn[R * s : R * s + R]


def call(body, outs, *args, smem=(), scratch=()):
    def space(i):
        return pltpu.SMEM if i in smem else pltpu.VMEM

    specs = [pl.BlockSpec(memory_space=space(i)) for i in range(len(args))]
    out_shape = tuple(jax.ShapeDtypeStruct(s, t) for s, t in outs)
    return pl.pallas_call(
        body,
        out_shape=out_shape,
        in_specs=specs,
        out_specs=tuple(pl.BlockSpec(memory_space=pltpu.VMEM) for _ in outs),
        scratch_shapes=scratch,
        compiler_params=pltpu.CompilerParams(vmem_limit_bytes=VMEM_LIMIT),
    )(*args)


def to_owner(x, axis):
    return lax.all_to_all(x, axis, 0, 0, tiled=True)


def f32(*shape):
    return (shape, F32)


FIELD = f32(ROWS, D)


SENDS = (f32(ROWS, B), f32(ROWS, B), f32(2 * R, B), f32(2 * R, B))


def swap(x, axis, n, first):
    low = range(0 if first else 1, n - 1, 2)
    return lax.ppermute(x, axis, [p for i in low for p in ((i, i + 1), (i + 1, i))])


def exchange_across(first, second, n_cl):
    first = swap(first, CLUSTER, n_cl, True)
    second = swap(second, CLUSTER, n_cl, False)
    return first, second


def exchange(in1, in2, out1, out2, n_sub, n_cl):
    across = exchange_across(out1, out2, n_cl)
    in2 = swap(in2, "sub", n_sub, False)
    in1 = swap(in1, "sub", n_sub, True)
    return in1, in2, *across


def solve_all(rhs, operators, signs, links, cb, kb, ids, cluster_coarse, gc):
    n_sub = lax.axis_size("sub")
    n_y = lax.axis_size("y")
    n_z = lax.axis_size("z")
    n_cl = n_y * n_z
    cc = cluster_coarse.reshape(NCL, NSUB * NCL)
    message = f32(NSUB, R, MSG)
    picked = ((2 * B, 2 * B), BF16)
    answer = (f32(NSUB, R, B), f32(ROWS, B), f32(R, B))

    w = jnp.concatenate([cb.reshape(NCL, D), kb.reshape(NB - NCL, D)], axis=0)
    msg, v = call(k_coefs, (message, FIELD), ids, rhs, w, cc, smem=(0,))
    recv = to_owner(msg, "sub")
    rows, csol, all_ids = call(
        k_first_rows, (f32(n_y, R, 4 * B), f32(3, R, B), f32(8, B)), recv
    )
    recv = to_owner(rows, "y")
    (rows,) = call(k_pass, (f32(n_z, R, 6 * B),), recv)
    recv_z = to_owner(rows, "z")
    sg, idx, in1, in2, *out = call(
        k_send_static,
        (
            FIELD, ((3, ROWS, B), I32), f32(WITHIN, B), f32(WITHIN, B),
            f32(PACK, B), f32(PACK, B),
        ),
        recv, signs, links.transpose(1, 0, 2), w, v, cc,
    )
    across = exchange_across(*out, n_cl)
    in2 = swap(in2, "sub", n_sub, False)
    in1 = swap(in1, "sub", n_sub, True)
    to_all, scal0, cacross, gh, gl, ah, al = call(
        k_first_global, (*answer, picked, picked, picked, picked), recv_z, all_ids, gc
    )
    to_all = to_owner(to_all, "sub")
    pw, pv, d, pd, signed, curv, up, down, *out = call(
        k_first_image,
        (f32(NB, D), FIELD, FIELD, FIELD, FIELD, f32(8, B), *SENDS),
        to_all, csol, cacross, in1, in2, *across,
        w, v, sg, operators, idx,
    )
    got = exchange_across(*out, n_cl)
    across, msg = call(
        k_product,
        (f32(ROWS, B), f32(NSUB, R, MSG + S * B)),
        ids, signed, up, down, *got, in1, in2, w, pw, cc, all_ids, smem=(0,),
    )
    rows, csol, ap, pap = call(
        make_joined(n_cl),
        (f32(n_y, R, D), f32(3, R, B), FIELD, FIELD),
        to_owner(msg, "sub"), signed, across, curv, v,
    )
    (rows,) = call(k_pass, (f32(n_z, R, 4 * B),), to_owner(rows, "y"))
    to_all, cacross = call(
        k_global,
        (f32(NSUB, R, 2 * B), f32(R, B)),
        to_owner(rows, "z"), gh, gl, ah, al,
    )
    r, x, d1, signed, line, *out = call(
        k_last_image,
        (FIELD, FIELD, FIELD, FIELD, f32(n_y * n_sub, 1, B), *SENDS),
        to_owner(to_all, "sub"), csol, cacross, scal0,
        w, pw, v, d, pd, ap, pap, sg, operators, idx,
    )
    line = to_owner(line, ("y", "sub"))
    (line,) = call(k_total, (f32(n_z, 1, B),), line)
    line = to_owner(line, "z")
    got = exchange(*out, n_sub, n_cl)
    out = f32(S, R, D)
    return call(k_finish, (out, out), line, signed, *got, x, r, d1)


def solution(mesh):
    n_y, n_z = 8, 12
    torus = Mesh(mesh.devices.reshape(n_y, n_z, NSUB), ("y", "z", "sub"))
    both = ("y", "z", "sub")
    in_specs = (
        P(both, None, None),
        P(both, None, None),
        P(both, None),
        P(both, None, None),
        P(both, None, None),
        P(both, None, None),
        P(both, None),
        P(CLUSTER, "sub", None),
        P("sub", None),
    )
    out_specs = (P(both, None, None), P(both, None, None))
    return jax.shard_map(solve_all, mesh=torus, in_specs=in_specs, out_specs=out_specs, check_vma=False)
```

```python
import jax
import jax.numpy as jnp
from jax import lax
from jax.experimental import pallas as pl
from jax.experimental.pallas import tpu as pltpu
from jax.sharding import Mesh
from jax.sharding import PartitionSpec as P


F32 = jnp.float32
BF16 = jnp.bfloat16
I32 = jnp.int32
R = 4
S = 4
ROWS = R * S
B = 128
D = 384
KC = 24
NB = 128
NCL = S * KC
CHUNK = 192
NSUB = 8
CLUSTER = ("y", "z")
VMEM_LIMIT = 16 * 2**20


def iota(shape, dim):
    return lax.broadcasted_iota(I32, shape, dim)


def pick(flag, a, b):
    return jnp.where(jnp.full(a.shape, flag.astype(I32), I32) == 1, a, b)


def even_member():
    return lax.axis_index("sub") % 2 == 0


def even_cluster():
    return (lax.axis_index("y") * lax.axis_size("z") + lax.axis_index("z")) % 2 == 0


def split(x):
    hi = x.astype(BF16)
    return hi, (x - hi.astype(F32)).astype(BF16)


def mm(a, b):
    return lax.dot_general(a, b, (((1,), (0,)), ((), ())), preferred_element_type=F32)


def mm_t(a, b):
    return lax.dot_general(a, b, (((1,), (1,)), ((), ())), preferred_element_type=F32)


def dot2(x, w, f=mm):
    n = x.shape[0]
    xh, xl = split(x)
    wh, wl = split(w)
    xs = jnp.concatenate([xh, xl], axis=0)
    both = f(xs, wh)
    return both[:n] + both[n:] + f(xh, wl)


def lanes_of_sub(shape):
    lane = iota(shape, 1)
    return jnp.where(lane < NCL, lane // KC, (lane - NCL) // 8)


def own_mask():
    return iota((ROWS, NB), 0) // R == lanes_of_sub((ROWS, NB))


def by_load(x):
    y = x[:8] + x[8:]
    y = y + pltpu.roll(y, 4, 0)
    return jnp.concatenate([y, y], axis=0)


def coefs(v, w):
    return by_load(jnp.where(own_mask(), dot2(v, w, mm_t), 0.0))


def spread_back(sol, w):
    return dot2(jnp.where(own_mask(), sol, 0.0), w)


def ids_row(ids):
    lane = iota((8, NB), 1)
    row = jnp.full((8, NB), -1, I32)
    for s in range(S):
        for c in range(8):
            row = jnp.where(lane == NCL + 8 * s + c, ids[s, c], row)
    return row


def to_column(row):
    full = jnp.broadcast_to(row[:1], (NB, NB))
    eye = iota((NB, NB), 0) == iota((NB, NB), 1)
    return jnp.sum(jnp.where(eye, full, 0.0), axis=1, keepdims=True)


def window(x, at, width):
    lane = iota((x.shape[0], B), 1)
    tile, off = at // B, at % B
    here = x[:, tile * B : (tile + 1) * B]
    if off:
        here = pltpu.roll(here, B - off, 1)
        if off + width > B:
            after = pltpu.roll(x[:, (tile + 1) * B : (tile + 2) * B], B - off, 1)
            here = jnp.where(lane < B - off, here, after)
    return here


MSG = 5 * B


def clustered(c4, cc):
    return dot2(jnp.where(iota((8, NB), 1) < NCL, c4, 0.0)[:, :NCL], cc)


def marked(scalars):
    lane = iota((8, B), 1)
    extra = jnp.zeros((8, B), F32)
    for j, val in enumerate(scalars):
        extra = jnp.where(lane == 64 + j, val, extra)
    return extra


def write_message(msg, c4, ccp, row, scalars=()):
    col = to_column(row).astype(I32)
    hi, lo = split(c4)
    low = (c4 - hi.astype(F32) - lo.astype(F32)).astype(BF16)
    parts = jnp.concatenate([hi, lo, low], axis=0)
    lane = iota((8, B), 1)
    extra = marked(scalars)
    none = jnp.zeros((8, B), F32)
    cluster = [jnp.where(lane < NCL, window(ccp, NCL * k, NCL), 0.0) for k in range(NSUB)]
    for k in range(NSUB):
        n = iota((NB, 2 * B), 1)
        onehot = jnp.where((col == n + CHUNK * k) & (n < CHUNK), 1.0, 0.0).astype(BF16)
        y = mm(parts, onehot)
        y = y[:8] + y[8:16] + y[16:24]
        tiles = (
            y[:, :B],
            y[:, B:] + extra,
            jnp.where(lane < NCL, cluster[k], row),
            cluster[k + 1] if k + 1 < NSUB else none,
            cluster[k - 1] if k > 0 else none,
        )
        for t, x in enumerate(tiles):
            msg[k, :, t * B : (t + 1) * B] = x[:R]


def row_dot(a, b):
    return by_load(jnp.sum(a * b, axis=1, keepdims=True))


STATIC = NB + ROWS
WITHIN = STATIC + NCL * 6
PACK = 72


def k_coefs(ids, rhs, w, cc, msg, v_out):
    for s in range(S):
        v_out[R * s : R * s + R, :] = rhs[s]
    v = v_out[...]
    c4 = coefs(v, w[...])[:8]
    row = ids_row(ids).astype(F32)
    write_message(msg, c4, clustered(c4, cc[...]), row, [row_dot(v, v)[:8]])


def k_tables(after, signs, links, sg_out, idx_out):
    del after
    pos = iota((8, B), 1).astype(BF16)
    for s in range(S):
        sg_out[R * s : R * s + R, :] = jnp.broadcast_to(signs[s : s + 1, :].astype(F32), (R, D))
        for b in range(3):
            q = links[b, s : s + 1, :]
            if b == 0 or (b == 2 and s % 2 == 0):
                hot = jnp.where(iota((B, B), 0) == q, 1.0, 0.0).astype(BF16)
                q = mm_t(pos, hot)[:1].astype(I32)
            idx_out[b, R * s : R * s + R, :] = jnp.broadcast_to(q, (R, B))


def static_blocks(w, v, idx, b):
    lanes = pl.ds(pl.multiple_of(b * B, B), B)

    def moved(x, q):
        return jnp.take_along_axis(x, jnp.broadcast_to(q, x.shape), axis=1)

    for s in range(S):
        q = idx[b, R * s : R * s + 1, :]
        for at, n in ((KC * s, KC), (NCL + 8 * s, 8)):
            yield s, at, moved(w[at : at + n, lanes], q)
    yield None, NB, moved(v[:, lanes], idx[b])


def send_within(w, v, cc, idx, out, b):
    for _, at, x in static_blocks(w, v, idx, b):
        out[at : at + x.shape[0], :] = x
    for j in range(6):
        out[STATIC + NCL * j : STATIC + NCL * j + NCL, :] = cc[:, j * B : (j + 1) * B]


def coarse_rows(x):
    return jnp.concatenate([x[STATIC + NCL * j : STATIC + NCL * j + NCL, :] for j in range(6)], axis=1)


def k_send_first(after, signs, links, w, v, cc, sg_out, idx_out, first, second):
    k_tables(after, signs, links, sg_out, idx_out)
    odd = lax.axis_index("sub") % 2
    send_within(w, v, cc, idx_out, first, odd)
    send_within(w, v, cc, idx_out, second, 1 - odd)


def k_send_across(after, w, v, idx, first, second):
    del after
    flag = even_cluster()
    blocks = {(s, at): x for s, at, x in static_blocks(w, v, idx, 2)}

    def put(to, even, odd):
        n = even.shape[0]
        first[to : to + n, :] = pick(flag, even, odd)
        second[to : to + n, :] = pick(flag, odd, even)

    for h in range(2):
        s = 2 * h
        put(KC * h, blocks[s, KC * s], blocks[s + 1, KC * (s + 1)])
        put(2 * KC + 8 * h, blocks[s, NCL + 8 * s], blocks[s + 1, NCL + 8 * s + 8])
        x = blocks[None, NB][8 * h : 8 * h + 8]
        put(2 * KC + 16 + R * h, x[:R], x[R:])


def moved_blocks(v, idx):
    up, down, across = (
        jnp.take_along_axis(v[:, b * B : (b + 1) * B], idx[b], axis=1) for b in range(3)
    )
    even = jnp.concatenate([across[0:R], across[8 : 8 + R]], axis=0)
    odd = jnp.concatenate([across[R:8], across[8 + R :]], axis=0)
    return up, down, even, odd


def write_across(even, odd, first, second):
    flag = even_cluster()
    first[...] = pick(flag, even, odd)
    second[...] = pick(flag, odd, even)


def write_moved(v, idx, in1, in2, out1, out2):
    up, down, even, odd = moved_blocks(v, idx)
    flag = even_member()
    in1[...] = pick(flag, up, down)
    in2[...] = pick(flag, down, up)
    write_across(even, odd, out1, out2)


def across_of(out1, out2):
    flag = even_cluster()
    return pick(flag, out1, out2), pick(flag, out2, out1)


def within_of(in1, in2):
    flag = even_member()
    return pick(flag, in1, in2), pick(flag, in2, in1)


def take_static(in1, in2, out1, out2, pw_out, pv_out):
    from_next, from_prev = within_of(in1[0:STATIC, :], in2[0:STATIC, :])
    odd_in, even_in = across_of(out1[...], out2[...])
    pw_out[:, 0:B] = from_next[0:NB, :]
    pw_out[:, B : 2 * B] = from_prev[0:NB, :]
    for s in range(S):
        h = s // 2
        side = even_in if s % 2 else odd_in
        pw_out[KC * s : KC * s + KC, 2 * B :] = side[KC * h : KC * h + KC, :]
        at = 2 * KC + 8 * h
        pw_out[NCL + 8 * s : NCL + 8 * s + 8, 2 * B :] = side[at : at + 8, :]
        at = 2 * KC + 16 + R * h
        pv_out[R * s : R * s + R, 2 * B :] = side[at : at + R, :]
    pv_out[:, 0:B] = from_next[NB:STATIC, :]
    pv_out[:, B : 2 * B] = from_prev[NB:STATIC, :]


def member_sum(recv):
    total = recv[0]
    for k in range(1, NSUB):
        total = total + recv[k]
    return total


def k_rows(recv, out, csol, scalars=()):
    total = recv[0, :, 0:MSG]
    for k in range(1, NSUB):
        total = total + recv[k, :, 0:MSG]
    own = jnp.where(iota((R, B), 1) < NCL, total[:, 2 * B : 3 * B], 0.0)
    csol[0] = own
    csol[1] = total[:, 3 * B : 4 * B]
    csol[2] = total[:, 4 * B : 5 * B]
    second = total[:, B : 2 * B] + marked(scalars)[:R]
    x = jnp.concatenate([total[:, :B], second, own], axis=1)
    out[:, :, 0:D] = jnp.broadcast_to(x[None], (out.shape[0], R, D))


def cluster_ids(recv):
    lane = iota((8, B), 1)
    rows = []
    for half in range(2):
        ids = jnp.zeros((8, B), F32)
        for j in range(4):
            row = recv[4 * half + j, 0:1, 2 * B : 3 * B]
            row = pltpu.roll(jnp.broadcast_to(row, (8, B)), (32 + 32 * j) % B, 1)
            ids = jnp.where(lane // 32 == j, row, ids)
        rows.append(ids)
    return rows


def k_first_rows(recv, out, csol, ids_out):
    k_rows(recv, out, csol)
    low, high = cluster_ids(recv)
    ids = jnp.where(iota((8, B), 0) == 0, low, high)
    ids_out[...] = ids
    out[:, :, D:] = jnp.broadcast_to(ids[None, :R], (out.shape[0], R, B))


def k_pass(recv, out):
    y, z = lax.axis_index("y"), lax.axis_index("z")
    n_y, n_z = recv.shape[0], out.shape[0]
    total = jnp.sum(recv[:, :, 0 : 2 * B], axis=0)
    other = jnp.where(z == 0, jnp.minimum(y + 1, n_y - 1), jnp.maximum(y - 1, 0))
    x = jnp.concatenate([total, recv[y, :, 2 * B :], recv[other, :, 2 * B :]], axis=1)
    out[...] = jnp.broadcast_to(x[None], (n_z, *x.shape))


def neighbours(recv, at, wrapped_at):
    z = lax.axis_index("z")
    n_z = recv.shape[0]
    last, first = z == n_z - 1, z == 0
    nxt = recv[jnp.where(last, 0, z + 1)]
    prv = recv[jnp.where(first, n_z - 1, z - 1)]

    def tile(x, use_wrapped):
        plain = x[:, at : at + B]
        wrapped = x[:, wrapped_at : wrapped_at + B]
        x = jnp.where(jnp.full((R, B), use_wrapped.astype(I32), I32) == 1, wrapped, plain)
        return jnp.concatenate([x, x], axis=0)

    return tile(nxt, last), tile(prv, first)


def picked_columns(gc, rows, hi_out, lo_out):
    ids = jnp.concatenate([x[:1].astype(I32) for x in rows], axis=1)
    n = iota((gc.shape[1], ids.shape[1]), 0)
    onehot = jnp.where(n == ids, 1.0, 0.0).astype(BF16)
    gh, gl = split(gc[...])
    zero = jnp.zeros((2 * B - CHUNK, ids.shape[1]), BF16)
    hi_out[0:CHUNK, :] = mm(gh, onehot).astype(BF16)
    hi_out[CHUNK : 2 * B, :] = zero
    lo_out[0:CHUNK, :] = mm(gl, onehot).astype(BF16)
    lo_out[CHUNK : 2 * B, :] = zero


def solve(recv, parts, msg, cacross, stride):
    total = jnp.sum(recv[:, :, 0 : 2 * B], axis=0)
    total = jnp.concatenate([total, total], axis=0)
    second = total[:, B:]
    lane = iota((8, B), 1)
    x = jnp.concatenate([total[:, :B], jnp.where(lane < 64, second, 0.0)], axis=1)
    xh, xl = split(x)
    ys = []
    for gh, gl in parts:
        y = mm(jnp.concatenate([xh, xl], axis=0), gh[...])
        ys.append(y[:8] + y[8:] + mm(xh, gl[...]))

    def picked(kind, k, to):
        at = 32 * k
        return pltpu.roll(ys[kind][:, at // B * B : at // B * B + B], (to - at) % B, 1)

    none = jnp.zeros((8, B), F32)
    for k in range(NSUB):
        after = picked(0, k + 1, 32) if k + 1 < NSUB else none
        before = picked(0, k - 1, 64) if k > 0 else none
        here = jnp.where(lane < 32, picked(0, k, 0), jnp.where(lane < 64, after, before))
        msg[k, :, 0:B] = jnp.where(lane < 96, here, picked(1, k, 96))[:R]
        if msg.shape[2] > B:
            msg[k, :, B : 2 * B] = second[:R]
    after, before = neighbours(recv, 2 * B, 2 * B + stride)
    after = pltpu.roll(after, B - KC, 1)
    before = pltpu.roll(before, KC, 1)
    both = jnp.where(lane // KC % 2 == 0, after, before)
    cacross[...] = jnp.where(lane < NCL, both, 0.0)[:R]
    return second


def k_first_global(recv, own, gc, msg, scal, cacross, gh, gl, ah, al):
    picked_columns(gc, [own[0:1, :], own[1:2, :]], gh, gl)
    after, before = neighbours(recv, 3 * B, 5 * B)
    lane = iota((8, B), 1)
    after = pltpu.roll(after, B - 8, 1)
    before = pltpu.roll(before, 8, 1)
    ids = jnp.where(lane // 8 % 2 == 0, after, before)
    picked_columns(gc, [ids[0:1], ids[1:2]], ah, al)
    second = solve(recv, ((gh, gl), (ah, al)), msg, cacross, 2 * B)
    scal[...] = jnp.concatenate([second, second], axis=0)


def k_global(recv, gh, gl, ah, al, msg, cacross):
    solve(recv, ((gh, gl), (ah, al)), msg, cacross, B)


def four_times(x):
    x = jnp.concatenate([x, x], axis=0)
    return jnp.concatenate([x, x], axis=0)


def corrections(recv, csol, cacross, w, pw):
    picks = four_times(member_sum(recv)[:, :B])
    tail = iota((ROWS, B), 1) >= NCL

    def sol(cluster, turn):
        p = pltpu.roll(picks, turn, 1) if turn else picks
        return jnp.where(tail, p, four_times(cluster))

    own = spread_back(sol(csol[0], 96), w[...])
    sides = (sol(csol[1], 64), sol(csol[2], 32), sol(cacross[...], 0))
    pi = [spread_back(x, pw[:, b * B : (b + 1) * B]) for b, x in enumerate(sides)]
    return own, jnp.concatenate(pi, axis=1)


def across_received(out1, out2):
    odd_in, even_in = across_of(out1[...], out2[...])
    return jnp.concatenate([odd_in[0:R], even_in[0:R], odd_in[R:], even_in[R:]], axis=0)


def received(from_next, from_prev, out1, out2):
    return jnp.concatenate([from_next, from_prev, across_received(out1, out2)], axis=1)


def paired(n_cl):
    c, k = lax.axis_index("y") * lax.axis_size("z") + lax.axis_index("z"), lax.axis_index("sub")
    lane = iota((ROWS, D), 1)
    is_even = iota((ROWS, D), 0) // R % 2 == 0
    yes = [
        jnp.where(x, 1.0, 0.0) for x in (k < NSUB - 1, k > 0, c < n_cl - 1, c > 0)
    ]
    across = jnp.where(is_even, yes[2], yes[3])
    return jnp.where(lane < B, yes[0], jnp.where(lane < 2 * B, yes[1], across))


def image_of(d, pd, sg, ops):
    spread = sg * (d + pd)
    low = spread.astype(BF16)
    image = jnp.zeros((ROWS, D), F32)
    row = iota((ROWS, D), 0) // R
    for s in range(S):
        image = jnp.where(row == s, mm(low, ops[s]), image)
    return sg * image, row_dot(spread, image)


def k_first_image(
    recv, csol, cacross, in1, in2, out1, out2, w, v, sg, ops, idx,
    pw, pv, d_out, pd_out, signed_out, curv, up_out, down_out, *outs,
):
    take_static(in1, in2, out1, out2, pw, pv)
    fix, pfix = corrections(recv, csol, cacross, w, pw)
    d = v[...] - fix
    pd = pv[...] - pfix
    d_out[...] = d
    pd_out[...] = pd
    signed, c = image_of(d, pd, sg[...], ops)
    signed_out[...] = signed
    curv[...] = jnp.broadcast_to(c[:8], (8, B))
    up, down, even, odd = moved_blocks(signed, idx)
    up_out[...] = up
    down_out[...] = down
    write_across(even, odd, *outs)


def member_ids(all_ids, member, to):
    row = jnp.zeros((8, B), F32)
    which = jnp.full((8, B), member, I32)
    for j in range(NSUB):
        x = jnp.broadcast_to(all_ids[j // 4 : j // 4 + 1, :], (8, B))
        row = jnp.where(which == j, pltpu.roll(x, (to - 32 * (j % 4)) % B, 1), row)
    return row


def k_product(
    ids, signed, up, down, out1, out2, static1, static2, w, pw, cc, all_ids, across_out, msg
):
    k = lax.axis_index("sub")
    odd_k = k % 2
    across = across_received(out1, out2)
    across_out[...] = across
    u = signed[...]
    known = jnp.concatenate([u[:, : 2 * B], u[:, 2 * B :] + across], axis=1)
    own = coefs(known, w[...])[:8]

    def towards(b):
        lanes = pl.ds(pl.multiple_of(b * B, B), B)
        return coefs(signed[:, lanes], pw[:, lanes])[:8]

    first, second = towards(odd_k), towards(1 - odd_k)
    ccp = (
        clustered(own, cc[...])
        + clustered(first, coarse_rows(static1))
        + clustered(second, coarse_rows(static2))
    )
    lane = iota((8, B), 1)
    other = jnp.clip(k - 1 + 2 * odd_k, 0, NSUB - 1)

    def lanes_of(c96, c64, c32, rest):
        return jnp.where(
            lane >= 96, c96, jnp.where(lane >= 64, c64, jnp.where(lane >= 32, c32, rest))
        )

    c4 = lanes_of(own, pltpu.roll(first, B - 32, 1), pltpu.roll(second, B - 64, 1), 0.0)
    row = lanes_of(
        ids_row(ids).astype(F32),
        member_ids(all_ids, k + 1 - 2 * odd_k, 64),
        member_ids(all_ids, other, 32),
        -1.0,
    )
    write_message(msg, c4, ccp, row)
    after, before = jnp.minimum(k + 1, NSUB - 1), jnp.maximum(k - 1, 0)
    for s in range(S):
        at = MSG + B * s
        msg[after, :, at : at + B] = up[R * s : R * s + R, :]
        msg[before, :, at : at + B] = down[R * s : R * s + R, :]


def make_joined(n_cl):
    def k_joined(recv, signed, across, curv, v, out, csol, ap_out, pap_out):
        k = lax.axis_index("sub")

        def block(member, there):
            x = [recv[member, :, MSG + B * s : MSG + B * s + B] for s in range(S)]
            x = jnp.concatenate(x, axis=0)
            return pick(there, x, jnp.zeros_like(x))

        from_next = block(jnp.minimum(k + 1, NSUB - 1), k < NSUB - 1)
        from_prev = block(jnp.maximum(k - 1, 0), k > 0)
        u = signed[...]
        pi = jnp.concatenate([from_next, from_prev, across[...]], axis=1)
        ap = u + pi
        ap_out[...] = ap
        pap_out[...] = pi + paired(n_cl) * u
        scalars = [curv[...][:, :1], row_dot(v[...], ap)[:8], row_dot(ap, ap)[:8]]
        k_rows(recv, out, csol, scalars)

    return k_joined


def scalar_at(scal, j):
    return jnp.sum(jnp.where(iota((ROWS, B), 1) == 64 + j, scal, 0.0), axis=1, keepdims=True)


def k_last_image(
    recv, csol, cacross, scal0, w, pw, v, d, pd, ap, pap, sg, ops, idx,
    r_out, x_out, d_out, signed_out, msg, *outs,
):
    fix, pfix = corrections(recv, csol, cacross, w, pw)
    rho = scalar_at(scal0[...], 0)
    s1 = four_times(member_sum(recv)[:, B : 2 * B])
    step = rho / scalar_at(s1, 0)
    rho_new = rho - 2.0 * step * scalar_at(s1, 1) + step * step * scalar_at(s1, 2)
    beta = rho_new / rho
    ap_ = ap[...]
    d0 = d[...]
    pd0 = pd[...]
    r = v[...] - step * ap_
    r_out[...] = r
    x_out[...] = step * d0
    d1 = d0 - step * (ap_ - fix) + beta * d0
    pd1 = pd0 - step * (pap[...] - pfix) + beta * pd0
    d_out[...] = d1
    signed, c = image_of(d1, pd1, sg[...], ops)
    signed_out[...] = signed
    sq = row_dot(r, r)
    lane = iota((8, B), 1)
    row = iota((8, B), 0)
    both = jnp.where(lane == row, c[:8], jnp.where(lane == row + R, sq[:8], 0.0))
    line = jnp.sum(jnp.where(row < R, both, 0.0), axis=0, keepdims=True)
    msg[...] = jnp.broadcast_to(line[None], msg.shape)
    write_moved(signed, idx, *outs)


def k_total(recv, out):
    out[...] = jnp.broadcast_to(jnp.sum(recv[...], axis=0, keepdims=True), out.shape)


def k_finish(recv, signed, in1, in2, out1, out2, x, r, d, x_out, r_out):
    line = jnp.broadcast_to(jnp.sum(recv[...], axis=0), (ROWS, B))
    lane = iota((ROWS, B), 1)
    row = iota((ROWS, B), 0) % R
    curv = jnp.sum(jnp.where(lane == row, line, 0.0), axis=1, keepdims=True)
    rho = jnp.sum(jnp.where(lane == row + R, line, 0.0), axis=1, keepdims=True)
    step = rho / curv
    xn = x[...] + step * d[...]
    pi = received(*within_of(in1[...], in2[...]), out1, out2)
    rn = r[...] - step * (signed[...] + pi)
    for s in range(S):
        x_out[s] = xn[R * s : R * s + R]
        r_out[s] = rn[R * s : R * s + R]


def call(body, outs, *args, smem=(), scratch=()):
    def space(i):
        return pltpu.SMEM if i in smem else pltpu.VMEM

    specs = [pl.BlockSpec(memory_space=space(i)) for i in range(len(args))]
    out_shape = tuple(jax.ShapeDtypeStruct(s, t) for s, t in outs)
    return pl.pallas_call(
        body,
        out_shape=out_shape,
        in_specs=specs,
        out_specs=tuple(pl.BlockSpec(memory_space=pltpu.VMEM) for _ in outs),
        scratch_shapes=scratch,
        compiler_params=pltpu.CompilerParams(vmem_limit_bytes=VMEM_LIMIT),
    )(*args)


def to_owner(x, axis):
    return lax.all_to_all(x, axis, 0, 0, tiled=True)


def f32(*shape):
    return (shape, F32)


FIELD = f32(ROWS, D)


SENDS = (f32(ROWS, B), f32(ROWS, B), f32(2 * R, B), f32(2 * R, B))


def swap(x, axis, n, first):
    low = range(0 if first else 1, n - 1, 2)
    return lax.ppermute(x, axis, [p for i in low for p in ((i, i + 1), (i + 1, i))])


def exchange_across(first, second, n_cl):
    first = swap(first, CLUSTER, n_cl, True)
    second = swap(second, CLUSTER, n_cl, False)
    return first, second


def exchange(in1, in2, out1, out2, n_sub, n_cl):
    across = exchange_across(out1, out2, n_cl)
    in2 = swap(in2, "sub", n_sub, False)
    in1 = swap(in1, "sub", n_sub, True)
    return in1, in2, *across


def solve_all(rhs, operators, signs, links, cb, kb, ids, cluster_coarse, gc):
    n_sub = lax.axis_size("sub")
    n_y = lax.axis_size("y")
    n_z = lax.axis_size("z")
    n_cl = n_y * n_z
    cc = cluster_coarse.reshape(NCL, NSUB * NCL)
    message = f32(NSUB, R, MSG)
    picked = ((2 * B, 2 * B), BF16)
    answer = (f32(NSUB, R, B), f32(ROWS, B), f32(R, B))

    w = jnp.concatenate([cb.reshape(NCL, D), kb.reshape(NB - NCL, D)], axis=0)
    msg, v = call(k_coefs, (message, FIELD), ids, rhs, w, cc, smem=(0,))
    recv = to_owner(msg, "sub")
    rows, csol, all_ids = call(
        k_first_rows, (f32(n_y, R, 4 * B), f32(3, R, B), f32(8, B)), recv
    )
    sg, idx, in1, in2 = call(
        k_send_first,
        (FIELD, ((3, ROWS, B), I32), f32(WITHIN, B), f32(WITHIN, B)),
        all_ids, signs, links.transpose(1, 0, 2), w, v, cc,
    )
    recv = to_owner(rows, "y")
    in1 = swap(in1, "sub", n_sub, True)
    in2 = swap(in2, "sub", n_sub, False)
    (rows,) = call(k_pass, (f32(n_z, R, 6 * B),), recv)
    recv_z = to_owner(rows, "z")
    out = call(k_send_across, (f32(PACK, B), f32(PACK, B)), recv, w, v, idx)
    across = exchange_across(*out, n_cl)
    to_all, scal0, cacross, gh, gl, ah, al = call(
        k_first_global, (*answer, picked, picked, picked, picked), recv_z, all_ids, gc
    )
    to_all = to_owner(to_all, "sub")
    pw, pv, d, pd, signed, curv, up, down, *out = call(
        k_first_image,
        (f32(NB, D), FIELD, FIELD, FIELD, FIELD, f32(8, B), *SENDS),
        to_all, csol, cacross, in1, in2, *across,
        w, v, sg, operators, idx,
    )
    got = exchange_across(*out, n_cl)
    across, msg = call(
        k_product,
        (f32(ROWS, B), f32(NSUB, R, MSG + S * B)),
        ids, signed, up, down, *got, in1, in2, w, pw, cc, all_ids, smem=(0,),
    )
    rows, csol, ap, pap = call(
        make_joined(n_cl),
        (f32(n_y, R, D), f32(3, R, B), FIELD, FIELD),
        to_owner(msg, "sub"), signed, across, curv, v,
    )
    (rows,) = call(k_pass, (f32(n_z, R, 4 * B),), to_owner(rows, "y"))
    to_all, cacross = call(
        k_global,
        (f32(NSUB, R, 2 * B), f32(R, B)),
        to_owner(rows, "z"), gh, gl, ah, al,
    )
    r, x, d1, signed, line, *out = call(
        k_last_image,
        (FIELD, FIELD, FIELD, FIELD, f32(n_y * n_sub, 1, B), *SENDS),
        to_owner(to_all, "sub"), csol, cacross, scal0,
        w, pw, v, d, pd, ap, pap, sg, operators, idx,
    )
    line = to_owner(line, ("y", "sub"))
    (line,) = call(k_total, (f32(n_z, 1, B),), line)
    line = to_owner(line, "z")
    got = exchange(*out, n_sub, n_cl)
    out = f32(S, R, D)
    return call(k_finish, (out, out), line, signed, *got, x, r, d1)


def solution(mesh):
    n_y, n_z = 8, 12
    torus = Mesh(mesh.devices.reshape(n_y, n_z, NSUB), ("y", "z", "sub"))
    both = ("y", "z", "sub")
    in_specs = (
        P(both, None, None),
        P(both, None, None),
        P(both, None),
        P(both, None, None),
        P(both, None, None),
        P(both, None, None),
        P(both, None),
        P(CLUSTER, "sub", None),
        P("sub", None),
    )
    out_specs = (P(both, None, None), P(both, None, None))
    return jax.shard_map(solve_all, mesh=torus, in_specs=in_specs, out_specs=out_specs, check_vma=False)
```
